128 devices in a mesh: grp: 2 (over core), shard: 64 (over y, z, x).
Axes of the slice: x: 4, y: 4, z: 4, core: 2. Of those that a mesh axis runs over, the one named last changes fastest.
Arguments:
- blocks: float32 [8192, 128, 128], P(('grp', 'shard')), may hold values from -0.1875 to 0.1875
- block_row: int32 [8192], P(('grp', 'shard')), may hold values from 0 to 2047, as said below
- block_owner: int32 [8192, 1], P(('grp', 'shard')), may hold values from 0 to 63; in each aligned block of 64 rows (0 to 63, 64 to 127, ...) at most 2 rows name the same one
- block_col: int32 [8192], P(('grp', 'shard')), may hold values from 0 to 15
- right_side: float32 [262144, 8], P(('grp', 'shard')), may hold values from -6 to 6
Outputs:
- solution: float32 [131072, 8], P('shard')
- left_vector: float32 [262144, 8], P(('grp', 'shard'))
- rel_residual: float32 [8], replicated
The draws below stay inside these ranges and needn't reach their ends.
Inputs may be any that keep to these rules, and one draw needn't show every extreme that they name: `block_row`: block k lies in a row block of the device that holds it: between (k // 64) * 16 and (k // 64) * 16 + 15. `block_owner`: among the 64 blocks of one device, each owner is named at most 2 times, and in every draw some device names some owner exactly 2 times. `block_col`: a column block index among the 16 of the owner.
All inputs are finite; a program needn't handle non-finite values.
Results may differ from the reference program's by a relative error of at most 0.00024.
Values sent between devices are 32-bit elements; how exact they have to be, the bound alone decides.
No kernel may reach another device: no remote copies, remote signals or barrier semaphores. Data moves between devices by JAX's collectives and lax.ppermute only.
A program may use at most 64 MiB of HBM per device.

```python
import math
import jax
import jax.numpy as jnp
import numpy as np
from jax import lax

BS = 128
RHS = 8
ITERS = 4
BLK_DEV = 64
ROWS_DEV = 16
COLS_OWN = 16
CAP = 2
TOTAL_BLK = 8192
RB = 2048
CB = 1024
BLK_COL = 8
N_SHARD = 64


def draw_block_row(key, part):
    local = jax.random.randint(key, (TOTAL_BLK,), 0, ROWS_DEV, dtype=jnp.int32)
    holder = jnp.arange(TOTAL_BLK, dtype=jnp.int32) // BLK_DEV
    return (holder * ROWS_DEV + local).astype(jnp.int32)


def touch_ends(result, rng, smallest, top_value):
    index_at = [jax.random.randint(jax.random.fold_in(rng, axis), (), 0, length) for axis, length in enumerate(result.shape)]
    widest = result.shape.index(max(result.shape))
    neighbour = index_at[:widest] + [(index_at[widest] + 1) % result.shape[widest]] + index_at[widest + 1:]
    return result.at[tuple(index_at)].set(smallest).at[tuple(neighbour)].set(top_value)


def levels(key, shape, cuts, least, high):
    factor_of, own = 1.0, jax.random.fold_in(key, 6)
    for dim, parts in cuts:
        steps = jnp.exp(jax.random.uniform(jax.random.fold_in(own, dim), (parts,), jnp.float32, least / len(cuts), high / len(cuts)))
        factor_of = factor_of * jnp.repeat(steps, shape[dim] // parts).reshape([-1 if axis == dim else 1 for axis in range(len(shape))])
    return factor_of


def shared_out(own_key, own, number, rows, number_of, top, bound, lean):
    order = jax.random.permutation(own_key, number_of)
    crowded, ordinary = portions_of(number_of, rows * top, bound, lean, True), portions_of(number_of, rows * top, bound, lean, False)
    places = jnp.arange(number_of)

    def named(sizes, rotation):
        used = int((sizes > 0).sum())
        fixed = max(1, used // 4)
        passed = fixed + (places - fixed + rotation * (used - fixed)) % max(1, number_of - fixed)
        return jnp.zeros((number_of,), jnp.int32).at[order[jnp.where(places < fixed, places, passed)]].set(jnp.asarray(sizes, jnp.int32))

    sizes = jnp.where(number % 4 == 0, named(crowded, number // 4), named(ordinary, number - number // 4 - 1))
    mixed = jax.random.permutation(jax.random.fold_in(own, 3), number_of)
    giver, receiver = mixed[0:number_of // 2 * 2:2], mixed[1:number_of // 2 * 2:2]
    room = jnp.minimum(sizes[giver] - 1, bound - sizes[receiver]) // 2
    room = jnp.where((giver == order[0]) | (receiver == order[0]) | (sizes[receiver] == 0), 0, jnp.maximum(room, 0))
    passed = jax.random.randint(jax.random.fold_in(own, 4), (number_of // 2,), 0, 1 << 20) % (room + 1)
    sizes = sizes.at[giver].add(-passed).at[receiver].add(passed)
    labels = jnp.searchsorted(jnp.cumsum(sizes), jnp.arange(rows * top), side="right").astype(jnp.int32)
    grid = labels.reshape(top, rows).T
    grid = grid[jax.random.permutation(jax.random.fold_in(own, 1), rows)]
    rotation = jax.random.randint(jax.random.fold_in(own, 2), (rows, 1), 0, top)
    return jnp.take_along_axis(grid, (jnp.arange(top)[None, :] + rotation) % top, axis=1)


def portions_of(number_of, total, reach, lean, full):
    weights = [(1 << 20) // math.isqrt(standing ** lean) + 1 for standing in range(1, number_of + 1)]
    largest = reach if full else min(reach, max(-(-total // number_of), total * weights[0] // sum(weights)))
    least = 1 if total - largest >= number_of - 1 else 0
    holding, surplus = [largest] + [least] * (number_of - 1), total - largest - least * (number_of - 1)
    while surplus > 0:
        free = [i for i in range(1, number_of) if holding[i] < largest] or [i for i in range(1, number_of) if holding[i] < reach]
        pool, left = sum([weights[i] for i in free]), surplus
        for i in free:
            more = min(reach - holding[i], max(1, left * weights[i] // pool), surplus)
            holding[i] = holding[i] + more
            surplus = surplus - more
    return np.array(holding)


def normal_values(rng, dims, scale, most, cuts=(), kind=jnp.bfloat16):
    drawn = scale * jax.random.normal(rng, dims, jnp.float32)
    if cuts:
        drawn = drawn * levels(rng, dims, cuts, -0.22, 0.18)
    return jnp.clip(drawn, -most, most).astype(kind)


def setup_inputs(seed: int = 0) -> dict:
    keys = jax.random.split(jax.random.key(seed), 6)
    blocks = normal_values(keys[0], (TOTAL_BLK, BS, BS), (BS * BLK_COL) ** -0.5, 0.1875, ((0, 128),), jnp.float32)
    block_row = draw_block_row(jax.random.fold_in(keys[5], 71), 0)
    block_owner_keys = jax.random.split(jax.random.fold_in(keys[2], 1), TOTAL_BLK // BLK_DEV)
    block_owner_turns = jax.random.permutation(jax.random.fold_in(keys[2], 3), TOTAL_BLK // BLK_DEV)
    block_owner = jax.vmap(lambda own, number: shared_out(jax.random.fold_in(keys[2], 2), own, number, BLK_DEV, N_SHARD, 1, CAP, 2))(block_owner_keys, block_owner_turns).reshape((TOTAL_BLK, 1))
    block_col = touch_ends(jax.random.randint(keys[3], (TOTAL_BLK,), 0, COLS_OWN), jax.random.fold_in(keys[3], 1), 0, COLS_OWN - 1).astype(jnp.int32)
    right_side = normal_values(keys[4], (RB * BS, RHS), 1.0, 6.0, ((0, 128),), jnp.float32)
    return dict(blocks=blocks, block_row=block_row, block_owner=block_owner, block_col=block_col, right_side=right_side)


PRECISE = lax.Precision.HIGHEST

def forward(blocks, row_index, col_index, vector):
    pieces = vector.reshape(CB, BS, RHS)[col_index]
    product = jnp.einsum('kij,kjr->kir', blocks, pieces, precision=PRECISE)
    summed = jax.ops.segment_sum(product, row_index, num_segments=RB)
    return summed.reshape(RB * BS, RHS)

def adjoint(blocks, row_index, col_index, vector):
    pieces = vector.reshape(RB, BS, RHS)[row_index]
    product = jnp.einsum('kij,kir->kjr', blocks, pieces, precision=PRECISE)
    summed = jax.ops.segment_sum(product, col_index, num_segments=CB)
    return summed.reshape(CB * BS, RHS)

def column_norm(values):
    return jnp.sqrt(lax.optimization_barrier(jnp.sum(values * values, axis=0)))

def rotate(state, norm_left, norm_right, right_vec):
    solution, search, diag_bar, residual_norm = state
    radius = jnp.sqrt(diag_bar * diag_bar + norm_left * norm_left)
    cosine = diag_bar / radius
    sine_term = norm_left / radius
    coupling = sine_term * norm_right
    step_size = cosine * residual_norm
    solution = solution + step_size / radius * search
    search = right_vec - coupling / radius * search
    return (solution, search, -cosine * norm_right, sine_term * residual_norm)

def reference(blocks, block_row, block_owner, block_col, right_side):
    col_index = (block_owner[:, 0] * COLS_OWN + block_col).astype(jnp.int32)
    row_index = block_row.astype(jnp.int32)
    norm_start = column_norm(right_side)
    left_vec = right_side / norm_start
    right_vec = adjoint(blocks, row_index, col_index, left_vec)
    norm_right = column_norm(right_vec)
    right_vec = right_vec / norm_right
    state = (jnp.zeros_like(right_vec), right_vec, norm_right, norm_start)
    for repeat in range(ITERS):
        left_raw = forward(blocks, row_index, col_index, right_vec) - norm_right * left_vec
        norm_left = column_norm(left_raw)
        left_vec = left_raw / norm_left
        right_raw = adjoint(blocks, row_index, col_index, left_vec) - norm_left * right_vec
        norm_right = column_norm(right_raw)
        right_vec = right_raw / norm_right
        state = rotate(state, norm_left, norm_right, right_vec)
    return (state[0], left_vec, state[3] / norm_start)
```

```python
import jax
import jax.numpy as jnp
from jax import lax
from jax.experimental import pallas as pl
from jax.experimental.pallas import tpu as pltpu
from jax.sharding import Mesh
from jax.sharding import PartitionSpec as P

ITERS = 4
COLS_OWN = 16
SHARD = ("shard_0", "shard_1", "shard_2")
GRP_SHARD = ("grp", "shard_0", "shard_1", "shard_2")

OWNERS = 64
CAP = 2
BS = 128
RHS = 8
COUNT = 64
ROWS = 16
SLOTS = OWNERS * CAP
MSG = RHS * CAP + 1
TALL = OWNERS * MSG
CHUNK = 8
CHUNKS = COUNT // CHUNK

f32 = jnp.float32
bf16 = jnp.bfloat16


def diag_mask():
    sub = lax.broadcasted_iota(jnp.int32, (RHS, BS), 0)
    lane = lax.broadcasted_iota(jnp.int32, (RHS, BS), 1)
    return sub == lane


def row_of(column):
    return jnp.sum(jnp.where(diag_mask(), column, 0.0), axis=0, keepdims=True)


def column_of(row):
    spread = jnp.broadcast_to(row, (RHS, BS))
    total = jnp.sum(jnp.where(diag_mask(), spread, 0.0), axis=1, keepdims=True)
    return jnp.broadcast_to(total, (RHS, BS))


def squares(values):
    cube = values.reshape(values.shape[0] // RHS, RHS, BS)
    total = jnp.sum(jnp.sum(cube * cube, axis=0), axis=1, keepdims=True)
    return jnp.broadcast_to(total, (RHS, BS))


def tiled(column, count):
    return jnp.concatenate([column] * count, axis=0)


def sum_rows(ref):
    rows = [ref[pl.ds(MSG * o + MSG - 1, 1), :] for o in range(OWNERS)]
    while len(rows) > 1:
        rows = [rows[i] + rows[i + 1] for i in range(0, len(rows), 2)]
    return column_of(rows[0])


def put_rows(ref, row):
    for o in range(OWNERS):
        ref[pl.ds(MSG * o + MSG - 1, 1), :] = row


def split(x):
    high = x.astype(bf16)
    low = (x - high.astype(f32)).astype(bf16)
    return high, low


def stacked(x):
    high = x.astype(bf16).astype(f32)
    both = jnp.concatenate([high, x - high], axis=0).astype(bf16)
    return jnp.concatenate([both, both], axis=1)


def fold(out):
    first = out[0:8, 0:BS] + out[8:16, 0:BS]
    second = out[16:24, BS:] + out[24:32, BS:]
    return first, second


def chunk_copy(blocks, bbuf, sem, c):
    span = pl.ds(c * CHUNK, CHUNK)
    return pltpu.make_async_copy(blocks.at[span], bbuf.at[span], sem.at[c])


def split_left(us, left):
    for r in range(ROWS):
        us[r] = stacked(left[r * RHS : (r + 1) * RHS])


def adjoint_pair(k, row, pos, us, h0, l0, h1, l1, msg):
    lhs = jnp.concatenate([us[row[k]], us[row[k + 1]]], axis=0)
    rhs = jnp.concatenate(
        [jnp.concatenate([h0, l0], axis=0), jnp.concatenate([h1, l1], axis=0)], axis=1
    )
    out = lax.dot_general(lhs, rhs, (((1,), (0,)), ((), ())), preferred_element_type=f32)
    first, second = fold(out)
    msg[pl.ds(pos[k], RHS), :] = first
    msg[pl.ds(pos[k + 1], RHS), :] = second


def first_kernel(owner, row, col, right, blocks, msg, pos, bbuf, us, taken, sem):
    def begin(c, carry):
        chunk_copy(blocks, bbuf, sem, c).start()
        return carry

    lax.fori_loop(0, CHUNKS, begin, 0)
    right_all = right[...]
    msg[...] = jnp.zeros((TALL, BS), f32)
    put_rows(msg, row_of(squares(right_all)))
    split_left(us, right_all)

    def clear(o, carry):
        taken[o] = 0
        return carry

    lax.fori_loop(0, OWNERS, clear, 0)
    lane = lax.broadcasted_iota(jnp.int32, (1, BS), 1)

    def place(k, carry):
        o = owner[k]
        rank = taken[o]
        taken[o] = rank + 1
        pos[k] = o * MSG + rank * RHS
        span = pl.ds(o * MSG + MSG - 1, 1)
        msg[span, :] = jnp.where(lane == RHS + rank, col[k].astype(f32), msg[span, :])
        return carry

    lax.fori_loop(0, COUNT, place, 0)

    def chunk(c, carry):
        chunk_copy(blocks, bbuf, sem, c).wait()
        for j in range(0, CHUNK, 2):
            k = c * CHUNK + j
            h0, l0 = split(bbuf[k])
            h1, l1 = split(bbuf[k + 1])
            adjoint_pair(k, row, pos, us, h0, l0, h1, l1, msg)
        return carry

    lax.fori_loop(0, CHUNKS, chunk, 0)


def forward_part(pos, row, inc, uraw, nleft, blocks, lraw, bbuf, sem, keep):
    def begin(c, carry):
        chunk_copy(blocks, bbuf, sem, c).start()
        return carry

    lax.fori_loop(0, CHUNKS, begin, 0)
    norm_right = jnp.sqrt(sum_rows(inc))
    lraw[...] = jnp.zeros((ROWS * RHS, BS), f32)

    def chunk(c, carry):
        chunk_copy(blocks, bbuf, sem, c).wait()
        for j in range(0, CHUNK, 2):
            k = c * CHUNK + j
            h0, l0 = split(bbuf[k])
            h1, l1 = split(bbuf[k + 1])
            if keep is not None:
                keep[0][k] = h0
                keep[1][k] = l0
                keep[0][k + 1] = h1
                keep[1][k + 1] = l1
            lhs = jnp.concatenate(
                [stacked(inc[pl.ds(pos[k], RHS), :]), stacked(inc[pl.ds(pos[k + 1], RHS), :])],
                axis=0,
            )
            rhs = jnp.concatenate(
                [jnp.concatenate([h0, l0], axis=1), jnp.concatenate([h1, l1], axis=1)], axis=0
            )
            out = lax.dot_general(lhs, rhs, (((1,), (1,)), ((), ())), preferred_element_type=f32)
            first, second = fold(out)
            span = pl.ds(pl.multiple_of(row[k] * RHS, RHS), RHS)
            lraw[span, :] = lraw[span, :] + first
            span = pl.ds(pl.multiple_of(row[k + 1] * RHS, RHS), RHS)
            lraw[span, :] = lraw[span, :] + second
        return carry

    lax.fori_loop(0, CHUNKS, chunk, 0)
    left = lraw[...] / tiled(norm_right, ROWS) - tiled(norm_right, ROWS) * (
        uraw[...] / tiled(nleft[...], ROWS)
    )
    lraw[...] = left
    return left, norm_right


def user_kernel(pos, row, inc, uraw, nleft, blocks, msg, lraw, nright, bbuf, high, low, us, sem):
    left, norm_right = forward_part(
        pos, row, inc, uraw, nleft, blocks, lraw, bbuf, sem, (high, low)
    )
    nright[...] = norm_right
    msg[...] = jnp.zeros((TALL, BS), f32)
    put_rows(msg, row_of(squares(left)))
    split_left(us, left)

    def chunk(c, carry):
        for j in range(0, CHUNK, 2):
            k = c * CHUNK + j
            adjoint_pair(k, row, pos, us, high[k], low[k], high[k + 1], low[k + 1], msg)
        return carry

    lax.fori_loop(0, CHUNKS, chunk, 0)


def last_user_kernel(pos, row, inc, uraw, nleft, blocks, msg, lraw, nright, bbuf, sem):
    left, norm_right = forward_part(pos, row, inc, uraw, nleft, blocks, lraw, bbuf, sem, None)
    nright[...] = norm_right
    msg[...] = jnp.broadcast_to(row_of(squares(left)), msg.shape)


def gather_slots(inc, cols_of, half, parts):
    for part in parts:
        part[...] = jnp.zeros((COLS_OWN * RHS, BS), f32)

    def step(g, carry):
        for j in range(4):
            o = g * 4 + j
            for s in range(CAP):
                c = cols_of(o, s)
                span = pl.ds(pl.multiple_of(c * RHS, RHS), RHS)
                part = parts[(2 * j + s) % len(parts)]
                part[span, :] = part[span, :] + inc[pl.ds(o * MSG + s * RHS, RHS), :]
        return carry

    lax.fori_loop(0, OWNERS // 4, step, 0)
    half[pl.ds(0, COLS_OWN * RHS), :] = (parts[0][...] + parts[1][...]) + (
        parts[2][...] + parts[3][...]
    )
    half[pl.ds(COLS_OWN * RHS, RHS), :] = sum_rows(inc)


def first_owner_kernel(inc, half, cols, p0, p1, p2, p3, vcols, scols, sem):
    for o in range(OWNERS):
        vcols[pl.ds(o, 1), :] = inc[pl.ds(MSG * o + MSG - 1, 1), :].astype(jnp.int32)
    copy = pltpu.make_async_copy(vcols, scols, sem)
    copy.start()
    copy.wait()

    def cols_of(o, s):
        c = scols[o, RHS + s]
        cols[o * CAP + s] = c
        return c

    gather_slots(inc, cols_of, half, (p0, p1, p2, p3))


def owner_kernel(cols, inc, half, p0, p1, p2, p3):
    gather_slots(inc, lambda o, s: cols[o * CAP + s], half, (p0, p1, p2, p3))


def send_slots(cols, raw, msg):
    put_rows(msg, row_of(squares(raw[...])))

    def step(g, carry):
        for j in range(4):
            o = g * 4 + j
            for s in range(CAP):
                c = cols[o * CAP + s]
                span = pl.ds(pl.multiple_of(c * RHS, RHS), RHS)
                msg[pl.ds(o * MSG + s * RHS, RHS), :] = raw[span, :]
        return carry

    lax.fori_loop(0, OWNERS // 4, step, 0)


def first_send_kernel(cols, mine, theirs, msg, raw, nleft):
    norm_left = jnp.sqrt(mine[pl.ds(COLS_OWN * RHS, RHS), :] + theirs[pl.ds(COLS_OWN * RHS, RHS), :])
    nleft[...] = norm_left
    body = pl.ds(0, COLS_OWN * RHS)
    raw[...] = (mine[body, :] + theirs[body, :]) / tiled(norm_left, COLS_OWN)
    send_slots(cols, raw, msg)


def advance(first, solution, search, diag_bar, residual, norm_left, norm_right, right_vec):
    radius = jnp.sqrt(diag_bar * diag_bar + norm_left * norm_left)
    cosine = diag_bar / radius
    sine_term = norm_left / radius
    return radius, cosine, sine_term


def send_kernel(first, cols, mine, theirs, qprev, nright, *refs):
    if first:
        start, msg, raw, nleft, sol, search, scal = refs
    else:
        sol_in, search_in, scal_in, msg, raw, nleft, sol, search, scal = refs
    n = COLS_OWN
    norm_left = jnp.sqrt(mine[pl.ds(n * RHS, RHS), :] + theirs[pl.ds(n * RHS, RHS), :])
    norm_right = nright[...]
    nleft[...] = norm_left
    body = pl.ds(0, n * RHS)
    vec = qprev[...] / tiled(norm_right, n)
    raw[...] = (mine[body, :] + theirs[body, :]) / tiled(norm_left, n) - tiled(norm_left, n) * vec
    send_slots(cols, raw, msg)
    if first:
        old_search = vec
        diag_bar = norm_right
        residual = start[...]
        old_sol = jnp.zeros((n * RHS, BS), f32)
    else:
        radius = scal_in[pl.ds(0, RHS), :]
        cosine = scal_in[pl.ds(RHS, RHS), :]
        sine_term = scal_in[pl.ds(2 * RHS, RHS), :]
        residual = scal_in[pl.ds(3 * RHS, RHS), :]
        coupling = sine_term * norm_right
        old_search = vec - tiled(coupling / radius, n) * search_in[...]
        diag_bar = -cosine * norm_right
        old_sol = sol_in[...]
    radius = jnp.sqrt(diag_bar * diag_bar + norm_left * norm_left)
    cosine = diag_bar / radius
    sine_term = norm_left / radius
    sol[...] = old_sol + tiled(cosine * residual / radius, n) * old_search
    search[...] = old_search
    scal[pl.ds(0, RHS), :] = radius
    scal[pl.ds(RHS, RHS), :] = cosine
    scal[pl.ds(2 * RHS, RHS), :] = sine_term
    scal[pl.ds(3 * RHS, RHS), :] = sine_term * residual


def final_kernel(rows, lraw, qprev, nright, sol_in, search_in, scal_in, start, sol, left, rel):
    n = COLS_OWN
    norm_left = jnp.sqrt(column_of(jnp.sum(rows[...], axis=0, keepdims=True)))
    norm_right = nright[...]
    left[...] = lraw[...] / tiled(norm_left, ROWS)
    radius = scal_in[pl.ds(0, RHS), :]
    cosine = scal_in[pl.ds(RHS, RHS), :]
    sine_term = scal_in[pl.ds(2 * RHS, RHS), :]
    residual = scal_in[pl.ds(3 * RHS, RHS), :]
    vec = qprev[...] / tiled(norm_right, n)
    search = vec - tiled(sine_term * norm_right / radius, n) * search_in[...]
    diag_bar = -cosine * norm_right
    radius = jnp.sqrt(diag_bar * diag_bar + norm_left * norm_left)
    cosine = diag_bar / radius
    sine_term = norm_left / radius
    sol[...] = sol_in[...] + tiled(cosine * residual / radius, n) * search
    rel[...] = row_of(sine_term * residual / start[...])


def shape(*dims, dtype=f32):
    return jax.ShapeDtypeStruct(dims, dtype)


VMEM = pl.BlockSpec(memory_space=pltpu.VMEM)
SMEM = pl.BlockSpec(memory_space=pltpu.SMEM)
HBM = pl.BlockSpec(memory_space=pl.ANY)
PARTS = [pltpu.VMEM((COLS_OWN * RHS, BS), f32)] * 4
BUFFER = pltpu.VMEM((COUNT, BS, BS), f32)
LEFTS = pltpu.VMEM((ROWS, 2 * RHS, 2 * BS), bf16)
SEMS = pltpu.SemaphoreType.DMA((CHUNKS,))


def call(body, ins, outs, specs_out=None, scratch=()):
    return pl.pallas_call(
        body,
        out_shape=outs,
        in_specs=ins,
        out_specs=specs_out or jax.tree.map(lambda _: VMEM, outs),
        scratch_shapes=scratch,
        compiler_params=pltpu.CompilerParams(vmem_limit_bytes=24 * 1024 * 1024),
    )


def exchange(msg):
    sent = msg.reshape(OWNERS, MSG * BS)
    return lax.all_to_all(sent, SHARD, 0, 0, tiled=True).reshape(TALL, BS)


def swap(half):
    return lax.ppermute(half, "grp", [(0, 1), (1, 0)])


def on_device(blocks, block_row, block_owner, block_col, right_side):
    row = lax.rem(block_row, ROWS)
    owner = block_owner[:, 0]
    right = right_side.reshape(ROWS, BS, RHS).transpose(0, 2, 1).reshape(ROWS * RHS, BS)
    vec = shape(COLS_OWN * RHS, BS)
    col8 = shape(RHS, BS)
    msg_shape = shape(TALL, BS)
    half_shape = shape(COLS_OWN * RHS + RHS, BS)

    msg, pos = call(
        first_kernel,
        [SMEM, SMEM, SMEM, VMEM, HBM],
        (msg_shape, shape(COUNT, dtype=jnp.int32)),
        (VMEM, SMEM),
        [BUFFER, LEFTS, pltpu.SMEM((OWNERS,), jnp.int32), SEMS],
    )(owner, row, block_col, right, blocks)
    inc = exchange(msg)
    half, cols = call(
        first_owner_kernel,
        [VMEM],
        (half_shape, shape(SLOTS, dtype=jnp.int32)),
        (VMEM, SMEM),
        PARTS
        + [
            pltpu.VMEM((OWNERS, BS), jnp.int32),
            pltpu.SMEM((OWNERS, BS), jnp.int32),
            pltpu.SemaphoreType.DMA(()),
        ],
    )(inc)
    msg, raw, norm_left = call(
        first_send_kernel, [SMEM, VMEM, VMEM], (msg_shape, vec, col8)
    )(cols, half, swap(half))
    start = norm_left
    left = right
    state = None
    for repeat in range(ITERS):
        inc = exchange(msg)
        if repeat == ITERS - 1:
            break
        msg, left, norm_right = call(
            user_kernel,
            [SMEM, SMEM, VMEM, VMEM, VMEM, HBM],
            (msg_shape, vec, col8),
            None,
            [
                BUFFER,
                pltpu.VMEM((COUNT, BS, BS), bf16),
                pltpu.VMEM((COUNT, BS, BS), bf16),
                LEFTS,
                SEMS,
            ],
        )(pos, row, inc, left, norm_left, blocks)
        inc = exchange(msg)
        half = call(owner_kernel, [SMEM, VMEM], half_shape, None, PARTS)(cols, inc)
        first = repeat == 0
        tail = (start,) if first else state
        outs = call(
            lambda *refs, first=first: send_kernel(first, *refs),
            [SMEM] + [VMEM] * (4 + len(tail)),
            (msg_shape, vec, col8, vec, vec, shape(4 * RHS, BS)),
        )(cols, half, swap(half), raw, norm_right, *tail)
        msg, raw, norm_left = outs[:3]
        state = outs[3:]
    rows, left, norm_right = call(
        last_user_kernel,
        [SMEM, SMEM, VMEM, VMEM, VMEM, HBM],
        (shape(2 * OWNERS, BS), vec, col8),
        None,
        [BUFFER, SEMS],
    )(pos, row, inc, left, norm_left, blocks)
    rows = lax.all_to_all(rows, GRP_SHARD, 0, 0, tiled=True)
    sol, left, rel = call(
        final_kernel, [VMEM] * 8, (vec, vec, shape(1, BS))
    )(rows, left, raw, norm_right, *state, start)

    def tall(x):
        return x.reshape(COLS_OWN, RHS, BS).transpose(0, 2, 1).reshape(COLS_OWN * BS, RHS)

    return tall(sol), tall(left), rel[0, :RHS]


def solution(mesh):
    torus = Mesh(
        mesh.devices.reshape(mesh.shape["grp"], 4, 4, 4), ("grp", "shard_0", "shard_1", "shard_2")
    )
    return jax.shard_map(
        on_device,
        mesh=torus,
        in_specs=(
            P(GRP_SHARD, None, None),
            P(GRP_SHARD),
            P(GRP_SHARD, None),
            P(GRP_SHARD),
            P(GRP_SHARD, None),
        ),
        out_specs=(P(SHARD, None), P(GRP_SHARD, None), P()),
        check_vma=False,
    )
```

```python
import jax
import jax.numpy as jnp
from jax import lax
from jax.experimental import pallas as pl
from jax.experimental.pallas import tpu as pltpu
from jax.sharding import Mesh
from jax.sharding import PartitionSpec as P

ITERS = 4
COLS_OWN = 16
SHARD = ("shard_0", "shard_1", "shard_2")
GRP_SHARD = ("grp", "shard_0", "shard_1", "shard_2")

OWNERS = 64
CAP = 2
BS = 128
RHS = 8
COUNT = 64
ROWS = 16
SLOTS = OWNERS * CAP
MSG = RHS * CAP + 1
TALL = OWNERS * MSG
CHUNK = 8
UNROLL = 16
CHUNKS = COUNT // CHUNK

f32 = jnp.float32
bf16 = jnp.bfloat16


def diag_mask():
    sub = lax.broadcasted_iota(jnp.int32, (RHS, BS), 0)
    lane = lax.broadcasted_iota(jnp.int32, (RHS, BS), 1)
    return sub == lane


def row_of(column):
    return jnp.sum(jnp.where(diag_mask(), column, 0.0), axis=0, keepdims=True)


def column_of(row):
    spread = jnp.broadcast_to(row, (RHS, BS))
    total = jnp.sum(jnp.where(diag_mask(), spread, 0.0), axis=1, keepdims=True)
    return jnp.broadcast_to(total, (RHS, BS))


def squares(values):
    cube = values.reshape(values.shape[0] // RHS, RHS, BS)
    total = jnp.sum(jnp.sum(cube * cube, axis=0), axis=1, keepdims=True)
    return jnp.broadcast_to(total, (RHS, BS))


def tiled(column, count):
    return jnp.concatenate([column] * count, axis=0)


def sum_rows(ref):
    rows = [ref[pl.ds(MSG * o + MSG - 1, 1), :] for o in range(OWNERS)]
    while len(rows) > 1:
        rows = [rows[i] + rows[i + 1] for i in range(0, len(rows), 2)]
    return column_of(rows[0])


def put_rows(ref, row):
    for o in range(OWNERS):
        ref[pl.ds(MSG * o + MSG - 1, 1), :] = row


def split(x):
    high = x.astype(bf16)
    low = (x - high.astype(f32)).astype(bf16)
    return high, low


def stacked(x):
    high = x.astype(bf16).astype(f32)
    both = jnp.concatenate([high, x - high], axis=0).astype(bf16)
    return jnp.concatenate([both, both], axis=1)


def fold(out):
    first = out[0:8, 0:BS] + out[8:16, 0:BS]
    second = out[16:24, BS:] + out[24:32, BS:]
    return first, second


def chunk_copy(blocks, bbuf, sem, c):
    span = pl.ds(c * CHUNK, CHUNK)
    return pltpu.make_async_copy(blocks.at[span], bbuf.at[span], sem.at[c])


def split_left(us, left):
    for r in range(ROWS):
        us[r] = stacked(left[r * RHS : (r + 1) * RHS])


def adjoint_pair(k, tab, us, h0, l0, h1, l1, msg):
    lhs = jnp.concatenate([us[tab[COUNT + k]], us[tab[COUNT + k + 1]]], axis=0)
    rhs = jnp.concatenate(
        [jnp.concatenate([h0, l0], axis=0), jnp.concatenate([h1, l1], axis=0)], axis=1
    )
    out = lax.dot_general(lhs, rhs, (((1,), (0,)), ((), ())), preferred_element_type=f32)
    first, second = fold(out)
    msg[pl.ds(tab[k], RHS), :] = first
    msg[pl.ds(tab[k + 1], RHS), :] = second


def first_kernel(
    owner_in, row_in, col_in, right_in, blocks,
    msg, tab, high, low,
    bbuf, right, us, owner, row, col, taken, sem, small,
):
    loads = [
        pltpu.make_async_copy(owner_in, owner, small.at[0]),
        pltpu.make_async_copy(row_in, row, small.at[1]),
        pltpu.make_async_copy(col_in, col, small.at[2]),
        pltpu.make_async_copy(right_in, right, small.at[3]),
    ]
    for load in loads:
        load.start()

    def begin(c, carry):
        chunk_copy(blocks, bbuf, sem, c).start()
        return carry

    lax.fori_loop(0, CHUNKS, begin, 0)
    msg[...] = jnp.zeros((TALL, BS), f32)

    def clear(g, carry):
        for j in range(8):
            taken[g * 8 + j] = 0
        return carry

    lax.fori_loop(0, OWNERS // 8, clear, 0)
    for load in loads:
        load.wait()
    right_all = right[...]
    put_rows(msg, row_of(squares(right_all)))
    split_left(us, right_all)
    lane = lax.broadcasted_iota(jnp.int32, (1, BS), 1)

    def place(g, carry):
        for j in range(4):
            k = g * 4 + j
            o = owner[k]
            rank = taken[o]
            taken[o] = rank + 1
            tab[k] = o * MSG + rank * RHS
            tab[COUNT + k] = lax.rem(row[k], ROWS)
            span = pl.ds(o * MSG + MSG - 1, 1)
            msg[span, :] = jnp.where(lane == RHS + rank, col[k].astype(f32), msg[span, :])
        return carry

    lax.fori_loop(0, COUNT // 4, place, 0)

    def chunk(c, carry):
        chunk_copy(blocks, bbuf, sem, c).wait()
        for j in range(0, CHUNK, 2):
            k = c * CHUNK + j
            h0, l0 = split(bbuf[k])
            h1, l1 = split(bbuf[k + 1])
            high[k] = h0
            low[k] = l0
            high[k + 1] = h1
            low[k + 1] = l1
            adjoint_pair(k, tab, us, h0, l0, h1, l1, msg)
        return carry

    lax.fori_loop(0, CHUNKS, chunk, 0)


def forward_part(tab_in, inc, uraw, nleft, high, low, lraw, other, tab, sem):
    copy = pltpu.make_async_copy(tab_in, tab, sem)
    copy.start()
    norm_right = jnp.sqrt(sum_rows(inc))
    lraw[...] = jnp.zeros((ROWS * RHS, BS), f32)
    other[...] = jnp.zeros((ROWS * RHS, BS), f32)
    copy.wait()

    def chunk(c, carry):
        for j in range(0, UNROLL, 2):
            k = c * UNROLL + j
            lhs = jnp.concatenate(
                [stacked(inc[pl.ds(tab[k], RHS), :]), stacked(inc[pl.ds(tab[k + 1], RHS), :])],
                axis=0,
            )
            rhs = jnp.concatenate(
                [
                    jnp.concatenate([high[k], low[k]], axis=1),
                    jnp.concatenate([high[k + 1], low[k + 1]], axis=1),
                ],
                axis=0,
            )
            out = lax.dot_general(lhs, rhs, (((1,), (1,)), ((), ())), preferred_element_type=f32)
            first, second = fold(out)
            span = pl.ds(pl.multiple_of(tab[COUNT + k] * RHS, RHS), RHS)
            lraw[span, :] = lraw[span, :] + first
            span = pl.ds(pl.multiple_of(tab[COUNT + k + 1] * RHS, RHS), RHS)
            other[span, :] = other[span, :] + second
        return carry

    lax.fori_loop(0, COUNT // UNROLL, chunk, 0)
    image = lraw[...] + other[...]
    left = image / tiled(norm_right, ROWS) - tiled(norm_right, ROWS) * (
        uraw[...] / tiled(nleft[...], ROWS)
    )
    lraw[...] = left
    return left, norm_right


def user_kernel(tab_in, inc, uraw, nleft, high, low, msg, lraw, nright, other, us, tab, sem):
    left, norm_right = forward_part(
        tab_in, inc, uraw, nleft, high, low, lraw, other, tab, sem
    )
    nright[...] = norm_right
    msg[...] = jnp.zeros((TALL, BS), f32)
    put_rows(msg, row_of(squares(left)))
    split_left(us, left)

    def chunk(c, carry):
        for j in range(0, UNROLL, 2):
            k = c * UNROLL + j
            adjoint_pair(k, tab, us, high[k], low[k], high[k + 1], low[k + 1], msg)
        return carry

    lax.fori_loop(0, COUNT // UNROLL, chunk, 0)


def last_user_kernel(tab_in, inc, uraw, nleft, high, low, msg, lraw, nright, other, tab, sem):
    left, norm_right = forward_part(
        tab_in, inc, uraw, nleft, high, low, lraw, other, tab, sem
    )
    nright[...] = norm_right
    msg[...] = jnp.broadcast_to(row_of(squares(left)), msg.shape)


def gather_slots(inc, cols_of, half, parts, copy):
    copy.start()
    half[pl.ds(COLS_OWN * RHS, RHS), :] = sum_rows(inc)
    for part in parts:
        part[...] = jnp.zeros((COLS_OWN * RHS, BS), f32)
    copy.wait()

    def step(g, carry):
        for j in range(8):
            o = g * 8 + j
            for s in range(CAP):
                c = cols_of(o, s)
                span = pl.ds(pl.multiple_of(c * RHS, RHS), RHS)
                part = parts[(2 * j + s) % len(parts)]
                part[span, :] = part[span, :] + inc[pl.ds(o * MSG + s * RHS, RHS), :]
        return carry

    lax.fori_loop(0, OWNERS // 8, step, 0)
    half[pl.ds(0, COLS_OWN * RHS), :] = (parts[0][...] + parts[1][...]) + (
        parts[2][...] + parts[3][...]
    )


def first_owner_kernel(inc, half, cols, p0, p1, p2, p3, vcols, scols, sem):
    for o in range(OWNERS):
        vcols[pl.ds(o, 1), :] = inc[pl.ds(MSG * o + MSG - 1, 1), :].astype(jnp.int32)
    copy = pltpu.make_async_copy(vcols, scols, sem)

    def cols_of(o, s):
        c = scols[o, RHS + s]
        cols[o * CAP + s] = c
        return c

    gather_slots(inc, cols_of, half, (p0, p1, p2, p3), copy)


def owner_kernel(cols_in, inc, half, p0, p1, p2, p3, cols, sem):
    copy = pltpu.make_async_copy(cols_in, cols, sem)
    gather_slots(inc, lambda o, s: cols[o * CAP + s], half, (p0, p1, p2, p3), copy)


def send_slots(cols, raw, msg, copy):
    put_rows(msg, row_of(squares(raw[...])))
    copy.wait()

    def step(g, carry):
        for j in range(8):
            o = g * 8 + j
            for s in range(CAP):
                c = cols[o * CAP + s]
                span = pl.ds(pl.multiple_of(c * RHS, RHS), RHS)
                msg[pl.ds(o * MSG + s * RHS, RHS), :] = raw[span, :]
        return carry

    lax.fori_loop(0, OWNERS // 8, step, 0)


def first_send_kernel(cols_in, mine, theirs, msg, raw, nleft, cols, sem):
    copy = pltpu.make_async_copy(cols_in, cols, sem)
    copy.start()
    norm_left = jnp.sqrt(mine[pl.ds(COLS_OWN * RHS, RHS), :] + theirs[pl.ds(COLS_OWN * RHS, RHS), :])
    nleft[...] = norm_left
    body = pl.ds(0, COLS_OWN * RHS)
    raw[...] = (mine[body, :] + theirs[body, :]) / tiled(norm_left, COLS_OWN)
    send_slots(cols, raw, msg, copy)


def send_kernel(first, cols_in, mine, theirs, qprev, nright, *refs):
    cols, sem = refs[-2:]
    copy = pltpu.make_async_copy(cols_in, cols, sem)
    copy.start()
    if first:
        start, msg, raw, nleft, sol, search, scal = refs[:-2]
    else:
        sol_in, search_in, scal_in, msg, raw, nleft, sol, search, scal = refs[:-2]
    n = COLS_OWN
    norm_left = jnp.sqrt(mine[pl.ds(n * RHS, RHS), :] + theirs[pl.ds(n * RHS, RHS), :])
    norm_right = nright[...]
    nleft[...] = norm_left
    body = pl.ds(0, n * RHS)
    vec = qprev[...] / tiled(norm_right, n)
    raw[...] = (mine[body, :] + theirs[body, :]) / tiled(norm_left, n) - tiled(norm_left, n) * vec
    send_slots(cols, raw, msg, copy)
    if first:
        old_search = vec
        diag_bar = norm_right
        residual = start[...]
        old_sol = jnp.zeros((n * RHS, BS), f32)
    else:
        radius = scal_in[pl.ds(0, RHS), :]
        cosine = scal_in[pl.ds(RHS, RHS), :]
        sine_term = scal_in[pl.ds(2 * RHS, RHS), :]
        residual = scal_in[pl.ds(3 * RHS, RHS), :]
        coupling = sine_term * norm_right
        old_search = vec - tiled(coupling / radius, n) * search_in[...]
        diag_bar = -cosine * norm_right
        old_sol = sol_in[...]
    radius = jnp.sqrt(diag_bar * diag_bar + norm_left * norm_left)
    cosine = diag_bar / radius
    sine_term = norm_left / radius
    sol[...] = old_sol + tiled(cosine * residual / radius, n) * old_search
    search[...] = old_search
    scal[pl.ds(0, RHS), :] = radius
    scal[pl.ds(RHS, RHS), :] = cosine
    scal[pl.ds(2 * RHS, RHS), :] = sine_term
    scal[pl.ds(3 * RHS, RHS), :] = sine_term * residual


def final_kernel(rows, lraw, qprev, nright, sol_in, search_in, scal_in, start, sol, left, rel):
    n = COLS_OWN
    norm_left = jnp.sqrt(column_of(jnp.sum(rows[...], axis=0, keepdims=True)))
    norm_right = nright[...]
    left[...] = lraw[...] / tiled(norm_left, ROWS)
    radius = scal_in[pl.ds(0, RHS), :]
    cosine = scal_in[pl.ds(RHS, RHS), :]
    sine_term = scal_in[pl.ds(2 * RHS, RHS), :]
    residual = scal_in[pl.ds(3 * RHS, RHS), :]
    vec = qprev[...] / tiled(norm_right, n)
    search = vec - tiled(sine_term * norm_right / radius, n) * search_in[...]
    diag_bar = -cosine * norm_right
    radius = jnp.sqrt(diag_bar * diag_bar + norm_left * norm_left)
    cosine = diag_bar / radius
    sine_term = norm_left / radius
    sol[...] = sol_in[...] + tiled(cosine * residual / radius, n) * search
    rel[...] = row_of(sine_term * residual / start[...])[0, :RHS]


def shape(*dims, dtype=f32):
    return jax.ShapeDtypeStruct(dims, dtype)


VMEM = pl.BlockSpec(memory_space=pltpu.VMEM)
SMEM = pl.BlockSpec(memory_space=pltpu.SMEM)
HBM = pl.BlockSpec(memory_space=pltpu.HBM)
ANY = pl.BlockSpec(memory_space=pl.ANY)
PARTS = [pltpu.VMEM((COLS_OWN * RHS, BS), f32)] * 4
LEFTS = pltpu.VMEM((ROWS, 2 * RHS, 2 * BS), bf16)
LEFT = pltpu.VMEM((ROWS * RHS, BS), f32)
ONE = pltpu.SemaphoreType.DMA(())
TABLE = [pltpu.SMEM((SLOTS,), jnp.int32), ONE]


def call(body, ins, outs, specs_out=None, scratch=()):
    return pl.pallas_call(
        body,
        out_shape=outs,
        in_specs=ins,
        out_specs=specs_out or jax.tree.map(lambda _: VMEM, outs),
        scratch_shapes=scratch,
        compiler_params=pltpu.CompilerParams(vmem_limit_bytes=24 * 1024 * 1024),
    )


def exchange(msg):
    sent = msg.reshape(OWNERS, MSG * BS)
    return lax.all_to_all(sent, SHARD, 0, 0, tiled=True).reshape(TALL, BS)


def swap(half):
    return lax.ppermute(half, "grp", [(0, 1), (1, 0)])


def on_device(blocks, block_row, block_owner, block_col, right_side):
    owner = block_owner[:, 0]
    right = right_side.reshape(ROWS, BS, RHS).transpose(0, 2, 1).reshape(ROWS * RHS, BS)
    vec = shape(COLS_OWN * RHS, BS)
    col8 = shape(RHS, BS)
    msg_shape = shape(TALL, BS)
    half_shape = shape(COLS_OWN * RHS + RHS, BS)
    table = shape(SLOTS, dtype=jnp.int32)
    halves = shape(COUNT, BS, BS, dtype=bf16)

    msg, tab, high, low = call(
        first_kernel,
        [HBM] * 5,
        (msg_shape, table, halves, halves),
        (VMEM, SMEM, VMEM, VMEM),
        [pltpu.VMEM((COUNT, BS, BS), f32), LEFT, LEFTS]
        + [pltpu.SMEM((COUNT,), jnp.int32)] * 4
        + [pltpu.SemaphoreType.DMA((CHUNKS,)), pltpu.SemaphoreType.DMA((4,))],
    )(owner, block_row, block_col, right, blocks)
    inc = exchange(msg)
    half, cols = call(
        first_owner_kernel,
        [VMEM],
        (half_shape, table),
        (VMEM, SMEM),
        PARTS + [pltpu.VMEM((OWNERS, BS), jnp.int32), pltpu.SMEM((OWNERS, BS), jnp.int32), ONE],
    )(inc)
    msg, raw, norm_left = call(
        first_send_kernel, [ANY, VMEM, VMEM], (msg_shape, vec, col8), None, TABLE
    )(cols, half, swap(half))
    start = norm_left
    left = right
    state = None
    for repeat in range(ITERS):
        inc = exchange(msg)
        if repeat == ITERS - 1:
            break
        msg, left, norm_right = call(
            user_kernel,
            [ANY] + [VMEM] * 5,
            (msg_shape, vec, col8),
            None,
            [LEFT, LEFTS] + TABLE,
        )(tab, inc, left, norm_left, high, low)
        inc = exchange(msg)
        half = call(owner_kernel, [ANY, VMEM], half_shape, None, PARTS + TABLE)(cols, inc)
        first = repeat == 0
        tail = (start,) if first else state
        outs = call(
            lambda *refs, first=first: send_kernel(first, *refs),
            [ANY] + [VMEM] * (4 + len(tail)),
            (msg_shape, vec, col8, vec, vec, shape(4 * RHS, BS)),
            None,
            TABLE,
        )(cols, half, swap(half), raw, norm_right, *tail)
        msg, raw, norm_left = outs[:3]
        state = outs[3:]
    rows, left, norm_right = call(
        last_user_kernel,
        [ANY] + [VMEM] * 5,
        (shape(2 * OWNERS, BS), vec, col8),
        None,
        [LEFT] + TABLE,
    )(tab, inc, left, norm_left, high, low)
    rows = lax.all_to_all(rows, GRP_SHARD, 0, 0, tiled=True)
    sol, left, rel = call(
        final_kernel, [VMEM] * 8, (vec, vec, shape(RHS))
    )(rows, left, raw, norm_right, *state, start)

    def tall(x):
        return x.reshape(COLS_OWN, RHS, BS).transpose(0, 2, 1).reshape(COLS_OWN * BS, RHS)

    return tall(sol), tall(left), rel


def solution(mesh):
    torus = Mesh(
        mesh.devices.reshape(mesh.shape["grp"], 4, 4, 4), ("grp", "shard_0", "shard_1", "shard_2")
    )
    return jax.shard_map(
        on_device,
        mesh=torus,
        in_specs=(
            P(GRP_SHARD, None, None),
            P(GRP_SHARD),
            P(GRP_SHARD, None),
            P(GRP_SHARD),
            P(GRP_SHARD, None),
        ),
        out_specs=(P(SHARD, None), P(GRP_SHARD, None), P()),
        check_vma=False,
    )
```

```python
import jax
import jax.numpy as jnp
from jax import lax
from jax.experimental import pallas as pl
from jax.experimental.pallas import tpu as pltpu
from jax.sharding import Mesh
from jax.sharding import PartitionSpec as P

ITERS = 4
COLS_OWN = 16
SHARD = ("shard_0", "shard_1", "shard_2")
GRP_SHARD = ("grp", "shard_0", "shard_1", "shard_2")

OWNERS = 64
CAP = 2
BS = 128
RHS = 8
COUNT = 64
ROWS = 16
SLOTS = OWNERS * CAP
MSG = RHS * CAP + 1
TALL = OWNERS * MSG
CHUNK = 8
UNROLL = 16
CHUNKS = COUNT // CHUNK

f32 = jnp.float32
bf16 = jnp.bfloat16


def diag_mask():
    sub = lax.broadcasted_iota(jnp.int32, (RHS, BS), 0)
    lane = lax.broadcasted_iota(jnp.int32, (RHS, BS), 1)
    return sub == lane


def row_of(column):
    return jnp.sum(jnp.where(diag_mask(), column, 0.0), axis=0, keepdims=True)


def column_of(row):
    spread = jnp.broadcast_to(row, (RHS, BS))
    total = jnp.sum(jnp.where(diag_mask(), spread, 0.0), axis=1, keepdims=True)
    return jnp.broadcast_to(total, (RHS, BS))


def squares(values):
    cube = values.reshape(values.shape[0] // RHS, RHS, BS)
    total = jnp.sum(jnp.sum(cube * cube, axis=0), axis=1, keepdims=True)
    return jnp.broadcast_to(total, (RHS, BS))


def tiled(column, count):
    return jnp.concatenate([column] * count, axis=0)


def sum_rows(ref):
    rows = [ref[pl.ds(MSG * o + MSG - 1, 1), :] for o in range(OWNERS)]
    while len(rows) > 1:
        rows = [rows[i] + rows[i + 1] for i in range(0, len(rows), 2)]
    return column_of(rows[0])


def put_rows(ref, row):
    for o in range(OWNERS):
        ref[pl.ds(MSG * o + MSG - 1, 1), :] = row


def split(x):
    high = x.astype(bf16)
    low = (x - high.astype(f32)).astype(bf16)
    return high, low


def stacked(x):
    high = x.astype(bf16).astype(f32)
    both = jnp.concatenate([high, x - high], axis=0).astype(bf16)
    return jnp.concatenate([both, both], axis=1)


def fold(out):
    first = out[0:8, 0:BS] + out[8:16, 0:BS]
    second = out[16:24, BS:] + out[24:32, BS:]
    return first, second


def chunk_copy(blocks, bbuf, sem, c):
    span = pl.ds(c * CHUNK, CHUNK)
    return pltpu.make_async_copy(blocks.at[span], bbuf.at[span], sem.at[c])


def split_left(us, left):
    for r in range(ROWS):
        us[r] = stacked(left[r * RHS : (r + 1) * RHS])


def adjoint_pair(k, tab, us, h0, l0, h1, l1, msg):
    lhs = jnp.concatenate([us[tab[COUNT + k]], us[tab[COUNT + k + 1]]], axis=0)
    rhs = jnp.concatenate(
        [jnp.concatenate([h0, l0], axis=0), jnp.concatenate([h1, l1], axis=0)], axis=1
    )
    out = lax.dot_general(lhs, rhs, (((1,), (0,)), ((), ())), preferred_element_type=f32)
    first, second = fold(out)
    msg[pl.ds(tab[k], RHS), :] = first
    msg[pl.ds(tab[k + 1], RHS), :] = second


def first_kernel(
    owner_in, row_in, col_in, right_in, blocks,
    msg, tab, high, low,
    bbuf, right, us, owner, row, col, taken, sem, little,
):
    loads = [
        pltpu.make_async_copy(owner_in, owner, little.at[0]),
        pltpu.make_async_copy(row_in, row, little.at[1]),
        pltpu.make_async_copy(col_in, col, little.at[2]),
        pltpu.make_async_copy(right_in, right, little.at[3]),
    ]
    for load in loads:
        load.start()

    def begin(c, carry):
        chunk_copy(blocks, bbuf, sem, c).start()
        return carry

    lax.fori_loop(0, CHUNKS, begin, 0)
    msg[...] = jnp.zeros((TALL, BS), f32)

    def clear(g, carry):
        for j in range(8):
            taken[g * 8 + j] = 0
        return carry

    lax.fori_loop(0, OWNERS // 8, clear, 0)
    for load in loads:
        load.wait()
    right_all = right[...]
    put_rows(msg, row_of(squares(right_all)))
    split_left(us, right_all)
    lane = lax.broadcasted_iota(jnp.int32, (1, BS), 1)

    def place(g, carry):
        for j in range(4):
            k = g * 4 + j
            o = owner[k]
            rank = taken[o]
            taken[o] = rank + 1
            tab[k] = o * MSG + rank * RHS
            tab[COUNT + k] = lax.rem(row[k], ROWS)
            span = pl.ds(o * MSG + MSG - 1, 1)
            msg[span, :] = jnp.where(lane == RHS + rank, col[k].astype(f32), msg[span, :])
        return carry

    lax.fori_loop(0, COUNT // 4, place, 0)

    def chunk(c, carry):
        chunk_copy(blocks, bbuf, sem, c).wait()
        for j in range(0, CHUNK, 2):
            k = c * CHUNK + j
            h0, l0 = split(bbuf[k])
            h1, l1 = split(bbuf[k + 1])
            high[k] = h0
            low[k] = l0
            high[k + 1] = h1
            low[k + 1] = l1
            adjoint_pair(k, tab, us, h0, l0, h1, l1, msg)
        return carry

    lax.fori_loop(0, CHUNKS, chunk, 0)


def forward_part(tab, inc, uraw, nleft, high, low, lraw, other):
    norm_right = jnp.sqrt(sum_rows(inc))
    lraw[...] = jnp.zeros((ROWS * RHS, BS), f32)
    other[...] = jnp.zeros((ROWS * RHS, BS), f32)

    def chunk(c, carry):
        for j in range(0, UNROLL, 2):
            k = c * UNROLL + j
            lhs = jnp.concatenate(
                [stacked(inc[pl.ds(tab[k], RHS), :]), stacked(inc[pl.ds(tab[k + 1], RHS), :])],
                axis=0,
            )
            rhs = jnp.concatenate(
                [
                    jnp.concatenate([high[k], low[k]], axis=1),
                    jnp.concatenate([high[k + 1], low[k + 1]], axis=1),
                ],
                axis=0,
            )
            out = lax.dot_general(lhs, rhs, (((1,), (1,)), ((), ())), preferred_element_type=f32)
            first, second = fold(out)
            span = pl.ds(pl.multiple_of(tab[COUNT + k] * RHS, RHS), RHS)
            lraw[span, :] = lraw[span, :] + first
            span = pl.ds(pl.multiple_of(tab[COUNT + k + 1] * RHS, RHS), RHS)
            other[span, :] = other[span, :] + second
        return carry

    lax.fori_loop(0, COUNT // UNROLL, chunk, 0)
    image = lraw[...] + other[...]
    left = image / tiled(norm_right, ROWS) - tiled(norm_right, ROWS) * (
        uraw[...] / tiled(nleft[...], ROWS)
    )
    lraw[...] = left
    return left, norm_right


def user_kernel(tab, inc, uraw, nleft, high, low, msg, lraw, nright, other, us):
    left, norm_right = forward_part(tab, inc, uraw, nleft, high, low, lraw, other)
    nright[...] = norm_right
    msg[...] = jnp.zeros((TALL, BS), f32)
    put_rows(msg, row_of(squares(left)))
    split_left(us, left)

    def chunk(c, carry):
        for j in range(0, UNROLL, 2):
            k = c * UNROLL + j
            adjoint_pair(k, tab, us, high[k], low[k], high[k + 1], low[k + 1], msg)
        return carry

    lax.fori_loop(0, COUNT // UNROLL, chunk, 0)


def last_user_kernel(tab, inc, uraw, nleft, high, low, msg, lraw, nright, other):
    left, norm_right = forward_part(tab, inc, uraw, nleft, high, low, lraw, other)
    nright[...] = norm_right
    msg[...] = jnp.broadcast_to(row_of(squares(left)), msg.shape)


def gather_slots(inc, cols_of, half, parts, copy=None):
    if copy is not None:
        copy.start()
    half[pl.ds(COLS_OWN * RHS, RHS), :] = sum_rows(inc)
    for part in parts:
        part[...] = jnp.zeros((COLS_OWN * RHS, BS), f32)
    if copy is not None:
        copy.wait()

    def step(g, carry):
        for j in range(8):
            o = g * 8 + j
            for s in range(CAP):
                c = cols_of(o, s)
                span = pl.ds(pl.multiple_of(c * RHS, RHS), RHS)
                part = parts[(2 * j + s) % len(parts)]
                part[span, :] = part[span, :] + inc[pl.ds(o * MSG + s * RHS, RHS), :]
        return carry

    lax.fori_loop(0, OWNERS // 8, step, 0)
    half[pl.ds(0, COLS_OWN * RHS), :] = (parts[0][...] + parts[1][...]) + (
        parts[2][...] + parts[3][...]
    )


def first_owner_kernel(inc, half, cols, p0, p1, p2, p3, vcols, scols, sem):
    for o in range(OWNERS):
        vcols[pl.ds(o, 1), :] = inc[pl.ds(MSG * o + MSG - 1, 1), :].astype(jnp.int32)
    copy = pltpu.make_async_copy(vcols, scols, sem)

    def cols_of(o, s):
        c = scols[o, RHS + s]
        cols[o * CAP + s] = c
        return c

    gather_slots(inc, cols_of, half, (p0, p1, p2, p3), copy)


def owner_kernel(cols, inc, half, p0, p1, p2, p3):
    gather_slots(inc, lambda o, s: cols[o * CAP + s], half, (p0, p1, p2, p3))


def send_slots(cols, raw, msg):
    put_rows(msg, row_of(squares(raw[...])))

    def step(g, carry):
        for j in range(8):
            o = g * 8 + j
            for s in range(CAP):
                c = cols[o * CAP + s]
                span = pl.ds(pl.multiple_of(c * RHS, RHS), RHS)
                msg[pl.ds(o * MSG + s * RHS, RHS), :] = raw[span, :]
        return carry

    lax.fori_loop(0, OWNERS // 8, step, 0)


def first_send_kernel(cols, mine, theirs, msg, raw, nleft):
    norm_left = jnp.sqrt(mine[pl.ds(COLS_OWN * RHS, RHS), :] + theirs[pl.ds(COLS_OWN * RHS, RHS), :])
    nleft[...] = norm_left
    body = pl.ds(0, COLS_OWN * RHS)
    raw[...] = (mine[body, :] + theirs[body, :]) / tiled(norm_left, COLS_OWN)
    send_slots(cols, raw, msg)


def send_kernel(first, cols, mine, theirs, qprev, nright, *refs):
    if first:
        start, msg, raw, nleft, sol, search, scal = refs
    else:
        sol_in, search_in, scal_in, msg, raw, nleft, sol, search, scal = refs
    n = COLS_OWN
    norm_left = jnp.sqrt(mine[pl.ds(n * RHS, RHS), :] + theirs[pl.ds(n * RHS, RHS), :])
    norm_right = nright[...]
    nleft[...] = norm_left
    body = pl.ds(0, n * RHS)
    vec = qprev[...] / tiled(norm_right, n)
    raw[...] = (mine[body, :] + theirs[body, :]) / tiled(norm_left, n) - tiled(norm_left, n) * vec
    send_slots(cols, raw, msg)
    if first:
        old_search = vec
        diag_bar = norm_right
        residual = start[...]
        old_sol = jnp.zeros((n * RHS, BS), f32)
    else:
        radius = scal_in[pl.ds(0, RHS), :]
        cosine = scal_in[pl.ds(RHS, RHS), :]
        sine_term = scal_in[pl.ds(2 * RHS, RHS), :]
        residual = scal_in[pl.ds(3 * RHS, RHS), :]
        coupling = sine_term * norm_right
        old_search = vec - tiled(coupling / radius, n) * search_in[...]
        diag_bar = -cosine * norm_right
        old_sol = sol_in[...]
    radius = jnp.sqrt(diag_bar * diag_bar + norm_left * norm_left)
    cosine = diag_bar / radius
    sine_term = norm_left / radius
    sol[...] = old_sol + tiled(cosine * residual / radius, n) * old_search
    search[...] = old_search
    scal[pl.ds(0, RHS), :] = radius
    scal[pl.ds(RHS, RHS), :] = cosine
    scal[pl.ds(2 * RHS, RHS), :] = sine_term
    scal[pl.ds(3 * RHS, RHS), :] = sine_term * residual


def final_kernel(rows, lraw, qprev, nright, sol_in, search_in, scal_in, start, sol, left, rel):
    n = COLS_OWN
    norm_left = jnp.sqrt(column_of(jnp.sum(rows[...], axis=0, keepdims=True)))
    norm_right = nright[...]
    left[...] = lraw[...] / tiled(norm_left, ROWS)
    radius = scal_in[pl.ds(0, RHS), :]
    cosine = scal_in[pl.ds(RHS, RHS), :]
    sine_term = scal_in[pl.ds(2 * RHS, RHS), :]
    residual = scal_in[pl.ds(3 * RHS, RHS), :]
    vec = qprev[...] / tiled(norm_right, n)
    search = vec - tiled(sine_term * norm_right / radius, n) * search_in[...]
    diag_bar = -cosine * norm_right
    radius = jnp.sqrt(diag_bar * diag_bar + norm_left * norm_left)
    cosine = diag_bar / radius
    sine_term = norm_left / radius
    sol[...] = sol_in[...] + tiled(cosine * residual / radius, n) * search
    rel[...] = row_of(sine_term * residual / start[...])[0, :RHS]


def shape(*dims, dtype=f32):
    return jax.ShapeDtypeStruct(dims, dtype)


VMEM = pl.BlockSpec(memory_space=pltpu.VMEM)
SMEM = pl.BlockSpec(memory_space=pltpu.SMEM)
HBM = pl.BlockSpec(memory_space=pltpu.HBM)
ANY = pl.BlockSpec(memory_space=pl.ANY)
PARTS = [pltpu.VMEM((COLS_OWN * RHS, BS), f32)] * 4
LEFTS = pltpu.VMEM((ROWS, 2 * RHS, 2 * BS), bf16)
LEFT = pltpu.VMEM((ROWS * RHS, BS), f32)
ONE = pltpu.SemaphoreType.DMA(())


def call(body, ins, outs, specs_out=None, scratch=()):
    return pl.pallas_call(
        body,
        out_shape=outs,
        in_specs=ins,
        out_specs=specs_out or jax.tree.map(lambda _: VMEM, outs),
        scratch_shapes=scratch,
        compiler_params=pltpu.CompilerParams(vmem_limit_bytes=24 * 1024 * 1024),
    )


def exchange(msg):
    sent = msg.reshape(OWNERS, MSG * BS)
    return lax.all_to_all(sent, SHARD, 0, 0, tiled=True).reshape(TALL, BS)


def swap(half):
    return lax.ppermute(half, "grp", [(0, 1), (1, 0)])


def small(x):
    return pltpu.with_memory_space_constraint(x, pltpu.SMEM)


def on_device(blocks, block_row, block_owner, block_col, right_side):
    owner = block_owner[:, 0]
    right = right_side.reshape(ROWS, BS, RHS).transpose(0, 2, 1).reshape(ROWS * RHS, BS)
    vec = shape(COLS_OWN * RHS, BS)
    col8 = shape(RHS, BS)
    msg_shape = shape(TALL, BS)
    half_shape = shape(COLS_OWN * RHS + RHS, BS)
    table = pltpu.MemorySpace.SMEM((SLOTS,), jnp.int32)
    halves = shape(COUNT, BS, BS, dtype=bf16)

    msg, tab, high, low = call(
        first_kernel,
        [HBM] * 5,
        (msg_shape, table, halves, halves),
        (VMEM, SMEM, VMEM, VMEM),
        [pltpu.VMEM((COUNT, BS, BS), f32), LEFT, LEFTS]
        + [pltpu.SMEM((COUNT,), jnp.int32)] * 4
        + [pltpu.SemaphoreType.DMA((CHUNKS,)), pltpu.SemaphoreType.DMA((4,))],
    )(*(pltpu.with_memory_space_constraint(x, pltpu.HBM) for x in (owner, block_row, block_col, right, blocks)))
    inc = exchange(msg)
    half, cols = call(
        first_owner_kernel,
        [VMEM],
        (half_shape, table),
        (VMEM, SMEM),
        PARTS + [pltpu.VMEM((OWNERS, BS), jnp.int32), pltpu.SMEM((OWNERS, BS), jnp.int32), ONE],
    )(inc)
    msg, raw, norm_left = call(
        first_send_kernel, [SMEM, VMEM, VMEM], (msg_shape, vec, col8)
    )(small(cols), half, swap(half))
    start = norm_left
    left = right
    state = None
    for repeat in range(ITERS):
        inc = exchange(msg)
        if repeat == ITERS - 1:
            break
        msg, left, norm_right = call(
            user_kernel,
            [SMEM] + [VMEM] * 5,
            (msg_shape, vec, col8),
            None,
            [LEFT, LEFTS],
        )(small(tab), inc, left, norm_left, high, low)
        inc = exchange(msg)
        half = call(owner_kernel, [SMEM, VMEM], half_shape, None, PARTS)(small(cols), inc)
        first = repeat == 0
        tail = (start,) if first else state
        outs = call(
            lambda *refs, first=first: send_kernel(first, *refs),
            [SMEM] + [VMEM] * (4 + len(tail)),
            (msg_shape, vec, col8, vec, vec, shape(4 * RHS, BS)),
        )(small(cols), half, swap(half), raw, norm_right, *tail)
        msg, raw, norm_left = outs[:3]
        state = outs[3:]
    rows, left, norm_right = call(
        last_user_kernel,
        [SMEM] + [VMEM] * 5,
        (shape(2 * OWNERS, BS), vec, col8),
        None,
        [LEFT],
    )(small(tab), inc, left, norm_left, high, low)
    rows = lax.all_to_all(rows, GRP_SHARD, 0, 0, tiled=True)
    sol, left, rel = call(
        final_kernel, [VMEM] * 8, (vec, vec, shape(RHS))
    )(rows, left, raw, norm_right, *state, start)

    def tall(x):
        return x.reshape(COLS_OWN, RHS, BS).transpose(0, 2, 1).reshape(COLS_OWN * BS, RHS)

    return tall(sol), tall(left), rel


def solution(mesh):
    torus = Mesh(
        mesh.devices.reshape(mesh.shape["grp"], 4, 4, 4), ("grp", "shard_0", "shard_1", "shard_2")
    )
    return jax.shard_map(
        on_device,
        mesh=torus,
        in_specs=(
            P(GRP_SHARD, None, None),
            P(GRP_SHARD),
            P(GRP_SHARD, None),
            P(GRP_SHARD),
            P(GRP_SHARD, None),
        ),
        out_specs=(P(SHARD, None), P(GRP_SHARD, None), P()),
        check_vma=False,
    )
```

```python
import jax
import jax.numpy as jnp
from jax import lax
from jax.experimental import pallas as pl
from jax.experimental.pallas import tpu as pltpu
from jax.sharding import Mesh
from jax.sharding import PartitionSpec as P

ITERS = 4
COLS_OWN = 16
SHARD = ("shard_0", "shard_1", "shard_2")
GRP_SHARD = ("grp", "shard_0", "shard_1", "shard_2")

OWNERS = 64
CAP = 2
BS = 128
RHS = 8
COUNT = 64
ROWS = 16
SLOTS = OWNERS * CAP
MSG = RHS * CAP + 1
TALL = OWNERS * MSG
CHUNK = 8
CHUNKS = COUNT // CHUNK

f32 = jnp.float32
bf16 = jnp.bfloat16


def diag_mask():
    sub = lax.broadcasted_iota(jnp.int32, (RHS, BS), 0)
    lane = lax.broadcasted_iota(jnp.int32, (RHS, BS), 1)
    return sub == lane


def row_of(column):
    return jnp.sum(jnp.where(diag_mask(), column, 0.0), axis=0, keepdims=True)


def column_of(row):
    spread = jnp.broadcast_to(row, (RHS, BS))
    total = jnp.sum(jnp.where(diag_mask(), spread, 0.0), axis=1, keepdims=True)
    return jnp.broadcast_to(total, (RHS, BS))


def squares(values):
    cube = values.reshape(values.shape[0] // RHS, RHS, BS)
    total = jnp.sum(jnp.sum(cube * cube, axis=0), axis=1, keepdims=True)
    return jnp.broadcast_to(total, (RHS, BS))


def tiled(column, count):
    return jnp.concatenate([column] * count, axis=0)


def sum_rows(ref):
    rows = [ref[pl.ds(MSG * o + MSG - 1, 1), :] for o in range(OWNERS)]
    while len(rows) > 1:
        rows = [rows[i] + rows[i + 1] for i in range(0, len(rows), 2)]
    return column_of(rows[0])


def put_rows(ref, row):
    for o in range(OWNERS):
        ref[pl.ds(MSG * o + MSG - 1, 1), :] = row


def split(x):
    high = x.astype(bf16)
    low = (x - high.astype(f32)).astype(bf16)
    return high, low


def stacked(x):
    high = x.astype(bf16).astype(f32)
    both = jnp.concatenate([high, x - high], axis=0).astype(bf16)
    return jnp.concatenate([both, both], axis=1)


def fold(out):
    return out[0:RHS] + out[RHS:]


def chunk_copy(blocks, bbuf, sem, c):
    span = pl.ds(c * CHUNK, CHUNK)
    return pltpu.make_async_copy(blocks.at[span], bbuf.at[span], sem.at[c])


def split_left(us, left):
    for r in range(ROWS):
        us[r] = stacked(left[r * RHS : (r + 1) * RHS])


def adjoint_block(pos, row, us, high, low, msg):
    rhs = jnp.concatenate([high, low], axis=0)
    out = lax.dot_general(us[row], rhs, (((1,), (0,)), ((), ())), preferred_element_type=f32)
    msg[pl.ds(pos, RHS), :] = fold(out)


def forward_block(piece, high, low):
    rhs = jnp.concatenate([high, low], axis=1)
    out = lax.dot_general(
        stacked(piece), rhs, (((1,), (1,)), ((), ())), preferred_element_type=f32
    )
    return fold(out)


def first_kernel(
    owner_in, row_in, col_in, right_in, blocks,
    msg, tab, high, low,
    bbuf, right, us, owner, row, col, taken, sem, little,
):
    loads = [
        pltpu.make_async_copy(owner_in, owner, little.at[0]),
        pltpu.make_async_copy(row_in, row, little.at[1]),
        pltpu.make_async_copy(col_in, col, little.at[2]),
        pltpu.make_async_copy(right_in, right, little.at[3]),
    ]
    for load in loads:
        load.start()

    def begin(c, carry):
        chunk_copy(blocks, bbuf, sem, c).start()
        return carry

    lax.fori_loop(0, CHUNKS, begin, 0)
    msg[...] = jnp.zeros((TALL, BS), f32)

    def clear(g, carry):
        for j in range(8):
            taken[g * 8 + j] = 0
        return carry

    lax.fori_loop(0, OWNERS // 8, clear, 0)
    for load in loads:
        load.wait()
    right_all = right[...]
    put_rows(msg, row_of(squares(right_all)))
    split_left(us, right_all)
    lane = lax.broadcasted_iota(jnp.int32, (1, BS), 1)

    for c in range(CHUNKS):
        chunk_copy(blocks, bbuf, sem, c).wait()
        for k in range(c * CHUNK, (c + 1) * CHUNK):
            o = owner[k]
            rank = taken[o]
            taken[o] = rank + 1
            pos = o * MSG + rank * RHS
            line = lax.rem(row[k], ROWS)
            tab[k] = pos
            tab[COUNT + k] = line
            span = pl.ds(o * MSG + MSG - 1, 1)
            msg[span, :] = jnp.where(lane == RHS + rank, col[k].astype(f32), msg[span, :])
            h, l = split(bbuf[k])
            high[k] = h
            low[k] = l
            adjoint_block(pos, line, us, h, l, msg)


def forward_part(tab, inc, uraw, nleft, high, low, lraw, other):
    norm_right = jnp.sqrt(sum_rows(inc))
    lraw[...] = jnp.zeros((ROWS * RHS, BS), f32)
    other[...] = jnp.zeros((ROWS * RHS, BS), f32)

    for k in range(COUNT):
        part = forward_block(inc[pl.ds(tab[k], RHS), :], high[k], low[k])
        span = pl.ds(pl.multiple_of(tab[COUNT + k] * RHS, RHS), RHS)
        into = other if k % 2 else lraw
        into[span, :] = into[span, :] + part
    image = lraw[...] + other[...]
    left = image / tiled(norm_right, ROWS) - tiled(norm_right, ROWS) * (
        uraw[...] / tiled(nleft[...], ROWS)
    )
    lraw[...] = left
    return left, norm_right


def user_kernel(tab, inc, uraw, nleft, high, low, msg, lraw, nright, other, us):
    left, norm_right = forward_part(tab, inc, uraw, nleft, high, low, lraw, other)
    nright[...] = norm_right
    msg[...] = jnp.zeros((TALL, BS), f32)
    put_rows(msg, row_of(squares(left)))
    split_left(us, left)

    for k in range(COUNT):
        adjoint_block(tab[k], tab[COUNT + k], us, high[k], low[k], msg)


def last_user_kernel(tab, inc, uraw, nleft, high, low, msg, lraw, nright, other):
    left, norm_right = forward_part(tab, inc, uraw, nleft, high, low, lraw, other)
    nright[...] = norm_right
    msg[...] = jnp.broadcast_to(row_of(squares(left)), msg.shape)


def gather_slots(inc, cols_of, half, parts, copy=None):
    if copy is not None:
        copy.start()
    half[pl.ds(COLS_OWN * RHS, RHS), :] = sum_rows(inc)
    for part in parts:
        part[...] = jnp.zeros((COLS_OWN * RHS, BS), f32)
    if copy is not None:
        copy.wait()

    def step(g, carry):
        for j in range(8):
            o = g * 8 + j
            for s in range(CAP):
                c = cols_of(o, s)
                span = pl.ds(pl.multiple_of(c * RHS, RHS), RHS)
                part = parts[(2 * j + s) % len(parts)]
                part[span, :] = part[span, :] + inc[pl.ds(o * MSG + s * RHS, RHS), :]
        return carry

    lax.fori_loop(0, OWNERS // 8, step, 0)
    half[pl.ds(0, COLS_OWN * RHS), :] = (parts[0][...] + parts[1][...]) + (
        parts[2][...] + parts[3][...]
    )


def first_owner_kernel(inc, half, cols, p0, p1, p2, p3, vcols, scols, sem):
    for o in range(OWNERS):
        vcols[pl.ds(o, 1), :] = inc[pl.ds(MSG * o + MSG - 1, 1), :].astype(jnp.int32)
    copy = pltpu.make_async_copy(vcols, scols, sem)

    def cols_of(o, s):
        c = scols[o, RHS + s]
        cols[o * CAP + s] = c
        return c

    gather_slots(inc, cols_of, half, (p0, p1, p2, p3), copy)


def owner_kernel(cols, inc, half, p0, p1, p2, p3):
    gather_slots(inc, lambda o, s: cols[o * CAP + s], half, (p0, p1, p2, p3))


def send_slots(cols, raw, msg):
    put_rows(msg, row_of(squares(raw[...])))

    def step(g, carry):
        for j in range(8):
            o = g * 8 + j
            for s in range(CAP):
                c = cols[o * CAP + s]
                span = pl.ds(pl.multiple_of(c * RHS, RHS), RHS)
                msg[pl.ds(o * MSG + s * RHS, RHS), :] = raw[span, :]
        return carry

    lax.fori_loop(0, OWNERS // 8, step, 0)


def first_send_kernel(cols, mine, theirs, msg, raw, nleft):
    norm_left = jnp.sqrt(mine[pl.ds(COLS_OWN * RHS, RHS), :] + theirs[pl.ds(COLS_OWN * RHS, RHS), :])
    nleft[...] = norm_left
    body = pl.ds(0, COLS_OWN * RHS)
    raw[...] = (mine[body, :] + theirs[body, :]) / tiled(norm_left, COLS_OWN)
    send_slots(cols, raw, msg)


def send_kernel(first, cols, mine, theirs, qprev, nright, *refs):
    if first:
        start, msg, raw, nleft, sol, search, scal = refs
    else:
        sol_in, search_in, scal_in, msg, raw, nleft, sol, search, scal = refs
    n = COLS_OWN
    norm_left = jnp.sqrt(mine[pl.ds(n * RHS, RHS), :] + theirs[pl.ds(n * RHS, RHS), :])
    norm_right = nright[...]
    nleft[...] = norm_left
    body = pl.ds(0, n * RHS)
    vec = qprev[...] / tiled(norm_right, n)
    raw[...] = (mine[body, :] + theirs[body, :]) / tiled(norm_left, n) - tiled(norm_left, n) * vec
    send_slots(cols, raw, msg)
    if first:
        old_search = vec
        diag_bar = norm_right
        residual = start[...]
        old_sol = jnp.zeros((n * RHS, BS), f32)
    else:
        radius = scal_in[pl.ds(0, RHS), :]
        cosine = scal_in[pl.ds(RHS, RHS), :]
        sine_term = scal_in[pl.ds(2 * RHS, RHS), :]
        residual = scal_in[pl.ds(3 * RHS, RHS), :]
        coupling = sine_term * norm_right
        old_search = vec - tiled(coupling / radius, n) * search_in[...]
        diag_bar = -cosine * norm_right
        old_sol = sol_in[...]
    radius = jnp.sqrt(diag_bar * diag_bar + norm_left * norm_left)
    cosine = diag_bar / radius
    sine_term = norm_left / radius
    sol[...] = old_sol + tiled(cosine * residual / radius, n) * old_search
    search[...] = old_search
    scal[pl.ds(0, RHS), :] = radius
    scal[pl.ds(RHS, RHS), :] = cosine
    scal[pl.ds(2 * RHS, RHS), :] = sine_term
    scal[pl.ds(3 * RHS, RHS), :] = sine_term * residual


def final_kernel(rows, lraw, qprev, nright, sol_in, search_in, scal_in, start, sol, left, rel):
    n = COLS_OWN
    norm_left = jnp.sqrt(column_of(jnp.sum(rows[...], axis=0, keepdims=True)))
    norm_right = nright[...]
    left[...] = lraw[...] / tiled(norm_left, ROWS)
    radius = scal_in[pl.ds(0, RHS), :]
    cosine = scal_in[pl.ds(RHS, RHS), :]
    sine_term = scal_in[pl.ds(2 * RHS, RHS), :]
    residual = scal_in[pl.ds(3 * RHS, RHS), :]
    vec = qprev[...] / tiled(norm_right, n)
    search = vec - tiled(sine_term * norm_right / radius, n) * search_in[...]
    diag_bar = -cosine * norm_right
    radius = jnp.sqrt(diag_bar * diag_bar + norm_left * norm_left)
    cosine = diag_bar / radius
    sine_term = norm_left / radius
    sol[...] = sol_in[...] + tiled(cosine * residual / radius, n) * search
    rel[...] = row_of(sine_term * residual / start[...])[0, :RHS]


def shape(*dims, dtype=f32):
    return jax.ShapeDtypeStruct(dims, dtype)


VMEM = pl.BlockSpec(memory_space=pltpu.VMEM)
SMEM = pl.BlockSpec(memory_space=pltpu.SMEM)
HBM = pl.BlockSpec(memory_space=pltpu.HBM)
ANY = pl.BlockSpec(memory_space=pl.ANY)
PARTS = [pltpu.VMEM((COLS_OWN * RHS, BS), f32)] * 4
LEFTS = pltpu.VMEM((ROWS, 2 * RHS, 2 * BS), bf16)
LEFT = pltpu.VMEM((ROWS * RHS, BS), f32)
ONE = pltpu.SemaphoreType.DMA(())


def call(body, ins, outs, specs_out=None, scratch=()):
    return pl.pallas_call(
        body,
        out_shape=outs,
        in_specs=ins,
        out_specs=specs_out or jax.tree.map(lambda _: VMEM, outs),
        scratch_shapes=scratch,
        compiler_params=pltpu.CompilerParams(vmem_limit_bytes=24 * 1024 * 1024),
    )


def exchange(msg):
    sent = msg.reshape(OWNERS, MSG * BS)
    return lax.all_to_all(sent, SHARD, 0, 0, tiled=True).reshape(TALL, BS)


def swap(half):
    return lax.ppermute(half, "grp", [(0, 1), (1, 0)])


def small(x):
    return pltpu.with_memory_space_constraint(x, pltpu.SMEM)


def on_device(blocks, block_row, block_owner, block_col, right_side):
    owner = block_owner[:, 0]
    right = right_side.reshape(ROWS, BS, RHS).transpose(0, 2, 1).reshape(ROWS * RHS, BS)
    vec = shape(COLS_OWN * RHS, BS)
    col8 = shape(RHS, BS)
    msg_shape = shape(TALL, BS)
    half_shape = shape(COLS_OWN * RHS + RHS, BS)
    table = pltpu.MemorySpace.SMEM((SLOTS,), jnp.int32)
    halves = shape(COUNT, BS, BS, dtype=bf16)

    msg, tab, high, low = call(
        first_kernel,
        [HBM] * 5,
        (msg_shape, table, halves, halves),
        (VMEM, SMEM, VMEM, VMEM),
        [pltpu.VMEM((COUNT, BS, BS), f32), LEFT, LEFTS]
        + [pltpu.SMEM((COUNT,), jnp.int32)] * 4
        + [pltpu.SemaphoreType.DMA((CHUNKS,)), pltpu.SemaphoreType.DMA((4,))],
    )(*(pltpu.with_memory_space_constraint(x, pltpu.HBM) for x in (owner, block_row, block_col, right, blocks)))
    inc = exchange(msg)
    half, cols = call(
        first_owner_kernel,
        [VMEM],
        (half_shape, table),
        (VMEM, SMEM),
        PARTS + [pltpu.VMEM((OWNERS, BS), jnp.int32), pltpu.SMEM((OWNERS, BS), jnp.int32), ONE],
    )(inc)
    msg, raw, norm_left = call(
        first_send_kernel, [SMEM, VMEM, VMEM], (msg_shape, vec, col8)
    )(small(cols), half, swap(half))
    start = norm_left
    left = right
    state = None
    for repeat in range(ITERS):
        inc = exchange(msg)
        if repeat == ITERS - 1:
            break
        msg, left, norm_right = call(
            user_kernel,
            [SMEM] + [VMEM] * 5,
            (msg_shape, vec, col8),
            None,
            [LEFT, LEFTS],
        )(small(tab), inc, left, norm_left, high, low)
        inc = exchange(msg)
        half = call(owner_kernel, [SMEM, VMEM], half_shape, None, PARTS)(small(cols), inc)
        first = repeat == 0
        tail = (start,) if first else state
        outs = call(
            lambda *refs, first=first: send_kernel(first, *refs),
            [SMEM] + [VMEM] * (4 + len(tail)),
            (msg_shape, vec, col8, vec, vec, shape(4 * RHS, BS)),
        )(small(cols), half, swap(half), raw, norm_right, *tail)
        msg, raw, norm_left = outs[:3]
        state = outs[3:]
    rows, left, norm_right = call(
        last_user_kernel,
        [SMEM] + [VMEM] * 5,
        (shape(2 * OWNERS, BS), vec, col8),
        None,
        [LEFT],
    )(small(tab), inc, left, norm_left, high, low)
    rows = lax.all_to_all(rows, GRP_SHARD, 0, 0, tiled=True)
    sol, left, rel = call(
        final_kernel, [VMEM] * 8, (vec, vec, shape(RHS))
    )(rows, left, raw, norm_right, *state, start)

    def tall(x):
        return x.reshape(COLS_OWN, RHS, BS).transpose(0, 2, 1).reshape(COLS_OWN * BS, RHS)

    return tall(sol), tall(left), rel


def solution(mesh):
    torus = Mesh(
        mesh.devices.reshape(mesh.shape["grp"], 4, 4, 4), ("grp", "shard_0", "shard_1", "shard_2")
    )
    return jax.shard_map(
        on_device,
        mesh=torus,
        in_specs=(
            P(GRP_SHARD, None, None),
            P(GRP_SHARD),
            P(GRP_SHARD, None),
            P(GRP_SHARD),
            P(GRP_SHARD, None),
        ),
        out_specs=(P(SHARD, None), P(GRP_SHARD, None), P()),
        check_vma=False,
    )
```

```python
import jax
import jax.numpy as jnp
from jax import lax
from jax.experimental import pallas as pl
from jax.experimental.pallas import tpu as pltpu
from jax.sharding import Mesh
from jax.sharding import PartitionSpec as P

ITERS = 4
COLS_OWN = 16
SHARD = ("shard_0", "shard_1", "shard_2")
GRP_SHARD = ("grp", "shard_0", "shard_1", "shard_2")

OWNERS = 64
CAP = 2
BS = 128
RHS = 8
COUNT = 64
ROWS = 16
SLOTS = OWNERS * CAP
MSG = RHS * CAP + 1
TALL = OWNERS * MSG
CHUNK = 8
CHUNKS = COUNT // CHUNK
PART = RHS // 2
LINES = 2 * ROWS
VEC = COLS_OWN * PART

f32 = jnp.float32
bf16 = jnp.bfloat16


def diag_mask():
    sub = lax.broadcasted_iota(jnp.int32, (RHS, BS), 0)
    lane = lax.broadcasted_iota(jnp.int32, (RHS, BS), 1)
    return sub == lane


def row_of(column):
    return jnp.sum(jnp.where(diag_mask(), column, 0.0), axis=0, keepdims=True)


def column_of(row):
    spread = jnp.broadcast_to(row, (RHS, BS))
    total = jnp.sum(jnp.where(diag_mask(), spread, 0.0), axis=1, keepdims=True)
    return jnp.broadcast_to(total, (RHS, BS))


def squares(values):
    cube = values.reshape(values.shape[0] // RHS, RHS, BS)
    total = jnp.sum(jnp.sum(cube * cube, axis=0), axis=1, keepdims=True)
    return jnp.broadcast_to(total, (RHS, BS))


def part_squares(values):
    cube = values.reshape(values.shape[0] // RHS, RHS, BS)
    total = jnp.sum(cube * cube, axis=0)
    total = total[:PART] + total[PART:]
    total = jnp.sum(jnp.concatenate([total, total], axis=0), axis=1, keepdims=True)
    return jnp.broadcast_to(total, (RHS, BS))


def part_mask(shift):
    sub = lax.broadcasted_iota(jnp.int32, (RHS, BS), 0)
    lane = lax.broadcasted_iota(jnp.int32, (RHS, BS), 1)
    return sub, lane, lane == jnp.where(sub < PART, sub, sub - PART) + shift


def part_row(column, shift=0):
    sub, _, mask = part_mask(shift)
    return jnp.sum(jnp.where(mask & (sub < PART), column, 0.0), axis=0, keepdims=True)


def part_column(row, shift=0):
    _, _, mask = part_mask(shift)
    spread = jnp.broadcast_to(row, (RHS, BS))
    total = jnp.sum(jnp.where(mask, spread, 0.0), axis=1, keepdims=True)
    return jnp.broadcast_to(total, (RHS, BS))


def tiled(column, count):
    return jnp.concatenate([column] * count, axis=0)


def sum_rows(ref, column_of):
    rows = [ref[pl.ds(MSG * o + MSG - 1, 1), :] for o in range(OWNERS)]
    while len(rows) > 1:
        rows = [rows[i] + rows[i + 1] for i in range(0, len(rows), 2)]
    return column_of(rows[0])


def put_rows(ref, row):
    for o in range(OWNERS):
        ref[pl.ds(MSG * o + MSG - 1, 1), :] = row


def split(x):
    high = x.astype(bf16)
    low = (x - high.astype(f32)).astype(bf16)
    return high, low


def stacked(x):
    high = x.astype(bf16).astype(f32)
    both = jnp.concatenate([high, x - high], axis=0).astype(bf16)
    return jnp.concatenate([both, both], axis=1)


def fold(out):
    half = out.shape[0] // 2
    return out[:half] + out[half:]


def chunk_copy(blocks, bbuf, sem, c):
    span = pl.ds(c * CHUNK, CHUNK)
    return pltpu.make_async_copy(blocks.at[span], bbuf.at[span], sem.at[c])


def split_left(us, left, height):
    for r in range(left.shape[0] // height):
        us[r] = stacked(left[r * height : (r + 1) * height])


def adjoint_block(pos, row, us, high, low, msg):
    rhs = jnp.concatenate([high, low], axis=0)
    out = lax.dot_general(us[row], rhs, (((1,), (0,)), ((), ())), preferred_element_type=f32)
    sent = fold(out)
    msg[pl.ds(pos, sent.shape[0]), :] = sent


def forward_block(piece, high, low):
    rhs = jnp.concatenate([high, low], axis=1)
    out = lax.dot_general(
        stacked(piece), rhs, (((1,), (1,)), ((), ())), preferred_element_type=f32
    )
    return fold(out)


def first_kernel(
    owner_in, row_in, col_in, right_in, blocks,
    msg, tab, line_row, high, low,
    bbuf, right, us, owner, row, col, taken, sem, little,
):
    loads = [
        pltpu.make_async_copy(owner_in, owner, little.at[0]),
        pltpu.make_async_copy(row_in, row, little.at[1]),
        pltpu.make_async_copy(col_in, col, little.at[2]),
        pltpu.make_async_copy(right_in, right, little.at[3]),
    ]
    for load in loads:
        load.start()

    def begin(c, carry):
        chunk_copy(blocks, bbuf, sem, c).start()
        return carry

    lax.fori_loop(0, CHUNKS, begin, 0)
    msg[...] = jnp.zeros((TALL, BS), f32)

    def clear(g, carry):
        for j in range(8):
            taken[g * 8 + j] = 0
        return carry

    lax.fori_loop(0, OWNERS // 8, clear, 0)
    for load in loads:
        load.wait()
    right_all = right[...]
    put_rows(msg, row_of(squares(right_all)))
    split_left(us, right_all, RHS)
    grp = lax.axis_index("grp")
    listed = jnp.zeros((1, BS), f32)
    lane = lax.broadcasted_iota(jnp.int32, (1, BS), 1)

    for c in range(CHUNKS):
        chunk_copy(blocks, bbuf, sem, c).wait()
        for k in range(c * CHUNK, (c + 1) * CHUNK):
            o = owner[k]
            rank = taken[o]
            taken[o] = rank + 1
            pos = o * MSG + rank * RHS
            line = lax.rem(row[k], ROWS)
            place = o * MSG + grp * (CAP * PART) + rank * PART
            here = line + grp * ROWS
            tab[k] = place
            tab[COUNT + k] = here
            listed = jnp.where(lane == k, place.astype(f32), listed)
            listed = jnp.where(lane == COUNT + k, here.astype(f32), listed)
            span = pl.ds(o * MSG + MSG - 1, 1)
            msg[span, :] = jnp.where(lane == RHS + rank, col[k].astype(f32), msg[span, :])
            h, l = split(bbuf[k])
            high[k] = h
            low[k] = l
            adjoint_block(pos, line, us, h, l, msg)
    line_row[...] = jnp.broadcast_to(listed, (RHS, BS))


def first_owner_kernel(inc, right, line_row, keep, send, p0, p1, p2, p3, vcols, cols, sem):
    grp = lax.axis_index("grp")
    parts = (p0, p1, p2, p3)
    lane = lax.broadcasted_iota(jnp.int32, (1, BS), 1)
    pairs = [
        jnp.where(
            lane == o * CAP,
            inc[pl.ds(MSG * o + MSG - 1, 1), RHS : RHS + 1],
            jnp.where(lane == o * CAP + 1, inc[pl.ds(MSG * o + MSG - 1, 1), RHS + 1 : RHS + 2], 0.0),
        )
        for o in range(OWNERS)
    ]
    while len(pairs) > 1:
        pairs = [pairs[i] + pairs[i + 1] for i in range(0, len(pairs), 2)]
    vcols[...] = pairs[0][0].astype(jnp.int32)
    copy = pltpu.make_async_copy(vcols, cols, sem)
    copy.start()
    norm = sum_rows(inc, column_of)
    for ref in (keep, send):
        ref[pl.ds(VEC, RHS), :] = norm
        ref[pl.ds(VEC + RHS, 1), :] = pairs[0]
        ref[pl.ds(VEC + RHS + 1, 1), :] = line_row[pl.ds(0, 1), :]
        ref[pl.ds(VEC + RHS + 2, RHS - 2), :] = jnp.zeros((RHS - 2, BS), f32)
    for part in parts:
        part[...] = jnp.zeros((COLS_OWN * RHS, BS), f32)

    def halves(at, tile):
        first, second = tile[:PART], tile[PART:]
        keep[pl.ds(at, PART), :] = jnp.where(grp == 0, first, second)
        send[pl.ds(at, PART), :] = jnp.where(grp == 0, second, first)

    for r in range(ROWS):
        halves(VEC + 2 * RHS + r * PART, right[pl.ds(r * RHS, RHS), :])
    copy.wait()

    def step(g, carry):
        for j in range(8):
            o = g * 8 + j
            for s in range(CAP):
                span = pl.ds(pl.multiple_of(cols[o * CAP + s] * RHS, RHS), RHS)
                part = parts[(2 * j + s) % len(parts)]
                part[span, :] = part[span, :] + inc[pl.ds(o * MSG + s * RHS, RHS), :]
        return carry

    lax.fori_loop(0, OWNERS // 8, step, 0)
    for c in range(COLS_OWN):
        span = pl.ds(c * RHS, RHS)
        halves(c * PART, (p0[span, :] + p1[span, :]) + (p2[span, :] + p3[span, :]))


def send_slots(cols, raw, msg):
    put_rows(msg, part_row(part_squares(raw[...])))

    def step(g, carry):
        for j in range(8):
            o = g * 8 + j
            for s in range(2 * CAP):
                c = cols[s // CAP][o * CAP + s % CAP]
                msg[pl.ds(o * MSG + s * PART, PART), :] = raw[pl.ds(c * PART, PART), :]
        return carry

    lax.fori_loop(0, OWNERS // 8, step, 0)


def first_send_kernel(
    keep, theirs,
    msg, raw, nleft, left, tab, cols0, cols1,
    vtab, vcols0, vcols1, sem,
):
    grp = lax.axis_index("grp")
    mine_cols = keep[pl.ds(VEC + RHS, 1), :]
    other_cols = theirs[pl.ds(VEC + RHS, 1), :]
    vtab[...] = theirs[pl.ds(VEC + RHS + 1, 1), :][0].astype(jnp.int32)
    vcols0[...] = jnp.where(grp == 0, mine_cols, other_cols)[0].astype(jnp.int32)
    vcols1[...] = jnp.where(grp == 0, other_cols, mine_cols)[0].astype(jnp.int32)
    copies = [
        pltpu.make_async_copy(vtab, tab, sem.at[0]),
        pltpu.make_async_copy(vcols0, cols0, sem.at[1]),
        pltpu.make_async_copy(vcols1, cols1, sem.at[2]),
    ]
    for copy in copies:
        copy.start()
    norm = jnp.sqrt(keep[pl.ds(VEC, RHS), :] + theirs[pl.ds(VEC, RHS), :])
    own = jnp.where(grp == 0, norm[:PART], norm[PART:])
    norm = jnp.concatenate([own, own], axis=0)
    nleft[...] = norm
    body = pl.ds(0, VEC)
    raw[...] = (keep[body, :] + theirs[body, :]) / tiled(norm, VEC // RHS)
    size = ROWS * PART
    tail = pl.ds(VEC + 2 * RHS, size)
    left[pl.ds(pl.multiple_of(grp * size, RHS), size), :] = keep[tail, :]
    left[pl.ds(pl.multiple_of((1 - grp) * size, RHS), size), :] = theirs[tail, :]
    for copy in copies:
        copy.wait()
    send_slots((cols0, cols1), raw, msg)


def send_kernel(first, cols0, cols1, inc, qprev, nright, *refs):
    parts = refs[-4:]
    if first:
        start, msg, raw, nleft, sol, search, scal = refs[:-4]
    else:
        sol_in, search_in, scal_in, msg, raw, nleft, sol, search, scal = refs[:-4]
    cols = (cols0, cols1)
    for part in parts:
        part[...] = jnp.zeros((VEC, BS), f32)

    def step(g, carry):
        for j in range(8):
            o = g * 8 + j
            for s in range(2 * CAP):
                span = pl.ds(cols[s // CAP][o * CAP + s % CAP] * PART, PART)
                part = parts[s]
                part[span, :] = part[span, :] + inc[pl.ds(o * MSG + s * PART, PART), :]
        return carry

    lax.fori_loop(0, OWNERS // 8, step, 0)
    total = (parts[0][...] + parts[1][...]) + (parts[2][...] + parts[3][...])
    n = VEC // RHS
    norm_left = jnp.sqrt(sum_rows(inc, part_column))
    norm_right = nright[...]
    nleft[...] = norm_left
    vec = qprev[...] / tiled(norm_right, n)
    raw[...] = total / tiled(norm_left, n) - tiled(norm_left, n) * vec
    send_slots(cols, raw, msg)
    if first:
        old_search = vec
        diag_bar = norm_right
        residual = start[...]
        old_sol = jnp.zeros((VEC, BS), f32)
    else:
        radius = scal_in[pl.ds(0, RHS), :]
        cosine = scal_in[pl.ds(RHS, RHS), :]
        sine_term = scal_in[pl.ds(2 * RHS, RHS), :]
        residual = scal_in[pl.ds(3 * RHS, RHS), :]
        coupling = sine_term * norm_right
        old_search = vec - tiled(coupling / radius, n) * search_in[...]
        diag_bar = -cosine * norm_right
        old_sol = sol_in[...]
    radius = jnp.sqrt(diag_bar * diag_bar + norm_left * norm_left)
    cosine = diag_bar / radius
    sine_term = norm_left / radius
    sol[...] = old_sol + tiled(cosine * residual / radius, n) * old_search
    search[...] = old_search
    scal[pl.ds(0, RHS), :] = radius
    scal[pl.ds(RHS, RHS), :] = cosine
    scal[pl.ds(2 * RHS, RHS), :] = sine_term
    scal[pl.ds(3 * RHS, RHS), :] = sine_term * residual


def forward_all(tab, inc, high, low, into):
    for k in range(COUNT):
        part = forward_block(inc[pl.ds(tab[k], PART), :], high[k], low[k])
        span = pl.ds(tab[COUNT + k] * PART, PART)
        ref = into[k % 2]
        ref[span, :] = ref[span, :] + part


def adjoint_all(tab, us, high, low, msg):
    for k in range(COUNT):
        adjoint_block(tab[k], tab[COUNT + k], us, high[k], low[k], msg)


def left_of(lraw, other, uraw, nleft, norm_right):
    n = LINES * PART // RHS
    left = (lraw[...] + other[...]) / tiled(norm_right, n) - tiled(norm_right, n) * (
        uraw[...] / tiled(nleft[...], n)
    )
    lraw[...] = left
    return left


def first_user_kernel(
    tab, tab2, inc, uraw, nleft, high, low, blocks,
    msg, lraw, nright, high2, low2,
    other, us, bbuf, sem,
):
    for c in range(CHUNKS):
        chunk_copy(blocks, bbuf, sem, c).start()
    norm_right = jnp.sqrt(sum_rows(inc, part_column))
    nright[...] = norm_right
    lraw[...] = jnp.zeros(lraw.shape, f32)
    other[...] = jnp.zeros(lraw.shape, f32)
    forward_all(tab, inc, high, low, (lraw, other))
    for c in range(CHUNKS):
        chunk_copy(blocks, bbuf, sem, c).wait()
        for k in range(c * CHUNK, (c + 1) * CHUNK):
            h, l = split(bbuf[k])
            high2[k] = h
            low2[k] = l
            part = forward_block(inc[pl.ds(tab2[k], PART), :], h, l)
            span = pl.ds(tab2[COUNT + k] * PART, PART)
            ref = other if k % 2 else lraw
            ref[span, :] = ref[span, :] + part
    left = left_of(lraw, other, uraw, nleft, norm_right)
    msg[...] = jnp.zeros((TALL, BS), f32)
    put_rows(msg, part_row(part_squares(left)))
    split_left(us, left, PART)
    adjoint_all(tab, us, high, low, msg)
    adjoint_all(tab2, us, high2, low2, msg)


def user_kernel(
    tab, tab2, inc, uraw, nleft, high, low, high2, low2, msg, lraw, nright, other, us
):
    norm_right = jnp.sqrt(sum_rows(inc, part_column))
    nright[...] = norm_right
    lraw[...] = jnp.zeros(lraw.shape, f32)
    other[...] = jnp.zeros(lraw.shape, f32)
    forward_all(tab, inc, high, low, (lraw, other))
    forward_all(tab2, inc, high2, low2, (lraw, other))
    left = left_of(lraw, other, uraw, nleft, norm_right)
    msg[...] = jnp.zeros((TALL, BS), f32)
    put_rows(msg, part_row(part_squares(left)))
    split_left(us, left, PART)
    adjoint_all(tab, us, high, low, msg)
    adjoint_all(tab2, us, high2, low2, msg)


def last_user_kernel(
    tab, tab2, inc, uraw, nleft, high, low, high2, low2, msg, lraw, nright, other
):
    norm_right = jnp.sqrt(sum_rows(inc, part_column))
    nright[...] = norm_right
    lraw[...] = jnp.zeros(lraw.shape, f32)
    other[...] = jnp.zeros(lraw.shape, f32)
    forward_all(tab, inc, high, low, (lraw, other))
    forward_all(tab2, inc, high2, low2, (lraw, other))
    left = left_of(lraw, other, uraw, nleft, norm_right)
    row = part_row(part_squares(left), lax.axis_index("grp") * PART)
    msg[...] = jnp.broadcast_to(row, msg.shape)


def final_kernel(rows, lraw, qprev, nright, sol_in, search_in, scal_in, start, keep, send):
    grp = lax.axis_index("grp")
    total = jnp.sum(rows[...], axis=0, keepdims=True)
    norm_left = jnp.sqrt(part_column(total, grp * PART))
    norm_right = nright[...]
    size = ROWS * PART
    n = size // RHS
    for ref, at in ((keep, grp), (send, 1 - grp)):
        left = lraw[pl.ds(pl.multiple_of(at * size, RHS), size), :] / tiled(norm_left, n)
        ref[pl.ds(VEC + RHS, size), :] = left
    n = VEC // RHS
    radius = scal_in[pl.ds(0, RHS), :]
    cosine = scal_in[pl.ds(RHS, RHS), :]
    sine_term = scal_in[pl.ds(2 * RHS, RHS), :]
    residual = scal_in[pl.ds(3 * RHS, RHS), :]
    vec = qprev[...] / tiled(norm_right, n)
    search = vec - tiled(sine_term * norm_right / radius, n) * search_in[...]
    diag_bar = -cosine * norm_right
    radius = jnp.sqrt(diag_bar * diag_bar + norm_left * norm_left)
    cosine = diag_bar / radius
    sine_term = norm_left / radius
    sol = sol_in[...] + tiled(cosine * residual / radius, n) * search
    rel = sine_term * residual / start[...]
    for ref in (keep, send):
        ref[pl.ds(0, VEC), :] = sol
        ref[pl.ds(VEC, RHS), :] = rel


def join_kernel(keep, theirs, sol, left, rel):
    grp = lax.axis_index("grp")

    def joined(at):
        mine = keep[pl.ds(at, PART), :]
        other = theirs[pl.ds(at, PART), :]
        first = jnp.where(grp == 0, mine, other)
        second = jnp.where(grp == 0, other, mine)
        return jnp.concatenate([first, second], axis=0)

    for c in range(COLS_OWN):
        sol[pl.ds(c * RHS, RHS), :] = joined(c * PART)
    for r in range(ROWS):
        left[pl.ds(r * RHS, RHS), :] = joined(VEC + RHS + r * PART)
    rel[...] = row_of(joined(VEC))[0, :RHS]


def shape(*dims, dtype=f32):
    return jax.ShapeDtypeStruct(dims, dtype)


VMEM = pl.BlockSpec(memory_space=pltpu.VMEM)
SMEM = pl.BlockSpec(memory_space=pltpu.SMEM)
HBM = pl.BlockSpec(memory_space=pltpu.HBM)
PARTS = [pltpu.VMEM((COLS_OWN * RHS, BS), f32)] * 4
LEFTS = pltpu.VMEM((ROWS, 2 * RHS, 2 * BS), bf16)
LEFTS2 = pltpu.VMEM((LINES, RHS, 2 * BS), bf16)
LEFT = pltpu.VMEM((ROWS * RHS, BS), f32)
BUFFER = pltpu.VMEM((COUNT, BS, BS), f32)
SEMS = pltpu.SemaphoreType.DMA((CHUNKS,))
ONE = pltpu.SemaphoreType.DMA(())
LINE = pltpu.VMEM((SLOTS,), jnp.int32)


def call(body, ins, outs, specs_out=None, scratch=()):
    return pl.pallas_call(
        body,
        out_shape=outs,
        in_specs=ins,
        out_specs=specs_out or jax.tree.map(lambda _: VMEM, outs),
        scratch_shapes=scratch,
        compiler_params=pltpu.CompilerParams(vmem_limit_bytes=24 * 1024 * 1024),
    )


def exchange(msg):
    sent = msg.reshape(OWNERS, MSG * BS)
    return lax.all_to_all(sent, SHARD, 0, 0, tiled=True).reshape(TALL, BS)


def swap(half):
    return lax.ppermute(half, "grp", [(0, 1), (1, 0)])


def small(*xs):
    return [pltpu.with_memory_space_constraint(x, pltpu.SMEM) for x in xs]


def near(*xs):
    return [pltpu.with_memory_space_constraint(x, pltpu.VMEM) for x in xs]


def far(*xs):
    return [pltpu.with_memory_space_constraint(x, pltpu.HBM) for x in xs]


def on_device(blocks, block_row, block_owner, block_col, right_side):
    owner = block_owner[:, 0]
    right = right_side.reshape(ROWS, BS, RHS).transpose(0, 2, 1).reshape(ROWS * RHS, BS)
    left_shape = shape(LINES * PART, BS)
    vec = shape(VEC, BS)
    col8 = shape(RHS, BS)
    msg_shape = shape(TALL, BS)
    table = pltpu.MemorySpace.SMEM((SLOTS,), jnp.int32)
    terms = pltpu.MemorySpace.VMEM((COUNT, BS, BS), bf16)
    swapped = shape(VEC + 2 * RHS + ROWS * PART, BS)

    blocks2 = swap(blocks)
    msg, tab, line_row, high, low = call(
        first_kernel,
        [HBM] * 5,
        (msg_shape, table, col8, terms, terms),
        (VMEM, SMEM, VMEM, VMEM, VMEM),
        [BUFFER, LEFT, LEFTS]
        + [pltpu.SMEM((COUNT,), jnp.int32)] * 4
        + [SEMS, pltpu.SemaphoreType.DMA((4,))],
    )(*far(owner, block_row, block_col, right, blocks))
    inc = exchange(msg)
    keep, send = call(
        first_owner_kernel,
        [VMEM] * 3,
        (swapped, swapped),
        None,
        PARTS + [LINE, pltpu.SMEM((SLOTS,), jnp.int32), ONE],
    )(inc, right, line_row)
    msg, raw, norm_left, left, tab2, cols0, cols1 = call(
        first_send_kernel,
        [VMEM] * 2,
        (msg_shape, vec, col8, left_shape, table, table, table),
        (VMEM,) * 4 + (SMEM,) * 3,
        [LINE] * 3 + [pltpu.SemaphoreType.DMA((3,))],
    )(keep, swap(send))
    start = norm_left
    state = None
    for repeat in range(ITERS):
        inc = exchange(msg)
        if repeat == ITERS - 1:
            break
        if repeat == 0:
            msg, left, norm_right, high2, low2 = call(
                first_user_kernel,
                [SMEM] * 2 + [VMEM] * 5 + [HBM],
                (msg_shape, left_shape, col8, terms, terms),
                (VMEM,) * 5,
                [LEFT, LEFTS2, BUFFER, SEMS],
            )(*small(tab, tab2), inc, left, norm_left, *near(high, low), *far(blocks2))
        else:
            msg, left, norm_right = call(
                user_kernel,
                [SMEM] * 2 + [VMEM] * 7,
                (msg_shape, left_shape, col8),
                None,
                [LEFT, LEFTS2],
            )(*small(tab, tab2), inc, left, norm_left, *near(high, low, high2, low2))
        inc = exchange(msg)
        first = repeat == 0
        tail = (start,) if first else state
        outs = call(
            lambda *refs, first=first: send_kernel(first, *refs),
            [SMEM] * 2 + [VMEM] * (3 + len(tail)),
            (msg_shape, vec, col8, vec, vec, shape(4 * RHS, BS)),
            None,
            [pltpu.VMEM((VEC, BS), f32)] * 4,
        )(*small(cols0, cols1), inc, raw, norm_right, *tail)
        msg, raw, norm_left = outs[:3]
        state = outs[3:]
    rows, left, norm_right = call(
        last_user_kernel,
        [SMEM] * 2 + [VMEM] * 7,
        (shape(2 * OWNERS, BS), left_shape, col8),
        None,
        [LEFT],
    )(*small(tab, tab2), inc, left, norm_left, *near(high, low, high2, low2))
    rows = lax.all_to_all(rows, GRP_SHARD, 0, 0, tiled=True)
    ends = shape(VEC + RHS + ROWS * PART, BS)
    keep, send = call(final_kernel, [VMEM] * 8, (ends, ends))(
        rows, left, raw, norm_right, *state, start
    )
    full = shape(COLS_OWN * RHS, BS)
    sol, left, rel = call(join_kernel, [VMEM] * 2, (full, full, shape(RHS)))(keep, swap(send))

    def tall(x):
        return x.reshape(COLS_OWN, RHS, BS).transpose(0, 2, 1).reshape(COLS_OWN * BS, RHS)

    return tall(sol), tall(left), rel


def solution(mesh):
    torus = Mesh(
        mesh.devices.reshape(mesh.shape["grp"], 4, 4, 4), ("grp", "shard_0", "shard_1", "shard_2")
    )
    return jax.shard_map(
        on_device,
        mesh=torus,
        in_specs=(
            P(GRP_SHARD, None, None),
            P(GRP_SHARD),
            P(GRP_SHARD, None),
            P(GRP_SHARD),
            P(GRP_SHARD, None),
        ),
        out_specs=(P(SHARD, None), P(GRP_SHARD, None), P()),
        check_vma=False,
    )
```

```python
import jax
import jax.numpy as jnp
from jax import lax
from jax.experimental import pallas as pl
from jax.experimental.pallas import tpu as pltpu
from jax.sharding import Mesh
from jax.sharding import PartitionSpec as P

ITERS = 4
COLS_OWN = 16
SHARD = ("shard_0", "shard_1", "shard_2")
GRP_SHARD = ("grp", "shard_0", "shard_1", "shard_2")

OWNERS = 64
CAP = 2
BS = 128
RHS = 8
COUNT = 64
ROWS = 16
SLOTS = OWNERS * CAP
MSG = RHS * CAP + 1
TALL = OWNERS * MSG
CHUNK = 8
CHUNKS = COUNT // CHUNK
PART = RHS // 2
LINES = 2 * ROWS
VEC = COLS_OWN * PART
ENDS = 2 * VEC + 3 * RHS + ROWS * PART

f32 = jnp.float32
bf16 = jnp.bfloat16


def diag_mask():
    sub = lax.broadcasted_iota(jnp.int32, (RHS, BS), 0)
    lane = lax.broadcasted_iota(jnp.int32, (RHS, BS), 1)
    return sub == lane


def row_of(column):
    return jnp.sum(jnp.where(diag_mask(), column, 0.0), axis=0, keepdims=True)


def column_of(row):
    spread = jnp.broadcast_to(row, (RHS, BS))
    total = jnp.sum(jnp.where(diag_mask(), spread, 0.0), axis=1, keepdims=True)
    return jnp.broadcast_to(total, (RHS, BS))


def squares(values):
    cube = values.reshape(values.shape[0] // RHS, RHS, BS)
    total = jnp.sum(jnp.sum(cube * cube, axis=0), axis=1, keepdims=True)
    return jnp.broadcast_to(total, (RHS, BS))


def part_squares(values):
    cube = values.reshape(values.shape[0] // RHS, RHS, BS)
    total = jnp.sum(cube * cube, axis=0)
    total = total[:PART] + total[PART:]
    total = jnp.sum(jnp.concatenate([total, total], axis=0), axis=1, keepdims=True)
    return jnp.broadcast_to(total, (RHS, BS))


def part_mask(shift):
    sub = lax.broadcasted_iota(jnp.int32, (RHS, BS), 0)
    lane = lax.broadcasted_iota(jnp.int32, (RHS, BS), 1)
    return sub, lane, lane == jnp.where(sub < PART, sub, sub - PART) + shift


def part_row(column, shift=0):
    sub, _, mask = part_mask(shift)
    return jnp.sum(jnp.where(mask & (sub < PART), column, 0.0), axis=0, keepdims=True)


def part_column(row, shift=0):
    _, _, mask = part_mask(shift)
    spread = jnp.broadcast_to(row, (RHS, BS))
    total = jnp.sum(jnp.where(mask, spread, 0.0), axis=1, keepdims=True)
    return jnp.broadcast_to(total, (RHS, BS))


def tiled(column, count):
    return jnp.concatenate([column] * count, axis=0)


def sum_rows(ref, column_of):
    rows = [ref[pl.ds(MSG * o + MSG - 1, 1), :] for o in range(OWNERS)]
    while len(rows) > 1:
        rows = [rows[i] + rows[i + 1] for i in range(0, len(rows), 2)]
    return column_of(rows[0])


def put_rows(ref, row):
    for o in range(OWNERS):
        ref[pl.ds(MSG * o + MSG - 1, 1), :] = row


def split(x):
    high = x.astype(bf16)
    low = (x - high.astype(f32)).astype(bf16)
    return high, low


def stacked(x):
    high = x.astype(bf16).astype(f32)
    both = jnp.concatenate([high, x - high], axis=0).astype(bf16)
    return jnp.concatenate([both, both], axis=1)


def fold(out):
    half = out.shape[0] // 2
    return out[:half] + out[half:]


def chunk_copy(blocks, bbuf, sem, c):
    span = pl.ds(c * CHUNK, CHUNK)
    return pltpu.make_async_copy(blocks.at[span], bbuf.at[span], sem.at[c])


def split_left(us, left, height):
    for r in range(left.shape[0] // height):
        us[r] = stacked(left[r * height : (r + 1) * height])


def adjoint_block(pos, row, us, high, low, msg):
    rhs = jnp.concatenate([high, low], axis=0)
    out = lax.dot_general(us[row], rhs, (((1,), (0,)), ((), ())), preferred_element_type=f32)
    sent = fold(out)
    msg[pl.ds(pos, sent.shape[0]), :] = sent


def forward_block(piece, high, low):
    rhs = jnp.concatenate([high, low], axis=1)
    out = lax.dot_general(
        stacked(piece), rhs, (((1,), (1,)), ((), ())), preferred_element_type=f32
    )
    return fold(out)


def first_kernel(
    owner_in, row_in, col_in, right_in, blocks,
    msg, tab, line_row, high, low,
    bbuf, right, us, owner, row, col, taken, sem, little,
):
    loads = [
        pltpu.make_async_copy(owner_in, owner, little.at[0]),
        pltpu.make_async_copy(row_in, row, little.at[1]),
        pltpu.make_async_copy(col_in, col, little.at[2]),
        pltpu.make_async_copy(right_in, right, little.at[3]),
    ]
    for load in loads:
        load.start()

    def begin(c, carry):
        chunk_copy(blocks, bbuf, sem, c).start()
        return carry

    lax.fori_loop(0, CHUNKS, begin, 0)
    msg[...] = jnp.zeros((TALL, BS), f32)

    def clear(g, carry):
        for j in range(8):
            taken[g * 8 + j] = 0
        return carry

    lax.fori_loop(0, OWNERS // 8, clear, 0)
    for load in loads:
        load.wait()
    right_all = right[...]
    put_rows(msg, row_of(squares(right_all)))
    split_left(us, right_all, RHS)
    grp = lax.axis_index("grp")
    listed = jnp.zeros((1, BS), f32)
    lane = lax.broadcasted_iota(jnp.int32, (1, BS), 1)

    for c in range(CHUNKS):
        chunk_copy(blocks, bbuf, sem, c).wait()
        for k in range(c * CHUNK, (c + 1) * CHUNK):
            o = owner[k]
            rank = taken[o]
            taken[o] = rank + 1
            pos = o * MSG + rank * RHS
            line = lax.rem(row[k], ROWS)
            place = o * MSG + grp * (CAP * PART) + rank * PART
            here = line + grp * ROWS
            tab[k] = place
            tab[COUNT + k] = here
            listed = jnp.where(lane == k, place.astype(f32), listed)
            listed = jnp.where(lane == COUNT + k, here.astype(f32), listed)
            span = pl.ds(o * MSG + MSG - 1, 1)
            msg[span, :] = jnp.where(lane == RHS + rank, col[k].astype(f32), msg[span, :])
            h, l = split(bbuf[k])
            high[k] = h
            low[k] = l
            adjoint_block(pos, line, us, h, l, msg)
    line_row[...] = jnp.broadcast_to(listed, (RHS, BS))


def first_owner_kernel(inc, right, line_row, keep, send, p0, p1, p2, p3, vcols, cols, sem):
    grp = lax.axis_index("grp")
    parts = (p0, p1, p2, p3)
    lane = lax.broadcasted_iota(jnp.int32, (1, BS), 1)
    pairs = [
        jnp.where(
            lane == o * CAP,
            inc[pl.ds(MSG * o + MSG - 1, 1), RHS : RHS + 1],
            jnp.where(lane == o * CAP + 1, inc[pl.ds(MSG * o + MSG - 1, 1), RHS + 1 : RHS + 2], 0.0),
        )
        for o in range(OWNERS)
    ]
    while len(pairs) > 1:
        pairs = [pairs[i] + pairs[i + 1] for i in range(0, len(pairs), 2)]
    vcols[...] = pairs[0][0].astype(jnp.int32)
    copy = pltpu.make_async_copy(vcols, cols, sem)
    copy.start()
    norm = sum_rows(inc, column_of)
    for ref in (keep, send):
        ref[pl.ds(VEC, RHS), :] = norm
        ref[pl.ds(VEC + RHS, 1), :] = pairs[0]
        ref[pl.ds(VEC + RHS + 1, 1), :] = line_row[pl.ds(0, 1), :]
        ref[pl.ds(VEC + RHS + 2, RHS - 2), :] = jnp.zeros((RHS - 2, BS), f32)
    for part in parts:
        part[...] = jnp.zeros((COLS_OWN * RHS, BS), f32)

    def halves(at, tile):
        first, second = tile[:PART], tile[PART:]
        keep[pl.ds(at, PART), :] = jnp.where(grp == 0, first, second)
        send[pl.ds(at, PART), :] = jnp.where(grp == 0, second, first)

    for r in range(ROWS):
        halves(VEC + 2 * RHS + r * PART, right[pl.ds(r * RHS, RHS), :])
    copy.wait()

    def step(g, carry):
        for j in range(8):
            o = g * 8 + j
            for s in range(CAP):
                span = pl.ds(pl.multiple_of(cols[o * CAP + s] * RHS, RHS), RHS)
                part = parts[(2 * j + s) % len(parts)]
                part[span, :] = part[span, :] + inc[pl.ds(o * MSG + s * RHS, RHS), :]
        return carry

    lax.fori_loop(0, OWNERS // 8, step, 0)
    for c in range(COLS_OWN):
        span = pl.ds(c * RHS, RHS)
        halves(c * PART, (p0[span, :] + p1[span, :]) + (p2[span, :] + p3[span, :]))


def send_slots(cols, raw, msg):
    put_rows(msg, part_row(part_squares(raw[...])))
    for o in range(OWNERS):
        for s in range(2 * CAP):
            at = cols[s // CAP][o * CAP + s % CAP]
            msg[pl.ds(o * MSG + s * PART, PART), :] = raw[pl.ds(at, PART), :]


def first_send_kernel(
    keep, theirs,
    msg, raw, nleft, left, tab, cols0, cols1,
    vtab, vcols0, vcols1, sem,
):
    grp = lax.axis_index("grp")
    mine_cols = keep[pl.ds(VEC + RHS, 1), :]
    other_cols = theirs[pl.ds(VEC + RHS, 1), :]
    vtab[...] = theirs[pl.ds(VEC + RHS + 1, 1), :][0].astype(jnp.int32)
    vcols0[...] = jnp.where(grp == 0, mine_cols, other_cols)[0].astype(jnp.int32) * PART
    vcols1[...] = jnp.where(grp == 0, other_cols, mine_cols)[0].astype(jnp.int32) * PART
    copies = [
        pltpu.make_async_copy(vtab, tab, sem.at[0]),
        pltpu.make_async_copy(vcols0, cols0, sem.at[1]),
        pltpu.make_async_copy(vcols1, cols1, sem.at[2]),
    ]
    for copy in copies:
        copy.start()
    norm = jnp.sqrt(keep[pl.ds(VEC, RHS), :] + theirs[pl.ds(VEC, RHS), :])
    own = jnp.where(grp == 0, norm[:PART], norm[PART:])
    norm = jnp.concatenate([own, own], axis=0)
    nleft[...] = norm
    body = pl.ds(0, VEC)
    raw[...] = (keep[body, :] + theirs[body, :]) / tiled(norm, VEC // RHS)
    size = ROWS * PART
    tail = pl.ds(VEC + 2 * RHS, size)
    left[pl.ds(pl.multiple_of(grp * size, RHS), size), :] = keep[tail, :]
    left[pl.ds(pl.multiple_of((1 - grp) * size, RHS), size), :] = theirs[tail, :]
    for copy in copies:
        copy.wait()
    send_slots((cols0, cols1), raw, msg)


def send_kernel(first, cols0, cols1, inc, qprev, nright, *refs):
    parts = refs[-4:]
    if first:
        start, msg, raw, nleft, sol, search, scal = refs[:-4]
    else:
        sol_in, search_in, scal_in, msg, raw, nleft, sol, search, scal = refs[:-4]
    cols = (cols0, cols1)
    for part in parts:
        part[...] = jnp.zeros((VEC, BS), f32)

    for o in range(OWNERS):
        for s in range(2 * CAP):
            span = pl.ds(cols[s // CAP][o * CAP + s % CAP], PART)
            part = parts[s]
            part[span, :] = part[span, :] + inc[pl.ds(o * MSG + s * PART, PART), :]
    total = (parts[0][...] + parts[1][...]) + (parts[2][...] + parts[3][...])
    n = VEC // RHS
    norm_left = jnp.sqrt(sum_rows(inc, part_column))
    norm_right = nright[...]
    nleft[...] = norm_left
    vec = qprev[...] / tiled(norm_right, n)
    raw[...] = total / tiled(norm_left, n) - tiled(norm_left, n) * vec
    send_slots(cols, raw, msg)
    if first:
        old_search = vec
        diag_bar = norm_right
        residual = start[...]
        old_sol = jnp.zeros((VEC, BS), f32)
    else:
        radius = scal_in[pl.ds(0, RHS), :]
        cosine = scal_in[pl.ds(RHS, RHS), :]
        sine_term = scal_in[pl.ds(2 * RHS, RHS), :]
        residual = scal_in[pl.ds(3 * RHS, RHS), :]
        coupling = sine_term * norm_right
        old_search = vec - tiled(coupling / radius, n) * search_in[...]
        diag_bar = -cosine * norm_right
        old_sol = sol_in[...]
    radius = jnp.sqrt(diag_bar * diag_bar + norm_left * norm_left)
    cosine = diag_bar / radius
    sine_term = norm_left / radius
    sol[...] = old_sol + tiled(cosine * residual / radius, n) * old_search
    search[...] = old_search
    scal[pl.ds(0, RHS), :] = radius
    scal[pl.ds(RHS, RHS), :] = cosine
    scal[pl.ds(2 * RHS, RHS), :] = sine_term
    scal[pl.ds(3 * RHS, RHS), :] = sine_term * residual


def forward_all(tab, inc, high, low, into):
    for k in range(COUNT):
        part = forward_block(inc[pl.ds(tab[k], PART), :], high[k], low[k])
        span = pl.ds(tab[COUNT + k] * PART, PART)
        ref = into[k % 2]
        ref[span, :] = ref[span, :] + part


def adjoint_all(tab, us, high, low, msg):
    for k in range(COUNT):
        adjoint_block(tab[k], tab[COUNT + k], us, high[k], low[k], msg)


def left_of(lraw, other, uraw, nleft, norm_right):
    n = LINES * PART // RHS
    left = (lraw[...] + other[...]) / tiled(norm_right, n) - tiled(norm_right, n) * (
        uraw[...] / tiled(nleft[...], n)
    )
    lraw[...] = left
    return left


def first_user_kernel(
    tab, tab2, inc, uraw, nleft, high, low, blocks,
    msg, lraw, nright, high2, low2,
    other, us,
):
    norm_right = jnp.sqrt(sum_rows(inc, part_column))
    nright[...] = norm_right
    lraw[...] = jnp.zeros(lraw.shape, f32)
    other[...] = jnp.zeros(lraw.shape, f32)
    forward_all(tab, inc, high, low, (lraw, other))
    for k in range(COUNT):
        h, l = split(blocks[k])
        high2[k] = h
        low2[k] = l
        part = forward_block(inc[pl.ds(tab2[k], PART), :], h, l)
        span = pl.ds(tab2[COUNT + k] * PART, PART)
        ref = other if k % 2 else lraw
        ref[span, :] = ref[span, :] + part
    left = left_of(lraw, other, uraw, nleft, norm_right)
    msg[...] = jnp.zeros((TALL, BS), f32)
    put_rows(msg, part_row(part_squares(left)))
    split_left(us, left, PART)
    adjoint_all(tab, us, high, low, msg)
    adjoint_all(tab2, us, high2, low2, msg)


def user_kernel(
    tab, tab2, inc, uraw, nleft, high, low, high2, low2, msg, lraw, nright, other, us
):
    norm_right = jnp.sqrt(sum_rows(inc, part_column))
    nright[...] = norm_right
    lraw[...] = jnp.zeros(lraw.shape, f32)
    other[...] = jnp.zeros(lraw.shape, f32)
    forward_all(tab, inc, high, low, (lraw, other))
    forward_all(tab2, inc, high2, low2, (lraw, other))
    left = left_of(lraw, other, uraw, nleft, norm_right)
    msg[...] = jnp.zeros((TALL, BS), f32)
    put_rows(msg, part_row(part_squares(left)))
    split_left(us, left, PART)
    adjoint_all(tab, us, high, low, msg)
    adjoint_all(tab2, us, high2, low2, msg)


def last_user_kernel(
    tab, tab2, inc, uraw, nleft, high, low, high2, low2, qprev, start, sol_in, search_in, scal_in,
    msg, keep, send, lraw, other,
):
    grp = lax.axis_index("grp")
    norm_right = jnp.sqrt(sum_rows(inc, part_column))
    lraw[...] = jnp.zeros(lraw.shape, f32)
    other[...] = jnp.zeros(lraw.shape, f32)
    n = VEC // RHS
    radius = scal_in[pl.ds(0, RHS), :]
    cosine = scal_in[pl.ds(RHS, RHS), :]
    sine_term = scal_in[pl.ds(2 * RHS, RHS), :]
    vec = qprev[...] / tiled(norm_right, n)
    search = vec - tiled(sine_term * norm_right / radius, n) * search_in[...]
    for ref in (keep, send):
        ref[pl.ds(0, VEC), :] = sol_in[...]
        ref[pl.ds(VEC, VEC), :] = search
        ref[pl.ds(2 * VEC, RHS), :] = -cosine * norm_right
        ref[pl.ds(2 * VEC + RHS, RHS), :] = scal_in[pl.ds(3 * RHS, RHS), :]
        ref[pl.ds(2 * VEC + 2 * RHS, RHS), :] = start[...]
    forward_all(tab, inc, high, low, (lraw, other))
    forward_all(tab2, inc, high2, low2, (lraw, other))
    left = left_of(lraw, other, uraw, nleft, norm_right)
    row = part_row(part_squares(left), grp * PART)
    msg[...] = jnp.broadcast_to(row, msg.shape)
    size = ROWS * PART
    for ref, at in ((keep, grp), (send, 1 - grp)):
        ref[pl.ds(ENDS - size, size), :] = lraw[pl.ds(pl.multiple_of(at * size, RHS), size), :]


def finished(total, ref, grp):
    norm_left = jnp.sqrt(part_column(total, grp * PART))
    size = ROWS * PART
    left = ref[pl.ds(ENDS - size, size), :] / tiled(norm_left, size // RHS)
    diag_bar = ref[pl.ds(2 * VEC, RHS), :]
    residual = ref[pl.ds(2 * VEC + RHS, RHS), :]
    radius = jnp.sqrt(diag_bar * diag_bar + norm_left * norm_left)
    cosine = diag_bar / radius
    sine_term = norm_left / radius
    step = tiled(cosine * residual / radius, VEC // RHS)
    sol = ref[pl.ds(0, VEC), :] + step * ref[pl.ds(VEC, VEC), :]
    rel = sine_term * residual / ref[pl.ds(2 * VEC + 2 * RHS, RHS), :]
    return sol, left, rel


def final_kernel(rows, keep, theirs, sol, left, rel):
    grp = lax.axis_index("grp")
    total = jnp.sum(rows[...], axis=0, keepdims=True)
    mine = finished(total, keep, grp)
    other = finished(total, theirs, 1 - grp)

    def join(ref, mine, other):
        first = jnp.where(grp == 0, mine, other)
        second = jnp.where(grp == 0, other, mine)
        for c in range(mine.shape[0] // PART):
            ref[pl.ds(c * RHS, PART), :] = first[c * PART : (c + 1) * PART]
            ref[pl.ds(c * RHS + PART, PART), :] = second[c * PART : (c + 1) * PART]

    join(sol, mine[0], other[0])
    join(left, mine[1], other[1])
    first = jnp.where(grp == 0, mine[2], other[2])
    second = jnp.where(grp == 0, other[2], mine[2])
    both = jnp.concatenate([first[:PART], second[:PART]], axis=0)
    rel[...] = row_of(both)[0, :RHS]


def shape(*dims, dtype=f32):
    return jax.ShapeDtypeStruct(dims, dtype)


VMEM = pl.BlockSpec(memory_space=pltpu.VMEM)
SMEM = pl.BlockSpec(memory_space=pltpu.SMEM)
HBM = pl.BlockSpec(memory_space=pltpu.HBM)
PARTS = [pltpu.VMEM((COLS_OWN * RHS, BS), f32)] * 4
LEFTS = pltpu.VMEM((ROWS, 2 * RHS, 2 * BS), bf16)
LEFTS2 = pltpu.VMEM((LINES, RHS, 2 * BS), bf16)
LEFT = pltpu.VMEM((ROWS * RHS, BS), f32)
BUFFER = pltpu.VMEM((COUNT, BS, BS), f32)
SEMS = pltpu.SemaphoreType.DMA((CHUNKS,))
ONE = pltpu.SemaphoreType.DMA(())
LINE = pltpu.VMEM((SLOTS,), jnp.int32)


def call(body, ins, outs, specs_out=None, scratch=()):
    return pl.pallas_call(
        body,
        out_shape=outs,
        in_specs=ins,
        out_specs=specs_out or jax.tree.map(lambda _: VMEM, outs),
        scratch_shapes=scratch,
        compiler_params=pltpu.CompilerParams(vmem_limit_bytes=24 * 1024 * 1024),
    )


def exchange(msg):
    sent = msg.reshape(OWNERS, MSG * BS)
    return lax.all_to_all(sent, SHARD, 0, 0, tiled=True).reshape(TALL, BS)


def swap(half):
    return lax.ppermute(half, "grp", [(0, 1), (1, 0)])


def small(*xs):
    return [pltpu.with_memory_space_constraint(x, pltpu.SMEM) for x in xs]


def near(*xs):
    return [pltpu.with_memory_space_constraint(x, pltpu.VMEM) for x in xs]


def far(*xs):
    return [pltpu.with_memory_space_constraint(x, pltpu.HBM) for x in xs]


def on_device(blocks, block_row, block_owner, block_col, right_side):
    owner = block_owner[:, 0]
    right = right_side.reshape(ROWS, BS, RHS).transpose(0, 2, 1).reshape(ROWS * RHS, BS)
    left_shape = shape(LINES * PART, BS)
    vec = shape(VEC, BS)
    col8 = shape(RHS, BS)
    msg_shape = shape(TALL, BS)
    table = pltpu.MemorySpace.SMEM((SLOTS,), jnp.int32)
    terms = pltpu.MemorySpace.VMEM((COUNT, BS, BS), bf16)
    swapped = shape(VEC + 2 * RHS + ROWS * PART, BS)

    blocks2 = swap(blocks)
    msg, tab, line_row, high, low = call(
        first_kernel,
        [HBM] * 5,
        (msg_shape, table, col8, terms, terms),
        (VMEM, SMEM, VMEM, VMEM, VMEM),
        [BUFFER, LEFT, LEFTS]
        + [pltpu.SMEM((COUNT,), jnp.int32)] * 4
        + [SEMS, pltpu.SemaphoreType.DMA((4,))],
    )(*far(owner, block_row, block_col, right, blocks))
    inc = exchange(msg)
    keep, send = call(
        first_owner_kernel,
        [VMEM] * 3,
        (swapped, swapped),
        None,
        PARTS + [LINE, pltpu.SMEM((SLOTS,), jnp.int32), ONE],
    )(inc, right, line_row)
    msg, raw, norm_left, left, tab2, cols0, cols1 = call(
        first_send_kernel,
        [VMEM] * 2,
        (msg_shape, vec, col8, left_shape, table, table, table),
        (VMEM,) * 4 + (SMEM,) * 3,
        [LINE] * 3 + [pltpu.SemaphoreType.DMA((3,))],
    )(keep, swap(send))
    start = norm_left
    state = None
    for repeat in range(ITERS):
        inc = exchange(msg)
        if repeat == ITERS - 1:
            break
        if repeat == 0:
            msg, left, norm_right, high2, low2 = call(
                first_user_kernel,
                [SMEM] * 2 + [VMEM] * 6,
                (msg_shape, left_shape, col8, terms, terms),
                (VMEM,) * 5,
                [LEFT, LEFTS2],
            )(*small(tab, tab2), inc, left, norm_left, *near(high, low, blocks2))
        else:
            msg, left, norm_right = call(
                user_kernel,
                [SMEM] * 2 + [VMEM] * 7,
                (msg_shape, left_shape, col8),
                None,
                [LEFT, LEFTS2],
            )(*small(tab, tab2), inc, left, norm_left, *near(high, low, high2, low2))
        inc = exchange(msg)
        first = repeat == 0
        tail = (start,) if first else state
        outs = call(
            lambda *refs, first=first: send_kernel(first, *refs),
            [SMEM] * 2 + [VMEM] * (3 + len(tail)),
            (msg_shape, vec, col8, vec, vec, shape(4 * RHS, BS)),
            None,
            [pltpu.VMEM((VEC, BS), f32)] * 4,
        )(*small(cols0, cols1), inc, raw, norm_right, *tail)
        msg, raw, norm_left = outs[:3]
        state = outs[3:]
    ends = shape(ENDS, BS)
    rows, keep, send = call(
        last_user_kernel,
        [SMEM] * 2 + [VMEM] * 12,
        (shape(2 * OWNERS, BS), ends, ends),
        None,
        [LEFT] * 2,
    )(
        *small(tab, tab2), inc, left, norm_left, *near(high, low, high2, low2),
        raw, start, *state,
    )
    theirs = swap(send)
    rows = lax.all_to_all(rows, GRP_SHARD, 0, 0, tiled=True)
    full = shape(COLS_OWN * RHS, BS)
    sol, left, rel = call(final_kernel, [VMEM] * 3, (full, full, shape(RHS)))(rows, keep, theirs)

    def tall(x):
        return x.reshape(COLS_OWN, RHS, BS).transpose(0, 2, 1).reshape(COLS_OWN * BS, RHS)

    return tall(sol), tall(left), rel


def solution(mesh):
    torus = Mesh(
        mesh.devices.reshape(mesh.shape["grp"], 4, 4, 4), ("grp", "shard_0", "shard_1", "shard_2")
    )
    return jax.shard_map(
        on_device,
        mesh=torus,
        in_specs=(
            P(GRP_SHARD, None, None),
            P(GRP_SHARD),
            P(GRP_SHARD, None),
            P(GRP_SHARD),
            P(GRP_SHARD, None),
        ),
        out_specs=(P(SHARD, None), P(GRP_SHARD, None), P()),
        check_vma=False,
    )
```

```python
import jax
import jax.numpy as jnp
from jax import lax
from jax.experimental import pallas as pl
from jax.experimental.pallas import tpu as pltpu
from jax.sharding import Mesh
from jax.sharding import PartitionSpec as P

ITERS = 4
COLS_OWN = 16
SHARD = ("shard_0", "shard_1", "shard_2")
GRP_SHARD = ("grp", "shard_0", "shard_1", "shard_2")

OWNERS = 64
CAP = 2
BS = 128
RHS = 8
COUNT = 64
ROWS = 16
SLOTS = OWNERS * CAP
MSG = RHS * CAP + 1
TALL = OWNERS * MSG
CHUNK = 8
CHUNKS = COUNT // CHUNK
PART = RHS // 2
LINES = 2 * ROWS
VEC = COLS_OWN * PART
ENDS = 2 * VEC + 3 * RHS + ROWS * PART

f32 = jnp.float32
bf16 = jnp.bfloat16


def diag_mask():
    sub = lax.broadcasted_iota(jnp.int32, (RHS, BS), 0)
    lane = lax.broadcasted_iota(jnp.int32, (RHS, BS), 1)
    return sub == lane


def row_of(column):
    return jnp.sum(jnp.where(diag_mask(), column, 0.0), axis=0, keepdims=True)


def column_of(row):
    spread = jnp.broadcast_to(row, (RHS, BS))
    total = jnp.sum(jnp.where(diag_mask(), spread, 0.0), axis=1, keepdims=True)
    return jnp.broadcast_to(total, (RHS, BS))


def squares(values):
    cube = values.reshape(values.shape[0] // RHS, RHS, BS)
    total = jnp.sum(jnp.sum(cube * cube, axis=0), axis=1, keepdims=True)
    return jnp.broadcast_to(total, (RHS, BS))


def part_squares(values):
    cube = values.reshape(values.shape[0] // RHS, RHS, BS)
    total = jnp.sum(cube * cube, axis=0)
    total = total[:PART] + total[PART:]
    total = jnp.sum(jnp.concatenate([total, total], axis=0), axis=1, keepdims=True)
    return jnp.broadcast_to(total, (RHS, BS))


def part_mask(shift):
    sub = lax.broadcasted_iota(jnp.int32, (RHS, BS), 0)
    lane = lax.broadcasted_iota(jnp.int32, (RHS, BS), 1)
    return sub, lane, lane == jnp.where(sub < PART, sub, sub - PART) + shift


def part_row(column, shift=0):
    sub, _, mask = part_mask(shift)
    return jnp.sum(jnp.where(mask & (sub < PART), column, 0.0), axis=0, keepdims=True)


def part_column(row, shift=0):
    _, _, mask = part_mask(shift)
    spread = jnp.broadcast_to(row, (RHS, BS))
    total = jnp.sum(jnp.where(mask, spread, 0.0), axis=1, keepdims=True)
    return jnp.broadcast_to(total, (RHS, BS))


def tiled(column, count):
    return jnp.concatenate([column] * count, axis=0)


def sum_rows(ref, column_of):
    rows = [ref[pl.ds(MSG * o + MSG - 1, 1), :] for o in range(OWNERS)]
    while len(rows) > 1:
        rows = [rows[i] + rows[i + 1] for i in range(0, len(rows), 2)]
    return column_of(rows[0])


def put_rows(ref, row):
    for o in range(OWNERS):
        ref[pl.ds(MSG * o + MSG - 1, 1), :] = row


def split(x):
    high = x.astype(bf16)
    low = (x - high.astype(f32)).astype(bf16)
    return high, low


def stacked(x):
    high = x.astype(bf16).astype(f32)
    both = jnp.concatenate([high, x - high], axis=0).astype(bf16)
    return jnp.concatenate([both, both], axis=1)


def fold(out):
    half = out.shape[0] // 2
    return out[:half] + out[half:]


def chunk_copy(blocks, bbuf, sem, c):
    span = pl.ds(c * CHUNK, CHUNK)
    return pltpu.make_async_copy(blocks.at[span], bbuf.at[span], sem.at[c])


def split_left(us, left, height):
    for r in range(left.shape[0] // height):
        us[r] = stacked(left[r * height : (r + 1) * height])


def adjoint_block(pos, row, us, high, low, msg):
    rhs = jnp.concatenate([high, low], axis=0)
    out = lax.dot_general(us[row], rhs, (((1,), (0,)), ((), ())), preferred_element_type=f32)
    sent = fold(out)
    msg[pl.ds(pos, sent.shape[0]), :] = sent


def forward_block(piece, high, low):
    rhs = jnp.concatenate([high, low], axis=0)
    out = lax.dot_general(
        stacked(piece), rhs, (((1,), (0,)), ((), ())), preferred_element_type=f32
    )
    return fold(out)


def first_kernel(
    owner_in, row_in, col_in, right_in, blocks,
    msg, tab, line_row, high, low, high_t, low_t,
    bbuf, right, us, owner, row, col, taken, sem, little,
):
    loads = [
        pltpu.make_async_copy(owner_in, owner, little.at[0]),
        pltpu.make_async_copy(row_in, row, little.at[1]),
        pltpu.make_async_copy(col_in, col, little.at[2]),
        pltpu.make_async_copy(right_in, right, little.at[3]),
    ]
    for load in loads:
        load.start()

    def begin(c, carry):
        chunk_copy(blocks, bbuf, sem, c).start()
        return carry

    lax.fori_loop(0, CHUNKS, begin, 0)
    msg[...] = jnp.zeros((TALL, BS), f32)

    def clear(g, carry):
        for j in range(8):
            taken[g * 8 + j] = 0
        return carry

    lax.fori_loop(0, OWNERS // 8, clear, 0)
    for load in loads:
        load.wait()
    right_all = right[...]
    put_rows(msg, row_of(squares(right_all)))
    split_left(us, right_all, RHS)
    grp = lax.axis_index("grp")
    listed = jnp.zeros((1, BS), f32)
    lane = lax.broadcasted_iota(jnp.int32, (1, BS), 1)

    for c in range(CHUNKS):
        chunk_copy(blocks, bbuf, sem, c).wait()
        for k in range(c * CHUNK, (c + 1) * CHUNK):
            o = owner[k]
            rank = taken[o]
            taken[o] = rank + 1
            pos = o * MSG + rank * RHS
            line = lax.rem(row[k], ROWS)
            place = o * MSG + grp * (CAP * PART) + rank * PART
            here = line + grp * ROWS
            tab[k] = place
            tab[COUNT + k] = here
            listed = jnp.where(lane == k, place.astype(f32), listed)
            listed = jnp.where(lane == COUNT + k, here.astype(f32), listed)
            span = pl.ds(o * MSG + MSG - 1, 1)
            msg[span, :] = jnp.where(lane == RHS + rank, col[k].astype(f32), msg[span, :])
            h, l = split(bbuf[k])
            high[k] = h
            low[k] = l
            adjoint_block(pos, line, us, h, l, msg)
            high_t[k], low_t[k] = split(bbuf[k].T)
    line_row[...] = jnp.broadcast_to(listed, (RHS, BS))


def first_owner_kernel(inc, right, line_row, keep, send, p0, p1, p2, p3, vcols, cols, sem):
    grp = lax.axis_index("grp")
    parts = (p0, p1, p2, p3)
    lane = lax.broadcasted_iota(jnp.int32, (1, BS), 1)
    pairs = [
        jnp.where(
            lane == o * CAP,
            inc[pl.ds(MSG * o + MSG - 1, 1), RHS : RHS + 1],
            jnp.where(lane == o * CAP + 1, inc[pl.ds(MSG * o + MSG - 1, 1), RHS + 1 : RHS + 2], 0.0),
        )
        for o in range(OWNERS)
    ]
    while len(pairs) > 1:
        pairs = [pairs[i] + pairs[i + 1] for i in range(0, len(pairs), 2)]
    vcols[...] = pairs[0][0].astype(jnp.int32)
    copy = pltpu.make_async_copy(vcols, cols, sem)
    copy.start()
    norm = sum_rows(inc, column_of)
    for ref in (keep, send):
        ref[pl.ds(VEC, RHS), :] = norm
        ref[pl.ds(VEC + RHS, 1), :] = pairs[0]
        ref[pl.ds(VEC + RHS + 1, 1), :] = line_row[pl.ds(0, 1), :]
        ref[pl.ds(VEC + RHS + 2, RHS - 2), :] = jnp.zeros((RHS - 2, BS), f32)
    for part in parts:
        part[...] = jnp.zeros((COLS_OWN * RHS, BS), f32)

    def halves(at, tile):
        first, second = tile[:PART], tile[PART:]
        keep[pl.ds(at, PART), :] = jnp.where(grp == 0, first, second)
        send[pl.ds(at, PART), :] = jnp.where(grp == 0, second, first)

    for r in range(ROWS):
        halves(VEC + 2 * RHS + r * PART, right[pl.ds(r * RHS, RHS), :])
    copy.wait()

    def step(g, carry):
        for j in range(8):
            o = g * 8 + j
            for s in range(CAP):
                span = pl.ds(pl.multiple_of(cols[o * CAP + s] * RHS, RHS), RHS)
                part = parts[(2 * j + s) % len(parts)]
                part[span, :] = part[span, :] + inc[pl.ds(o * MSG + s * RHS, RHS), :]
        return carry

    lax.fori_loop(0, OWNERS // 8, step, 0)
    for c in range(COLS_OWN):
        span = pl.ds(c * RHS, RHS)
        halves(c * PART, (p0[span, :] + p1[span, :]) + (p2[span, :] + p3[span, :]))


def send_slots(cols, raw, msg):
    put_rows(msg, part_row(part_squares(raw[...])))
    for o in range(OWNERS):
        for s in range(2 * CAP):
            at = cols[s // CAP][o * CAP + s % CAP]
            msg[pl.ds(o * MSG + s * PART, PART), :] = raw[pl.ds(at, PART), :]


def first_send_kernel(
    keep, theirs,
    msg, raw, nleft, left, tab, cols0, cols1,
    vtab, vcols0, vcols1, sem,
):
    grp = lax.axis_index("grp")
    mine_cols = keep[pl.ds(VEC + RHS, 1), :]
    other_cols = theirs[pl.ds(VEC + RHS, 1), :]
    vtab[...] = theirs[pl.ds(VEC + RHS + 1, 1), :][0].astype(jnp.int32)
    vcols0[...] = jnp.where(grp == 0, mine_cols, other_cols)[0].astype(jnp.int32) * PART
    vcols1[...] = jnp.where(grp == 0, other_cols, mine_cols)[0].astype(jnp.int32) * PART
    copies = [
        pltpu.make_async_copy(vtab, tab, sem.at[0]),
        pltpu.make_async_copy(vcols0, cols0, sem.at[1]),
        pltpu.make_async_copy(vcols1, cols1, sem.at[2]),
    ]
    for copy in copies:
        copy.start()
    norm = jnp.sqrt(keep[pl.ds(VEC, RHS), :] + theirs[pl.ds(VEC, RHS), :])
    own = jnp.where(grp == 0, norm[:PART], norm[PART:])
    norm = jnp.concatenate([own, own], axis=0)
    nleft[...] = norm
    body = pl.ds(0, VEC)
    raw[...] = (keep[body, :] + theirs[body, :]) / tiled(norm, VEC // RHS)
    size = ROWS * PART
    tail = pl.ds(VEC + 2 * RHS, size)
    left[pl.ds(pl.multiple_of(grp * size, RHS), size), :] = keep[tail, :]
    left[pl.ds(pl.multiple_of((1 - grp) * size, RHS), size), :] = theirs[tail, :]
    for copy in copies:
        copy.wait()
    send_slots((cols0, cols1), raw, msg)


def send_kernel(first, cols0, cols1, inc, qprev, nright, *refs):
    parts = refs[-4:]
    if first:
        start, msg, raw, nleft, sol, search, scal = refs[:-4]
    else:
        sol_in, search_in, scal_in, msg, raw, nleft, sol, search, scal = refs[:-4]
    cols = (cols0, cols1)
    for part in parts:
        part[...] = jnp.zeros((VEC, BS), f32)

    for o in range(OWNERS):
        for s in range(2 * CAP):
            span = pl.ds(cols[s // CAP][o * CAP + s % CAP], PART)
            part = parts[s]
            part[span, :] = part[span, :] + inc[pl.ds(o * MSG + s * PART, PART), :]
    total = (parts[0][...] + parts[1][...]) + (parts[2][...] + parts[3][...])
    n = VEC // RHS
    norm_left = jnp.sqrt(sum_rows(inc, part_column))
    norm_right = nright[...]
    nleft[...] = norm_left
    vec = qprev[...] / tiled(norm_right, n)
    raw[...] = total / tiled(norm_left, n) - tiled(norm_left, n) * vec
    send_slots(cols, raw, msg)
    if first:
        old_search = vec
        diag_bar = norm_right
        residual = start[...]
        old_sol = jnp.zeros((VEC, BS), f32)
    else:
        radius = scal_in[pl.ds(0, RHS), :]
        cosine = scal_in[pl.ds(RHS, RHS), :]
        sine_term = scal_in[pl.ds(2 * RHS, RHS), :]
        residual = scal_in[pl.ds(3 * RHS, RHS), :]
        coupling = sine_term * norm_right
        old_search = vec - tiled(coupling / radius, n) * search_in[...]
        diag_bar = -cosine * norm_right
        old_sol = sol_in[...]
    radius = jnp.sqrt(diag_bar * diag_bar + norm_left * norm_left)
    cosine = diag_bar / radius
    sine_term = norm_left / radius
    sol[...] = old_sol + tiled(cosine * residual / radius, n) * old_search
    search[...] = old_search
    scal[pl.ds(0, RHS), :] = radius
    scal[pl.ds(RHS, RHS), :] = cosine
    scal[pl.ds(2 * RHS, RHS), :] = sine_term
    scal[pl.ds(3 * RHS, RHS), :] = sine_term * residual


def forward_all(tab, inc, high, low, into):
    for k in range(COUNT):
        part = forward_block(inc[pl.ds(tab[k], PART), :], high[k], low[k])
        span = pl.ds(tab[COUNT + k] * PART, PART)
        ref = into[k % 2]
        ref[span, :] = ref[span, :] + part


def adjoint_all(tab, us, high, low, msg):
    for k in range(COUNT):
        adjoint_block(tab[k], tab[COUNT + k], us, high[k], low[k], msg)


def left_of(lraw, other, uraw, nleft, norm_right):
    n = LINES * PART // RHS
    left = (lraw[...] + other[...]) / tiled(norm_right, n) - tiled(norm_right, n) * (
        uraw[...] / tiled(nleft[...], n)
    )
    lraw[...] = left
    return left


def first_user_kernel(
    tab, tab2, inc, uraw, nleft, high, low, high_t, low_t, blocks,
    msg, lraw, nright, high2, low2, high2_t, low2_t,
    other, us,
):
    norm_right = jnp.sqrt(sum_rows(inc, part_column))
    nright[...] = norm_right
    lraw[...] = jnp.zeros(lraw.shape, f32)
    other[...] = jnp.zeros(lraw.shape, f32)
    forward_all(tab, inc, high_t, low_t, (lraw, other))
    for k in range(COUNT):
        high2[k], low2[k] = split(blocks[k])
        h, l = split(blocks[k].T)
        high2_t[k] = h
        low2_t[k] = l
        part = forward_block(inc[pl.ds(tab2[k], PART), :], h, l)
        span = pl.ds(tab2[COUNT + k] * PART, PART)
        ref = other if k % 2 else lraw
        ref[span, :] = ref[span, :] + part
    left = left_of(lraw, other, uraw, nleft, norm_right)
    msg[...] = jnp.zeros((TALL, BS), f32)
    put_rows(msg, part_row(part_squares(left)))
    split_left(us, left, PART)
    adjoint_all(tab, us, high, low, msg)
    adjoint_all(tab2, us, high2, low2, msg)


def user_kernel(
    tab, tab2, inc, uraw, nleft, high, low, high2, low2, high_t, low_t, high2_t, low2_t,
    msg, lraw, nright, other, us,
):
    norm_right = jnp.sqrt(sum_rows(inc, part_column))
    nright[...] = norm_right
    lraw[...] = jnp.zeros(lraw.shape, f32)
    other[...] = jnp.zeros(lraw.shape, f32)
    forward_all(tab, inc, high_t, low_t, (lraw, other))
    forward_all(tab2, inc, high2_t, low2_t, (lraw, other))
    left = left_of(lraw, other, uraw, nleft, norm_right)
    msg[...] = jnp.zeros((TALL, BS), f32)
    put_rows(msg, part_row(part_squares(left)))
    split_left(us, left, PART)
    adjoint_all(tab, us, high, low, msg)
    adjoint_all(tab2, us, high2, low2, msg)


def last_user_kernel(
    tab, tab2, inc, uraw, nleft, high, low, high2, low2, qprev, start, sol_in, search_in, scal_in,
    msg, keep, send, lraw, other,
):
    grp = lax.axis_index("grp")
    norm_right = jnp.sqrt(sum_rows(inc, part_column))
    lraw[...] = jnp.zeros(lraw.shape, f32)
    other[...] = jnp.zeros(lraw.shape, f32)
    n = VEC // RHS
    radius = scal_in[pl.ds(0, RHS), :]
    cosine = scal_in[pl.ds(RHS, RHS), :]
    sine_term = scal_in[pl.ds(2 * RHS, RHS), :]
    vec = qprev[...] / tiled(norm_right, n)
    search = vec - tiled(sine_term * norm_right / radius, n) * search_in[...]
    for ref in (keep, send):
        ref[pl.ds(0, VEC), :] = sol_in[...]
        ref[pl.ds(VEC, VEC), :] = search
        ref[pl.ds(2 * VEC, RHS), :] = -cosine * norm_right
        ref[pl.ds(2 * VEC + RHS, RHS), :] = scal_in[pl.ds(3 * RHS, RHS), :]
        ref[pl.ds(2 * VEC + 2 * RHS, RHS), :] = start[...]
    forward_all(tab, inc, high, low, (lraw, other))
    forward_all(tab2, inc, high2, low2, (lraw, other))
    left = left_of(lraw, other, uraw, nleft, norm_right)
    row = part_row(part_squares(left), grp * PART)
    msg[...] = jnp.broadcast_to(row, msg.shape)
    size = ROWS * PART
    for ref, at in ((keep, grp), (send, 1 - grp)):
        ref[pl.ds(ENDS - size, size), :] = lraw[pl.ds(pl.multiple_of(at * size, RHS), size), :]


def finished(total, ref, grp):
    norm_left = jnp.sqrt(part_column(total, grp * PART))
    size = ROWS * PART
    left = ref[pl.ds(ENDS - size, size), :] / tiled(norm_left, size // RHS)
    diag_bar = ref[pl.ds(2 * VEC, RHS), :]
    residual = ref[pl.ds(2 * VEC + RHS, RHS), :]
    radius = jnp.sqrt(diag_bar * diag_bar + norm_left * norm_left)
    cosine = diag_bar / radius
    sine_term = norm_left / radius
    step = tiled(cosine * residual / radius, VEC // RHS)
    sol = ref[pl.ds(0, VEC), :] + step * ref[pl.ds(VEC, VEC), :]
    rel = sine_term * residual / ref[pl.ds(2 * VEC + 2 * RHS, RHS), :]
    return sol, left, rel


def final_kernel(rows, keep, theirs, sol, left, rel):
    grp = lax.axis_index("grp")
    total = jnp.sum(rows[...], axis=0, keepdims=True)
    mine = finished(total, keep, grp)
    other = finished(total, theirs, 1 - grp)

    def join(ref, mine, other):
        first = jnp.where(grp == 0, mine, other)
        second = jnp.where(grp == 0, other, mine)
        for c in range(mine.shape[0] // PART):
            ref[pl.ds(c * RHS, PART), :] = first[c * PART : (c + 1) * PART]
            ref[pl.ds(c * RHS + PART, PART), :] = second[c * PART : (c + 1) * PART]

    join(sol, mine[0], other[0])
    join(left, mine[1], other[1])
    first = jnp.where(grp == 0, mine[2], other[2])
    second = jnp.where(grp == 0, other[2], mine[2])
    both = jnp.concatenate([first[:PART], second[:PART]], axis=0)
    rel[...] = row_of(both)[0, :RHS]


def shape(*dims, dtype=f32):
    return jax.ShapeDtypeStruct(dims, dtype)


VMEM = pl.BlockSpec(memory_space=pltpu.VMEM)
SMEM = pl.BlockSpec(memory_space=pltpu.SMEM)
HBM = pl.BlockSpec(memory_space=pltpu.HBM)
PARTS = [pltpu.VMEM((COLS_OWN * RHS, BS), f32)] * 4
LEFTS = pltpu.VMEM((ROWS, 2 * RHS, 2 * BS), bf16)
LEFTS2 = pltpu.VMEM((LINES, RHS, 2 * BS), bf16)
LEFT = pltpu.VMEM((ROWS * RHS, BS), f32)
BUFFER = pltpu.VMEM((COUNT, BS, BS), f32)
SEMS = pltpu.SemaphoreType.DMA((CHUNKS,))
ONE = pltpu.SemaphoreType.DMA(())
LINE = pltpu.VMEM((SLOTS,), jnp.int32)


def call(body, ins, outs, specs_out=None, scratch=()):
    return pl.pallas_call(
        body,
        out_shape=outs,
        in_specs=ins,
        out_specs=specs_out or jax.tree.map(lambda _: VMEM, outs),
        scratch_shapes=scratch,
        compiler_params=pltpu.CompilerParams(vmem_limit_bytes=24 * 1024 * 1024),
    )


def exchange(msg):
    sent = msg.reshape(OWNERS, MSG * BS)
    return lax.all_to_all(sent, SHARD, 0, 0, tiled=True).reshape(TALL, BS)


def swap(half):
    return lax.ppermute(half, "grp", [(0, 1), (1, 0)])


def small(*xs):
    return [pltpu.with_memory_space_constraint(x, pltpu.SMEM) for x in xs]


def near(*xs):
    return [pltpu.with_memory_space_constraint(x, pltpu.VMEM) for x in xs]


def far(*xs):
    return [pltpu.with_memory_space_constraint(x, pltpu.HBM) for x in xs]


def on_device(blocks, block_row, block_owner, block_col, right_side):
    owner = block_owner[:, 0]
    right = right_side.reshape(ROWS, BS, RHS).transpose(0, 2, 1).reshape(ROWS * RHS, BS)
    left_shape = shape(LINES * PART, BS)
    vec = shape(VEC, BS)
    col8 = shape(RHS, BS)
    msg_shape = shape(TALL, BS)
    table = pltpu.MemorySpace.SMEM((SLOTS,), jnp.int32)
    terms = pltpu.MemorySpace.VMEM((COUNT, BS, BS), bf16)
    swapped = shape(VEC + 2 * RHS + ROWS * PART, BS)

    blocks2 = swap(blocks)
    msg, tab, line_row, high, low, high_t, low_t = call(
        first_kernel,
        [HBM] * 5,
        (msg_shape, table, col8, terms, terms, terms, terms),
        (VMEM, SMEM) + (VMEM,) * 5,
        [BUFFER, LEFT, LEFTS]
        + [pltpu.SMEM((COUNT,), jnp.int32)] * 4
        + [SEMS, pltpu.SemaphoreType.DMA((4,))],
    )(*far(owner, block_row, block_col, right, blocks))
    inc = exchange(msg)
    keep, send = call(
        first_owner_kernel,
        [VMEM] * 3,
        (swapped, swapped),
        None,
        PARTS + [LINE, pltpu.SMEM((SLOTS,), jnp.int32), ONE],
    )(inc, right, line_row)
    msg, raw, norm_left, left, tab2, cols0, cols1 = call(
        first_send_kernel,
        [VMEM] * 2,
        (msg_shape, vec, col8, left_shape, table, table, table),
        (VMEM,) * 4 + (SMEM,) * 3,
        [LINE] * 3 + [pltpu.SemaphoreType.DMA((3,))],
    )(keep, swap(send))
    start = norm_left
    state = None
    for repeat in range(ITERS):
        inc = exchange(msg)
        if repeat == ITERS - 1:
            break
        if repeat == 0:
            msg, left, norm_right, high2, low2, high2_t, low2_t = call(
                first_user_kernel,
                [SMEM] * 2 + [VMEM] * 8,
                (msg_shape, left_shape, col8, terms, terms, terms, terms),
                (VMEM,) * 7,
                [LEFT, LEFTS2],
            )(*small(tab, tab2), inc, left, norm_left, *near(high, low, high_t, low_t, blocks2))
        else:
            msg, left, norm_right = call(
                user_kernel,
                [SMEM] * 2 + [VMEM] * 11,
                (msg_shape, left_shape, col8),
                None,
                [LEFT, LEFTS2],
            )(
                *small(tab, tab2), inc, left, norm_left,
                *near(high, low, high2, low2, high_t, low_t, high2_t, low2_t),
            )
        inc = exchange(msg)
        first = repeat == 0
        tail = (start,) if first else state
        outs = call(
            lambda *refs, first=first: send_kernel(first, *refs),
            [SMEM] * 2 + [VMEM] * (3 + len(tail)),
            (msg_shape, vec, col8, vec, vec, shape(4 * RHS, BS)),
            None,
            [pltpu.VMEM((VEC, BS), f32)] * 4,
        )(*small(cols0, cols1), inc, raw, norm_right, *tail)
        msg, raw, norm_left = outs[:3]
        state = outs[3:]
    ends = shape(ENDS, BS)
    rows, keep, send = call(
        last_user_kernel,
        [SMEM] * 2 + [VMEM] * 12,
        (shape(2 * OWNERS, BS), ends, ends),
        None,
        [LEFT] * 2,
    )(
        *small(tab, tab2), inc, left, norm_left, *near(high_t, low_t, high2_t, low2_t),
        raw, start, *state,
    )
    theirs = swap(send)
    rows = lax.all_to_all(rows, GRP_SHARD, 0, 0, tiled=True)
    full = shape(COLS_OWN * RHS, BS)
    sol, left, rel = call(final_kernel, [VMEM] * 3, (full, full, shape(RHS)))(rows, keep, theirs)

    def tall(x):
        return x.reshape(COLS_OWN, RHS, BS).transpose(0, 2, 1).reshape(COLS_OWN * BS, RHS)

    return tall(sol), tall(left), rel


def solution(mesh):
    torus = Mesh(
        mesh.devices.reshape(mesh.shape["grp"], 4, 4, 4), ("grp", "shard_0", "shard_1", "shard_2")
    )
    return jax.shard_map(
        on_device,
        mesh=torus,
        in_specs=(
            P(GRP_SHARD, None, None),
            P(GRP_SHARD),
            P(GRP_SHARD, None),
            P(GRP_SHARD),
            P(GRP_SHARD, None),
        ),
        out_specs=(P(SHARD, None), P(GRP_SHARD, None), P()),
        check_vma=False,
    )
```

```python
import jax
import jax.numpy as jnp
from jax import lax
from jax.experimental import pallas as pl
from jax.experimental.pallas import tpu as pltpu
from jax.sharding import Mesh
from jax.sharding import PartitionSpec as P

ITERS = 4
COLS_OWN = 16
SHARD = ("shard_0", "shard_1", "shard_2")
GRP_SHARD = ("grp", "shard_0", "shard_1", "shard_2")

OWNERS = 64
CAP = 2
BS = 128
RHS = 8
COUNT = 64
ROWS = 16
SLOTS = OWNERS * CAP
MSG = RHS * CAP + 1
TALL = OWNERS * MSG
CHUNK = 8
CHUNKS = COUNT // CHUNK
PART = RHS // 2
LINES = 2 * ROWS
STAGGER = 3000
VEC = COLS_OWN * PART
ENDS = 2 * VEC + 3 * RHS + ROWS * PART

f32 = jnp.float32
bf16 = jnp.bfloat16


def diag_mask():
    sub = lax.broadcasted_iota(jnp.int32, (RHS, BS), 0)
    lane = lax.broadcasted_iota(jnp.int32, (RHS, BS), 1)
    return sub == lane


def row_of(column):
    return jnp.sum(jnp.where(diag_mask(), column, 0.0), axis=0, keepdims=True)


def column_of(row):
    spread = jnp.broadcast_to(row, (RHS, BS))
    total = jnp.sum(jnp.where(diag_mask(), spread, 0.0), axis=1, keepdims=True)
    return jnp.broadcast_to(total, (RHS, BS))


def squares(values):
    cube = values.reshape(values.shape[0] // RHS, RHS, BS)
    total = jnp.sum(jnp.sum(cube * cube, axis=0), axis=1, keepdims=True)
    return jnp.broadcast_to(total, (RHS, BS))


def part_squares(values):
    cube = values.reshape(values.shape[0] // RHS, RHS, BS)
    total = jnp.sum(cube * cube, axis=0)
    total = total[:PART] + total[PART:]
    total = jnp.sum(jnp.concatenate([total, total], axis=0), axis=1, keepdims=True)
    return jnp.broadcast_to(total, (RHS, BS))


def part_mask(shift):
    sub = lax.broadcasted_iota(jnp.int32, (RHS, BS), 0)
    lane = lax.broadcasted_iota(jnp.int32, (RHS, BS), 1)
    return sub, lane, lane == jnp.where(sub < PART, sub, sub - PART) + shift


def part_row(column, shift=0):
    sub, _, mask = part_mask(shift)
    return jnp.sum(jnp.where(mask & (sub < PART), column, 0.0), axis=0, keepdims=True)


def part_column(row, shift=0):
    _, _, mask = part_mask(shift)
    spread = jnp.broadcast_to(row, (RHS, BS))
    total = jnp.sum(jnp.where(mask, spread, 0.0), axis=1, keepdims=True)
    return jnp.broadcast_to(total, (RHS, BS))


def tiled(column, count):
    return jnp.concatenate([column] * count, axis=0)


def sum_rows(ref, column_of):
    rows = [ref[pl.ds(MSG * o + MSG - 1, 1), :] for o in range(OWNERS)]
    while len(rows) > 1:
        rows = [rows[i] + rows[i + 1] for i in range(0, len(rows), 2)]
    return column_of(rows[0])


def put_rows(ref, row):
    for o in range(OWNERS):
        ref[pl.ds(MSG * o + MSG - 1, 1), :] = row


def split(x):
    high = x.astype(bf16)
    low = (x - high.astype(f32)).astype(bf16)
    return high, low


def stacked(x):
    high = x.astype(bf16).astype(f32)
    both = jnp.concatenate([high, x - high], axis=0).astype(bf16)
    return jnp.concatenate([both, both], axis=1)


def fold(out):
    half = out.shape[0] // 2
    return out[:half] + out[half:]


def chunk_copy(blocks, bbuf, sem, c):
    span = pl.ds(c * CHUNK, CHUNK)
    return pltpu.make_async_copy(blocks.at[span], bbuf.at[span], sem.at[c])


def split_left(us, left, height):
    for r in range(left.shape[0] // height):
        us[r] = stacked(left[r * height : (r + 1) * height])


def adjoint_block(pos, row, us, high, low, msg):
    rhs = jnp.concatenate([high, low], axis=0)
    out = lax.dot_general(us[row], rhs, (((1,), (0,)), ((), ())), preferred_element_type=f32)
    sent = fold(out)
    msg[pl.ds(pos, sent.shape[0]), :] = sent


def forward_block(piece, high, low):
    rhs = jnp.concatenate([high, low], axis=0)
    out = lax.dot_general(
        stacked(piece), rhs, (((1,), (0,)), ((), ())), preferred_element_type=f32
    )
    return fold(out)


def first_kernel(
    owner_in, row_in, col_in, right_in, blocks,
    msg, tab, line_row, high, low, high_t, low_t,
    bbuf, right, us, owner, row, col, taken, sem, little,
):
    loads = [
        pltpu.make_async_copy(owner_in, owner, little.at[0]),
        pltpu.make_async_copy(row_in, row, little.at[1]),
        pltpu.make_async_copy(col_in, col, little.at[2]),
        pltpu.make_async_copy(right_in, right, little.at[3]),
    ]
    for load in loads:
        load.start()

    def begin(c, carry):
        chunk_copy(blocks, bbuf, sem, c).start()
        return carry

    lax.fori_loop(0, CHUNKS, begin, 0)
    msg[...] = jnp.zeros((TALL, BS), f32)

    def clear(g, carry):
        for j in range(8):
            taken[g * 8 + j] = 0
        return carry

    lax.fori_loop(0, OWNERS // 8, clear, 0)
    for load in loads:
        load.wait()
    right_all = right[...]
    put_rows(msg, row_of(squares(right_all)))
    split_left(us, right_all, RHS)
    grp = lax.axis_index("grp")
    listed = jnp.zeros((1, BS), f32)
    lane = lax.broadcasted_iota(jnp.int32, (1, BS), 1)

    for c in range(CHUNKS):
        chunk_copy(blocks, bbuf, sem, c).wait()
        for k in range(c * CHUNK, (c + 1) * CHUNK):
            o = owner[k]
            rank = taken[o]
            taken[o] = rank + 1
            pos = o * MSG + rank * RHS
            line = lax.rem(row[k], ROWS)
            place = o * MSG + grp * (CAP * PART) + rank * PART
            here = line + grp * ROWS
            tab[k] = place
            tab[COUNT + k] = here
            listed = jnp.where(lane == k, place.astype(f32), listed)
            listed = jnp.where(lane == COUNT + k, here.astype(f32), listed)
            span = pl.ds(o * MSG + MSG - 1, 1)
            msg[span, :] = jnp.where(lane == RHS + rank, col[k].astype(f32), msg[span, :])
            h, l = split(bbuf[k])
            high[k] = h
            low[k] = l
            adjoint_block(pos, line, us, h, l, msg)
            high_t[k], low_t[k] = split(bbuf[k].T)
    line_row[...] = jnp.broadcast_to(listed, (RHS, BS))


def first_owner_kernel(inc, right, line_row, keep, send, p0, p1, p2, p3, vcols, cols, sem):
    grp = lax.axis_index("grp")
    parts = (p0, p1, p2, p3)
    lane = lax.broadcasted_iota(jnp.int32, (1, BS), 1)
    pairs = [
        jnp.where(
            lane == o * CAP,
            inc[pl.ds(MSG * o + MSG - 1, 1), RHS : RHS + 1],
            jnp.where(lane == o * CAP + 1, inc[pl.ds(MSG * o + MSG - 1, 1), RHS + 1 : RHS + 2], 0.0),
        )
        for o in range(OWNERS)
    ]
    while len(pairs) > 1:
        pairs = [pairs[i] + pairs[i + 1] for i in range(0, len(pairs), 2)]
    vcols[...] = pairs[0][0].astype(jnp.int32)
    copy = pltpu.make_async_copy(vcols, cols, sem)
    copy.start()
    norm = sum_rows(inc, column_of)
    for ref in (keep, send):
        ref[pl.ds(VEC, RHS), :] = norm
        ref[pl.ds(VEC + RHS, 1), :] = pairs[0]
        ref[pl.ds(VEC + RHS + 1, 1), :] = line_row[pl.ds(0, 1), :]
        ref[pl.ds(VEC + RHS + 2, RHS - 2), :] = jnp.zeros((RHS - 2, BS), f32)
    for part in parts:
        part[...] = jnp.zeros((COLS_OWN * RHS, BS), f32)

    def halves(at, tile):
        first, second = tile[:PART], tile[PART:]
        keep[pl.ds(at, PART), :] = jnp.where(grp == 0, first, second)
        send[pl.ds(at, PART), :] = jnp.where(grp == 0, second, first)

    for r in range(ROWS):
        halves(VEC + 2 * RHS + r * PART, right[pl.ds(r * RHS, RHS), :])
    copy.wait()

    for o in range(OWNERS):
        for s in range(CAP):
            span = pl.ds(pl.multiple_of(cols[o * CAP + s] * RHS, RHS), RHS)
            part = parts[(2 * o + s) % len(parts)]
            part[span, :] = part[span, :] + inc[pl.ds(o * MSG + s * RHS, RHS), :]
    for c in range(COLS_OWN):
        span = pl.ds(c * RHS, RHS)
        halves(c * PART, (p0[span, :] + p1[span, :]) + (p2[span, :] + p3[span, :]))


def send_slots(cols, raw, msg):
    put_rows(msg, part_row(part_squares(raw[...])))
    for o in range(OWNERS):
        for s in range(2 * CAP):
            at = cols[s // CAP][o * CAP + s % CAP]
            msg[pl.ds(o * MSG + s * PART, PART), :] = raw[pl.ds(at, PART), :]


def first_send_kernel(
    keep, theirs,
    msg, raw, nleft, left, tab, cols0, cols1,
    vtab, vcols0, vcols1, sem,
):
    grp = lax.axis_index("grp")
    mine_cols = keep[pl.ds(VEC + RHS, 1), :]
    other_cols = theirs[pl.ds(VEC + RHS, 1), :]
    vtab[...] = theirs[pl.ds(VEC + RHS + 1, 1), :][0].astype(jnp.int32)
    vcols0[...] = jnp.where(grp == 0, mine_cols, other_cols)[0].astype(jnp.int32) * PART
    vcols1[...] = jnp.where(grp == 0, other_cols, mine_cols)[0].astype(jnp.int32) * PART
    copies = [
        pltpu.make_async_copy(vtab, tab, sem.at[0]),
        pltpu.make_async_copy(vcols0, cols0, sem.at[1]),
        pltpu.make_async_copy(vcols1, cols1, sem.at[2]),
    ]
    for copy in copies:
        copy.start()
    norm = jnp.sqrt(keep[pl.ds(VEC, RHS), :] + theirs[pl.ds(VEC, RHS), :])
    own = jnp.where(grp == 0, norm[:PART], norm[PART:])
    norm = jnp.concatenate([own, own], axis=0)
    nleft[...] = norm
    body = pl.ds(0, VEC)
    raw[...] = (keep[body, :] + theirs[body, :]) / tiled(norm, VEC // RHS)
    size = ROWS * PART
    tail = pl.ds(VEC + 2 * RHS, size)
    left[pl.ds(pl.multiple_of(grp * size, RHS), size), :] = keep[tail, :]
    left[pl.ds(pl.multiple_of((1 - grp) * size, RHS), size), :] = theirs[tail, :]
    for copy in copies:
        copy.wait()
    send_slots((cols0, cols1), raw, msg)

    @pl.when(grp == 1)
    def _():
        pl.delay(STAGGER)


def send_kernel(first, cols0, cols1, inc, qprev, nright, *refs):
    parts = refs[-4:]
    if first:
        start, msg, raw, nleft, sol, search, scal = refs[:-4]
    else:
        sol_in, search_in, scal_in, msg, raw, nleft, sol, search, scal = refs[:-4]
    cols = (cols0, cols1)
    for part in parts:
        part[...] = jnp.zeros((VEC, BS), f32)

    for o in range(OWNERS):
        for s in range(2 * CAP):
            span = pl.ds(cols[s // CAP][o * CAP + s % CAP], PART)
            part = parts[s]
            part[span, :] = part[span, :] + inc[pl.ds(o * MSG + s * PART, PART), :]
    total = (parts[0][...] + parts[1][...]) + (parts[2][...] + parts[3][...])
    n = VEC // RHS
    norm_left = jnp.sqrt(sum_rows(inc, part_column))
    norm_right = nright[...]
    nleft[...] = norm_left
    vec = qprev[...] / tiled(norm_right, n)
    raw[...] = total / tiled(norm_left, n) - tiled(norm_left, n) * vec
    send_slots(cols, raw, msg)
    if first:
        old_search = vec
        diag_bar = norm_right
        residual = start[...]
        old_sol = jnp.zeros((VEC, BS), f32)
    else:
        radius = scal_in[pl.ds(0, RHS), :]
        cosine = scal_in[pl.ds(RHS, RHS), :]
        sine_term = scal_in[pl.ds(2 * RHS, RHS), :]
        residual = scal_in[pl.ds(3 * RHS, RHS), :]
        coupling = sine_term * norm_right
        old_search = vec - tiled(coupling / radius, n) * search_in[...]
        diag_bar = -cosine * norm_right
        old_sol = sol_in[...]
    radius = jnp.sqrt(diag_bar * diag_bar + norm_left * norm_left)
    cosine = diag_bar / radius
    sine_term = norm_left / radius
    sol[...] = old_sol + tiled(cosine * residual / radius, n) * old_search
    search[...] = old_search
    scal[pl.ds(0, RHS), :] = radius
    scal[pl.ds(RHS, RHS), :] = cosine
    scal[pl.ds(2 * RHS, RHS), :] = sine_term
    scal[pl.ds(3 * RHS, RHS), :] = sine_term * residual


def forward_all(tab, inc, high, low, into):
    for k in range(COUNT):
        part = forward_block(inc[pl.ds(tab[k], PART), :], high[k], low[k])
        span = pl.ds(tab[COUNT + k] * PART, PART)
        ref = into[k % 2]
        ref[span, :] = ref[span, :] + part


def adjoint_all(tab, us, high, low, msg):
    for k in range(COUNT):
        adjoint_block(tab[k], tab[COUNT + k], us, high[k], low[k], msg)


def left_of(lraw, other, uraw, nleft, norm_right):
    n = LINES * PART // RHS
    left = (lraw[...] + other[...]) / tiled(norm_right, n) - tiled(norm_right, n) * (
        uraw[...] / tiled(nleft[...], n)
    )
    lraw[...] = left
    return left


def first_user_kernel(
    tab, tab2, inc, uraw, nleft, high, low, high_t, low_t, blocks,
    msg, lraw, nright, high2, low2, high2_t, low2_t,
    other, us,
):
    norm_right = jnp.sqrt(sum_rows(inc, part_column))
    nright[...] = norm_right
    lraw[...] = jnp.zeros(lraw.shape, f32)
    other[...] = jnp.zeros(lraw.shape, f32)
    forward_all(tab, inc, high_t, low_t, (lraw, other))
    for k in range(COUNT):
        high2[k], low2[k] = split(blocks[k])
        h, l = split(blocks[k].T)
        high2_t[k] = h
        low2_t[k] = l
        part = forward_block(inc[pl.ds(tab2[k], PART), :], h, l)
        span = pl.ds(tab2[COUNT + k] * PART, PART)
        ref = other if k % 2 else lraw
        ref[span, :] = ref[span, :] + part
    left = left_of(lraw, other, uraw, nleft, norm_right)
    msg[...] = jnp.zeros((TALL, BS), f32)
    put_rows(msg, part_row(part_squares(left)))
    split_left(us, left, PART)
    adjoint_all(tab, us, high, low, msg)
    adjoint_all(tab2, us, high2, low2, msg)


def user_kernel(
    tab, tab2, inc, uraw, nleft, high, low, high2, low2, high_t, low_t, high2_t, low2_t,
    msg, lraw, nright, other, us,
):
    norm_right = jnp.sqrt(sum_rows(inc, part_column))
    nright[...] = norm_right
    lraw[...] = jnp.zeros(lraw.shape, f32)
    other[...] = jnp.zeros(lraw.shape, f32)
    forward_all(tab, inc, high_t, low_t, (lraw, other))
    forward_all(tab2, inc, high2_t, low2_t, (lraw, other))
    left = left_of(lraw, other, uraw, nleft, norm_right)
    msg[...] = jnp.zeros((TALL, BS), f32)
    put_rows(msg, part_row(part_squares(left)))
    split_left(us, left, PART)
    adjoint_all(tab, us, high, low, msg)
    adjoint_all(tab2, us, high2, low2, msg)


def last_user_kernel(
    tab, tab2, inc, uraw, nleft, high, low, high2, low2, qprev, start, sol_in, search_in, scal_in,
    msg, keep, send, lraw, other,
):
    grp = lax.axis_index("grp")
    norm_right = jnp.sqrt(sum_rows(inc, part_column))
    lraw[...] = jnp.zeros(lraw.shape, f32)
    other[...] = jnp.zeros(lraw.shape, f32)
    n = VEC // RHS
    radius = scal_in[pl.ds(0, RHS), :]
    cosine = scal_in[pl.ds(RHS, RHS), :]
    sine_term = scal_in[pl.ds(2 * RHS, RHS), :]
    vec = qprev[...] / tiled(norm_right, n)
    search = vec - tiled(sine_term * norm_right / radius, n) * search_in[...]
    for ref in (keep, send):
        ref[pl.ds(0, VEC), :] = sol_in[...]
        ref[pl.ds(VEC, VEC), :] = search
        ref[pl.ds(2 * VEC, RHS), :] = -cosine * norm_right
        ref[pl.ds(2 * VEC + RHS, RHS), :] = scal_in[pl.ds(3 * RHS, RHS), :]
        ref[pl.ds(2 * VEC + 2 * RHS, RHS), :] = start[...]
    forward_all(tab, inc, high, low, (lraw, other))
    forward_all(tab2, inc, high2, low2, (lraw, other))
    left = left_of(lraw, other, uraw, nleft, norm_right)
    row = part_row(part_squares(left), grp * PART)
    msg[...] = jnp.broadcast_to(row, msg.shape)
    size = ROWS * PART
    for ref, at in ((keep, grp), (send, 1 - grp)):
        ref[pl.ds(ENDS - size, size), :] = lraw[pl.ds(pl.multiple_of(at * size, RHS), size), :]


def finished(total, ref, grp):
    norm_left = jnp.sqrt(part_column(total, grp * PART))
    size = ROWS * PART
    left = ref[pl.ds(ENDS - size, size), :] / tiled(norm_left, size // RHS)
    diag_bar = ref[pl.ds(2 * VEC, RHS), :]
    residual = ref[pl.ds(2 * VEC + RHS, RHS), :]
    radius = jnp.sqrt(diag_bar * diag_bar + norm_left * norm_left)
    cosine = diag_bar / radius
    sine_term = norm_left / radius
    step = tiled(cosine * residual / radius, VEC // RHS)
    sol = ref[pl.ds(0, VEC), :] + step * ref[pl.ds(VEC, VEC), :]
    rel = sine_term * residual / ref[pl.ds(2 * VEC + 2 * RHS, RHS), :]
    return sol, left, rel


def final_kernel(rows, keep, theirs, sol, left, rel):
    grp = lax.axis_index("grp")
    total = jnp.sum(rows[...], axis=0, keepdims=True)
    mine = finished(total, keep, grp)
    other = finished(total, theirs, 1 - grp)

    def join(ref, mine, other):
        first = jnp.where(grp == 0, mine, other)
        second = jnp.where(grp == 0, other, mine)
        for c in range(mine.shape[0] // PART):
            ref[pl.ds(c * RHS, PART), :] = first[c * PART : (c + 1) * PART]
            ref[pl.ds(c * RHS + PART, PART), :] = second[c * PART : (c + 1) * PART]

    join(sol, mine[0], other[0])
    join(left, mine[1], other[1])
    first = jnp.where(grp == 0, mine[2], other[2])
    second = jnp.where(grp == 0, other[2], mine[2])
    both = jnp.concatenate([first[:PART], second[:PART]], axis=0)
    rel[...] = row_of(both)[0, :RHS]


def shape(*dims, dtype=f32):
    return jax.ShapeDtypeStruct(dims, dtype)


VMEM = pl.BlockSpec(memory_space=pltpu.VMEM)
SMEM = pl.BlockSpec(memory_space=pltpu.SMEM)
HBM = pl.BlockSpec(memory_space=pltpu.HBM)
PARTS = [pltpu.VMEM((COLS_OWN * RHS, BS), f32)] * 4
LEFTS = pltpu.VMEM((ROWS, 2 * RHS, 2 * BS), bf16)
LEFTS2 = pltpu.VMEM((LINES, RHS, 2 * BS), bf16)
LEFT = pltpu.VMEM((ROWS * RHS, BS), f32)
BUFFER = pltpu.VMEM((COUNT, BS, BS), f32)
SEMS = pltpu.SemaphoreType.DMA((CHUNKS,))
ONE = pltpu.SemaphoreType.DMA(())
LINE = pltpu.VMEM((SLOTS,), jnp.int32)


def call(body, ins, outs, specs_out=None, scratch=()):
    return pl.pallas_call(
        body,
        out_shape=outs,
        in_specs=ins,
        out_specs=specs_out or jax.tree.map(lambda _: VMEM, outs),
        scratch_shapes=scratch,
        compiler_params=pltpu.CompilerParams(vmem_limit_bytes=24 * 1024 * 1024),
    )


def exchange(msg):
    sent = msg.reshape(OWNERS, MSG * BS)
    return lax.all_to_all(sent, SHARD, 0, 0, tiled=True).reshape(TALL, BS)


def swap(half):
    return lax.ppermute(half, "grp", [(0, 1), (1, 0)])


def small(*xs):
    return [pltpu.with_memory_space_constraint(x, pltpu.SMEM) for x in xs]


def near(*xs):
    return [pltpu.with_memory_space_constraint(x, pltpu.VMEM) for x in xs]


def far(*xs):
    return [pltpu.with_memory_space_constraint(x, pltpu.HBM) for x in xs]


def on_device(blocks, block_row, block_owner, block_col, right_side):
    owner = block_owner[:, 0]
    right = right_side.reshape(ROWS, BS, RHS).transpose(0, 2, 1).reshape(ROWS * RHS, BS)
    left_shape = shape(LINES * PART, BS)
    vec = shape(VEC, BS)
    col8 = shape(RHS, BS)
    msg_shape = shape(TALL, BS)
    table = pltpu.MemorySpace.SMEM((SLOTS,), jnp.int32)
    terms = pltpu.MemorySpace.VMEM((COUNT, BS, BS), bf16)
    swapped = shape(VEC + 2 * RHS + ROWS * PART, BS)

    blocks2 = swap(blocks)
    msg, tab, line_row, high, low, high_t, low_t = call(
        first_kernel,
        [HBM] * 5,
        (msg_shape, table, col8, terms, terms, terms, terms),
        (VMEM, SMEM) + (VMEM,) * 5,
        [BUFFER, LEFT, LEFTS]
        + [pltpu.SMEM((COUNT,), jnp.int32)] * 4
        + [SEMS, pltpu.SemaphoreType.DMA((4,))],
    )(*far(owner, block_row, block_col, right, blocks))
    inc = exchange(msg)
    keep, send = call(
        first_owner_kernel,
        [VMEM] * 3,
        (swapped, swapped),
        None,
        PARTS + [LINE, pltpu.SMEM((SLOTS,), jnp.int32), ONE],
    )(inc, right, line_row)
    msg, raw, norm_left, left, tab2, cols0, cols1 = call(
        first_send_kernel,
        [VMEM] * 2,
        (msg_shape, vec, col8, left_shape, table, table, table),
        (VMEM,) * 4 + (SMEM,) * 3,
        [LINE] * 3 + [pltpu.SemaphoreType.DMA((3,))],
    )(keep, swap(send))
    start = norm_left
    state = None
    for repeat in range(ITERS):
        inc = exchange(msg)
        if repeat == ITERS - 1:
            break
        if repeat == 0:
            msg, left, norm_right, high2, low2, high2_t, low2_t = call(
                first_user_kernel,
                [SMEM] * 2 + [VMEM] * 8,
                (msg_shape, left_shape, col8, terms, terms, terms, terms),
                (VMEM,) * 7,
                [LEFT, LEFTS2],
            )(*small(tab, tab2), inc, left, norm_left, *near(high, low, high_t, low_t, blocks2))
        else:
            msg, left, norm_right = call(
                user_kernel,
                [SMEM] * 2 + [VMEM] * 11,
                (msg_shape, left_shape, col8),
                None,
                [LEFT, LEFTS2],
            )(
                *small(tab, tab2), inc, left, norm_left,
                *near(high, low, high2, low2, high_t, low_t, high2_t, low2_t),
            )
        inc = exchange(msg)
        first = repeat == 0
        tail = (start,) if first else state
        outs = call(
            lambda *refs, first=first: send_kernel(first, *refs),
            [SMEM] * 2 + [VMEM] * (3 + len(tail)),
            (msg_shape, vec, col8, vec, vec, shape(4 * RHS, BS)),
            None,
            [pltpu.VMEM((VEC, BS), f32)] * 4,
        )(*small(cols0, cols1), inc, raw, norm_right, *tail)
        msg, raw, norm_left = outs[:3]
        state = outs[3:]
    ends = shape(ENDS, BS)
    rows, keep, send = call(
        last_user_kernel,
        [SMEM] * 2 + [VMEM] * 12,
        (shape(2 * OWNERS, BS), ends, ends),
        None,
        [LEFT] * 2,
    )(
        *small(tab, tab2), inc, left, norm_left, *near(high_t, low_t, high2_t, low2_t),
        raw, start, *state,
    )
    theirs = swap(send)
    rows = lax.all_to_all(rows, GRP_SHARD, 0, 0, tiled=True)
    full = shape(COLS_OWN * RHS, BS)
    sol, left, rel = call(final_kernel, [VMEM] * 3, (full, full, shape(RHS)))(rows, keep, theirs)

    def tall(x):
        return x.reshape(COLS_OWN, RHS, BS).transpose(0, 2, 1).reshape(COLS_OWN * BS, RHS)

    return tall(sol), tall(left), rel


def solution(mesh):
    torus = Mesh(
        mesh.devices.reshape(mesh.shape["grp"], 4, 4, 4), ("grp", "shard_0", "shard_1", "shard_2")
    )
    return jax.shard_map(
        on_device,
        mesh=torus,
        in_specs=(
            P(GRP_SHARD, None, None),
            P(GRP_SHARD),
            P(GRP_SHARD, None),
            P(GRP_SHARD),
            P(GRP_SHARD, None),
        ),
        out_specs=(P(SHARD, None), P(GRP_SHARD, None), P()),
        check_vma=False,
    )
```

```python
import jax
import jax.numpy as jnp
from jax import lax
from jax.experimental import pallas as pl
from jax.experimental.pallas import tpu as pltpu
from jax.sharding import Mesh
from jax.sharding import PartitionSpec as P

ITERS = 4
COLS_OWN = 16
SHARD = ("shard_0", "shard_1", "shard_2")
GRP_SHARD = ("grp", "shard_0", "shard_1", "shard_2")

OWNERS = 64
CAP = 2
BS = 128
RHS = 8
COUNT = 64
ROWS = 16
SLOTS = OWNERS * CAP
MSG = RHS * CAP + 1
TALL = OWNERS * MSG
CHUNK = 8
CHUNKS = COUNT // CHUNK
PART = RHS // 2
LINES = 2 * ROWS
VEC = COLS_OWN * PART
ENDS = 2 * VEC + 3 * RHS + ROWS * PART

f32 = jnp.float32
bf16 = jnp.bfloat16


def diag_mask():
    sub = lax.broadcasted_iota(jnp.int32, (RHS, BS), 0)
    lane = lax.broadcasted_iota(jnp.int32, (RHS, BS), 1)
    return sub == lane


def row_of(column):
    return jnp.sum(jnp.where(diag_mask(), column, 0.0), axis=0, keepdims=True)


def column_of(row):
    spread = jnp.broadcast_to(row, (RHS, BS))
    total = jnp.sum(jnp.where(diag_mask(), spread, 0.0), axis=1, keepdims=True)
    return jnp.broadcast_to(total, (RHS, BS))


def squares(values):
    cube = values.reshape(values.shape[0] // RHS, RHS, BS)
    total = jnp.sum(jnp.sum(cube * cube, axis=0), axis=1, keepdims=True)
    return jnp.broadcast_to(total, (RHS, BS))


def part_squares(values):
    cube = values.reshape(values.shape[0] // RHS, RHS, BS)
    total = jnp.sum(cube * cube, axis=0)
    total = total[:PART] + total[PART:]
    total = jnp.sum(jnp.concatenate([total, total], axis=0), axis=1, keepdims=True)
    return jnp.broadcast_to(total, (RHS, BS))


def part_mask(shift):
    sub = lax.broadcasted_iota(jnp.int32, (RHS, BS), 0)
    lane = lax.broadcasted_iota(jnp.int32, (RHS, BS), 1)
    return sub, lane, lane == jnp.where(sub < PART, sub, sub - PART) + shift


def part_row(column, shift=0):
    sub, _, mask = part_mask(shift)
    return jnp.sum(jnp.where(mask & (sub < PART), column, 0.0), axis=0, keepdims=True)


def part_column(row, shift=0):
    _, _, mask = part_mask(shift)
    spread = jnp.broadcast_to(row, (RHS, BS))
    total = jnp.sum(jnp.where(mask, spread, 0.0), axis=1, keepdims=True)
    return jnp.broadcast_to(total, (RHS, BS))


def tiled(column, count):
    return jnp.concatenate([column] * count, axis=0)


def sum_rows(ref, column_of):
    rows = [ref[pl.ds(MSG * o + MSG - 1, 1), :] for o in range(OWNERS)]
    while len(rows) > 1:
        rows = [rows[i] + rows[i + 1] for i in range(0, len(rows), 2)]
    return column_of(rows[0])


def put_rows(ref, row):
    for o in range(OWNERS):
        ref[pl.ds(MSG * o + MSG - 1, 1), :] = row


def split(x):
    high = x.astype(bf16)
    low = (x - high.astype(f32)).astype(bf16)
    return high, low


def stacked(x):
    high = x.astype(bf16).astype(f32)
    both = jnp.concatenate([high, x - high], axis=0).astype(bf16)
    return jnp.concatenate([both, both], axis=1)


def fold(out):
    half = out.shape[0] // 2
    return out[:half] + out[half:]


def chunk_copy(blocks, bbuf, sem, c):
    span = pl.ds(c * CHUNK, CHUNK)
    return pltpu.make_async_copy(blocks.at[span], bbuf.at[span], sem.at[c])


def split_left(us, left, height):
    for r in range(left.shape[0] // height):
        us[r] = stacked(left[r * height : (r + 1) * height])


def adjoint_block(pos, row, us, high, low, msg):
    rhs = jnp.concatenate([high, low], axis=0)
    out = lax.dot_general(us[row], rhs, (((1,), (0,)), ((), ())), preferred_element_type=f32)
    sent = fold(out)
    msg[pl.ds(pos, sent.shape[0]), :] = sent


def forward_block(piece, high, low):
    rhs = jnp.concatenate([high, low], axis=0)
    out = lax.dot_general(
        stacked(piece), rhs, (((1,), (0,)), ((), ())), preferred_element_type=f32
    )
    return fold(out)


def first_kernel(
    owner_in, row_in, col_in, right_in, blocks,
    msg, tab, line_row, high, low, high_t, low_t,
    bbuf, right, us, owner, row, col, taken, sem, little,
):
    loads = [
        pltpu.make_async_copy(owner_in, owner, little.at[0]),
        pltpu.make_async_copy(row_in, row, little.at[1]),
        pltpu.make_async_copy(col_in, col, little.at[2]),
        pltpu.make_async_copy(right_in, right, little.at[3]),
    ]
    for load in loads:
        load.start()

    def begin(c, carry):
        chunk_copy(blocks, bbuf, sem, c).start()
        return carry

    lax.fori_loop(0, CHUNKS, begin, 0)
    msg[...] = jnp.zeros((TALL, BS), f32)

    def clear(g, carry):
        for j in range(8):
            taken[g * 8 + j] = 0
        return carry

    lax.fori_loop(0, OWNERS // 8, clear, 0)
    for load in loads:
        load.wait()
    right_all = right[...]
    put_rows(msg, row_of(squares(right_all)))
    split_left(us, right_all, RHS)
    grp = lax.axis_index("grp")
    listed = jnp.zeros((1, BS), f32)
    lane = lax.broadcasted_iota(jnp.int32, (1, BS), 1)

    for c in range(CHUNKS):
        chunk_copy(blocks, bbuf, sem, c).wait()
        for k in range(c * CHUNK, (c + 1) * CHUNK):
            o = owner[k]
            rank = taken[o]
            taken[o] = rank + 1
            pos = o * MSG + rank * RHS
            line = row[k] & (ROWS - 1)
            place = o * MSG + grp * (CAP * PART) + rank * PART
            here = line + grp * ROWS
            tab[k] = place
            tab[COUNT + k] = here
            listed = jnp.where(lane == k, place.astype(f32), listed)
            listed = jnp.where(lane == COUNT + k, here.astype(f32), listed)
            span = pl.ds(o * MSG + MSG - 1, 1)
            msg[span, :] = jnp.where(lane == RHS + rank, col[k].astype(f32), msg[span, :])
            h, l = split(bbuf[k])
            high[k] = h
            low[k] = l
            adjoint_block(pos, line, us, h, l, msg)
            high_t[k] = h.T
            low_t[k] = l.T
    line_row[...] = jnp.broadcast_to(listed, (RHS, BS))


def first_owner_kernel(inc, right, line_row, keep, send, p0, p1, p2, p3, vcols, cols, sem):
    grp = lax.axis_index("grp")
    parts = (p0, p1, p2, p3)
    lane = lax.broadcasted_iota(jnp.int32, (1, BS), 1)
    pairs = [
        jnp.where(
            lane == o * CAP,
            inc[pl.ds(MSG * o + MSG - 1, 1), RHS : RHS + 1],
            jnp.where(lane == o * CAP + 1, inc[pl.ds(MSG * o + MSG - 1, 1), RHS + 1 : RHS + 2], 0.0),
        )
        for o in range(OWNERS)
    ]
    while len(pairs) > 1:
        pairs = [pairs[i] + pairs[i + 1] for i in range(0, len(pairs), 2)]
    vcols[...] = pairs[0][0].astype(jnp.int32)
    copy = pltpu.make_async_copy(vcols, cols, sem)
    copy.start()
    norm = sum_rows(inc, column_of)
    for ref in (keep, send):
        ref[pl.ds(VEC, RHS), :] = norm
        ref[pl.ds(VEC + RHS, 1), :] = pairs[0]
        ref[pl.ds(VEC + RHS + 1, 1), :] = line_row[pl.ds(0, 1), :]
        ref[pl.ds(VEC + RHS + 2, RHS - 2), :] = jnp.zeros((RHS - 2, BS), f32)
    for part in parts:
        part[...] = jnp.zeros((COLS_OWN * RHS, BS), f32)

    def halves(at, tile):
        first, second = tile[:PART], tile[PART:]
        keep[pl.ds(at, PART), :] = jnp.where(grp == 0, first, second)
        send[pl.ds(at, PART), :] = jnp.where(grp == 0, second, first)

    for r in range(ROWS):
        halves(VEC + 2 * RHS + r * PART, right[pl.ds(r * RHS, RHS), :])
    copy.wait()

    for o in range(OWNERS):
        for s in range(CAP):
            span = pl.ds(pl.multiple_of(cols[o * CAP + s] * RHS, RHS), RHS)
            part = parts[(2 * o + s) % len(parts)]
            part[span, :] = part[span, :] + inc[pl.ds(o * MSG + s * RHS, RHS), :]
    for c in range(COLS_OWN):
        span = pl.ds(c * RHS, RHS)
        halves(c * PART, (p0[span, :] + p1[span, :]) + (p2[span, :] + p3[span, :]))


def send_slots(cols, raw, msg):
    put_rows(msg, part_row(part_squares(raw[...])))
    for o in range(OWNERS):
        for s in range(2 * CAP):
            at = cols[s // CAP][o * CAP + s % CAP]
            msg[pl.ds(o * MSG + s * PART, PART), :] = raw[pl.ds(at, PART), :]


def first_send_kernel(
    keep, theirs,
    msg, raw, nleft, left, tab, cols0, cols1,
    vtab, vcols0, vcols1, sem,
):
    grp = lax.axis_index("grp")
    mine_cols = keep[pl.ds(VEC + RHS, 1), :]
    other_cols = theirs[pl.ds(VEC + RHS, 1), :]
    vtab[...] = theirs[pl.ds(VEC + RHS + 1, 1), :][0].astype(jnp.int32)
    vcols0[...] = jnp.where(grp == 0, mine_cols, other_cols)[0].astype(jnp.int32) * PART
    vcols1[...] = jnp.where(grp == 0, other_cols, mine_cols)[0].astype(jnp.int32) * PART
    copies = [
        pltpu.make_async_copy(vtab, tab, sem.at[0]),
        pltpu.make_async_copy(vcols0, cols0, sem.at[1]),
        pltpu.make_async_copy(vcols1, cols1, sem.at[2]),
    ]
    for copy in copies:
        copy.start()
    norm = jnp.sqrt(keep[pl.ds(VEC, RHS), :] + theirs[pl.ds(VEC, RHS), :])
    own = jnp.where(grp == 0, norm[:PART], norm[PART:])
    norm = jnp.concatenate([own, own], axis=0)
    nleft[...] = norm
    body = pl.ds(0, VEC)
    raw[...] = (keep[body, :] + theirs[body, :]) / tiled(norm, VEC // RHS)
    size = ROWS * PART
    tail = pl.ds(VEC + 2 * RHS, size)
    left[pl.ds(pl.multiple_of(grp * size, RHS), size), :] = keep[tail, :]
    left[pl.ds(pl.multiple_of((1 - grp) * size, RHS), size), :] = theirs[tail, :]
    for copy in copies:
        copy.wait()
    send_slots((cols0, cols1), raw, msg)


def send_kernel(first, cols0, cols1, inc, qprev, nright, *refs):
    parts = refs[-4:]
    if first:
        start, msg, raw, nleft, sol, search, scal = refs[:-4]
    else:
        sol_in, search_in, scal_in, msg, raw, nleft, sol, search, scal = refs[:-4]
    cols = (cols0, cols1)
    for part in parts:
        part[...] = jnp.zeros((VEC, BS), f32)

    for o in range(OWNERS):
        for s in range(2 * CAP):
            span = pl.ds(cols[s // CAP][o * CAP + s % CAP], PART)
            part = parts[s]
            part[span, :] = part[span, :] + inc[pl.ds(o * MSG + s * PART, PART), :]
    total = (parts[0][...] + parts[1][...]) + (parts[2][...] + parts[3][...])
    n = VEC // RHS
    norm_left = jnp.sqrt(sum_rows(inc, part_column))
    norm_right = nright[...]
    nleft[...] = norm_left
    vec = qprev[...] / tiled(norm_right, n)
    raw[...] = total / tiled(norm_left, n) - tiled(norm_left, n) * vec
    send_slots(cols, raw, msg)
    if first:
        old_search = vec
        diag_bar = norm_right
        residual = start[...]
        old_sol = jnp.zeros((VEC, BS), f32)
    else:
        radius = scal_in[pl.ds(0, RHS), :]
        cosine = scal_in[pl.ds(RHS, RHS), :]
        sine_term = scal_in[pl.ds(2 * RHS, RHS), :]
        residual = scal_in[pl.ds(3 * RHS, RHS), :]
        coupling = sine_term * norm_right
        old_search = vec - tiled(coupling / radius, n) * search_in[...]
        diag_bar = -cosine * norm_right
        old_sol = sol_in[...]
    radius = jnp.sqrt(diag_bar * diag_bar + norm_left * norm_left)
    cosine = diag_bar / radius
    sine_term = norm_left / radius
    sol[...] = old_sol + tiled(cosine * residual / radius, n) * old_search
    search[...] = old_search
    scal[pl.ds(0, RHS), :] = radius
    scal[pl.ds(RHS, RHS), :] = cosine
    scal[pl.ds(2 * RHS, RHS), :] = sine_term
    scal[pl.ds(3 * RHS, RHS), :] = sine_term * residual


def forward_all(tab, inc, high, low, into):
    for k in range(COUNT):
        part = forward_block(inc[pl.ds(tab[k], PART), :], high[k], low[k])
        span = pl.ds(tab[COUNT + k] * PART, PART)
        ref = into[k % 2]
        ref[span, :] = ref[span, :] + part


def adjoint_all(tab, us, high, low, msg):
    for k in range(COUNT):
        adjoint_block(tab[k], tab[COUNT + k], us, high[k], low[k], msg)


def left_of(lraw, other, uraw, nleft, norm_right):
    n = LINES * PART // RHS
    left = (lraw[...] + other[...]) / tiled(norm_right, n) - tiled(norm_right, n) * (
        uraw[...] / tiled(nleft[...], n)
    )
    lraw[...] = left
    return left


def first_user_kernel(
    tab, tab2, inc, uraw, nleft, high, low, high_t, low_t, blocks,
    msg, lraw, nright, high2, low2, high2_t, low2_t,
    other, us,
):
    norm_right = jnp.sqrt(sum_rows(inc, part_column))
    nright[...] = norm_right
    lraw[...] = jnp.zeros(lraw.shape, f32)
    other[...] = jnp.zeros(lraw.shape, f32)
    forward_all(tab, inc, high_t, low_t, (lraw, other))
    for k in range(COUNT):
        h, l = split(blocks[k])
        high2[k] = h
        low2[k] = l
        h, l = h.T, l.T
        high2_t[k] = h
        low2_t[k] = l
        part = forward_block(inc[pl.ds(tab2[k], PART), :], h, l)
        span = pl.ds(tab2[COUNT + k] * PART, PART)
        ref = other if k % 2 else lraw
        ref[span, :] = ref[span, :] + part
    left = left_of(lraw, other, uraw, nleft, norm_right)
    msg[...] = jnp.zeros((TALL, BS), f32)
    put_rows(msg, part_row(part_squares(left)))
    split_left(us, left, PART)
    adjoint_all(tab, us, high, low, msg)
    adjoint_all(tab2, us, high2, low2, msg)


def user_kernel(
    tab, tab2, inc, uraw, nleft, high, low, high2, low2, high_t, low_t, high2_t, low2_t,
    msg, lraw, nright, other, us,
):
    norm_right = jnp.sqrt(sum_rows(inc, part_column))
    nright[...] = norm_right
    lraw[...] = jnp.zeros(lraw.shape, f32)
    other[...] = jnp.zeros(lraw.shape, f32)
    forward_all(tab, inc, high_t, low_t, (lraw, other))
    forward_all(tab2, inc, high2_t, low2_t, (lraw, other))
    left = left_of(lraw, other, uraw, nleft, norm_right)
    msg[...] = jnp.zeros((TALL, BS), f32)
    put_rows(msg, part_row(part_squares(left)))
    split_left(us, left, PART)
    adjoint_all(tab, us, high, low, msg)
    adjoint_all(tab2, us, high2, low2, msg)


def last_user_kernel(
    tab, tab2, inc, uraw, nleft, high, low, high2, low2, qprev, start, sol_in, search_in, scal_in,
    msg, keep, send, lraw, other,
):
    grp = lax.axis_index("grp")
    norm_right = jnp.sqrt(sum_rows(inc, part_column))
    lraw[...] = jnp.zeros(lraw.shape, f32)
    other[...] = jnp.zeros(lraw.shape, f32)
    n = VEC // RHS
    radius = scal_in[pl.ds(0, RHS), :]
    cosine = scal_in[pl.ds(RHS, RHS), :]
    sine_term = scal_in[pl.ds(2 * RHS, RHS), :]
    vec = qprev[...] / tiled(norm_right, n)
    search = vec - tiled(sine_term * norm_right / radius, n) * search_in[...]
    for ref in (keep, send):
        ref[pl.ds(0, VEC), :] = sol_in[...]
        ref[pl.ds(VEC, VEC), :] = search
        ref[pl.ds(2 * VEC, RHS), :] = -cosine * norm_right
        ref[pl.ds(2 * VEC + RHS, RHS), :] = scal_in[pl.ds(3 * RHS, RHS), :]
        ref[pl.ds(2 * VEC + 2 * RHS, RHS), :] = start[...]
    forward_all(tab, inc, high, low, (lraw, other))
    forward_all(tab2, inc, high2, low2, (lraw, other))
    left = left_of(lraw, other, uraw, nleft, norm_right)
    row = part_row(part_squares(left), grp * PART)
    msg[...] = jnp.broadcast_to(row, msg.shape)
    size = ROWS * PART
    for ref, at in ((keep, grp), (send, 1 - grp)):
        ref[pl.ds(ENDS - size, size), :] = lraw[pl.ds(pl.multiple_of(at * size, RHS), size), :]


def finished(total, ref, grp):
    norm_left = jnp.sqrt(part_column(total, grp * PART))
    size = ROWS * PART
    left = ref[pl.ds(ENDS - size, size), :] / tiled(norm_left, size // RHS)
    diag_bar = ref[pl.ds(2 * VEC, RHS), :]
    residual = ref[pl.ds(2 * VEC + RHS, RHS), :]
    radius = jnp.sqrt(diag_bar * diag_bar + norm_left * norm_left)
    cosine = diag_bar / radius
    sine_term = norm_left / radius
    step = tiled(cosine * residual / radius, VEC // RHS)
    sol = ref[pl.ds(0, VEC), :] + step * ref[pl.ds(VEC, VEC), :]
    rel = sine_term * residual / ref[pl.ds(2 * VEC + 2 * RHS, RHS), :]
    return sol, left, rel


def final_kernel(rows, keep, theirs, sol, left, rel):
    grp = lax.axis_index("grp")
    total = jnp.sum(rows[...], axis=0, keepdims=True)
    mine = finished(total, keep, grp)
    other = finished(total, theirs, 1 - grp)

    def join(ref, mine, other):
        first = jnp.where(grp == 0, mine, other)
        second = jnp.where(grp == 0, other, mine)
        for c in range(mine.shape[0] // PART):
            ref[pl.ds(c * RHS, PART), :] = first[c * PART : (c + 1) * PART]
            ref[pl.ds(c * RHS + PART, PART), :] = second[c * PART : (c + 1) * PART]

    join(sol, mine[0], other[0])
    join(left, mine[1], other[1])
    first = jnp.where(grp == 0, mine[2], other[2])
    second = jnp.where(grp == 0, other[2], mine[2])
    both = jnp.concatenate([first[:PART], second[:PART]], axis=0)
    rel[...] = row_of(both)[0, :RHS]


def shape(*dims, dtype=f32):
    return jax.ShapeDtypeStruct(dims, dtype)


VMEM = pl.BlockSpec(memory_space=pltpu.VMEM)
SMEM = pl.BlockSpec(memory_space=pltpu.SMEM)
HBM = pl.BlockSpec(memory_space=pltpu.HBM)
PARTS = [pltpu.VMEM((COLS_OWN * RHS, BS), f32)] * 4
LEFTS = pltpu.VMEM((ROWS, 2 * RHS, 2 * BS), bf16)
LEFTS2 = pltpu.VMEM((LINES, RHS, 2 * BS), bf16)
LEFT = pltpu.VMEM((ROWS * RHS, BS), f32)
BUFFER = pltpu.VMEM((COUNT, BS, BS), f32)
SEMS = pltpu.SemaphoreType.DMA((CHUNKS,))
ONE = pltpu.SemaphoreType.DMA(())
LINE = pltpu.VMEM((SLOTS,), jnp.int32)


def call(body, ins, outs, specs_out=None, scratch=()):
    return pl.pallas_call(
        body,
        out_shape=outs,
        in_specs=ins,
        out_specs=specs_out or jax.tree.map(lambda _: VMEM, outs),
        scratch_shapes=scratch,
        compiler_params=pltpu.CompilerParams(vmem_limit_bytes=24 * 1024 * 1024),
    )


def exchange(msg):
    sent = msg.reshape(OWNERS, MSG * BS)
    return lax.all_to_all(sent, SHARD, 0, 0, tiled=True).reshape(TALL, BS)


def swap(half):
    return lax.ppermute(half, "grp", [(0, 1), (1, 0)])


def small(*xs):
    return [pltpu.with_memory_space_constraint(x, pltpu.SMEM) for x in xs]


def near(*xs):
    return [pltpu.with_memory_space_constraint(x, pltpu.VMEM) for x in xs]


def far(*xs):
    return [pltpu.with_memory_space_constraint(x, pltpu.HBM) for x in xs]


def on_device(blocks, block_row, block_owner, block_col, right_side):
    owner = block_owner[:, 0]
    right = right_side.reshape(ROWS, BS, RHS).transpose(0, 2, 1).reshape(ROWS * RHS, BS)
    left_shape = shape(LINES * PART, BS)
    vec = shape(VEC, BS)
    col8 = shape(RHS, BS)
    msg_shape = shape(TALL, BS)
    table = pltpu.MemorySpace.SMEM((SLOTS,), jnp.int32)
    terms = pltpu.MemorySpace.VMEM((COUNT, BS, BS), bf16)
    swapped = shape(VEC + 2 * RHS + ROWS * PART, BS)

    blocks2 = swap(blocks)
    msg, tab, line_row, high, low, high_t, low_t = call(
        first_kernel,
        [HBM] * 5,
        (msg_shape, table, col8, terms, terms, terms, terms),
        (VMEM, SMEM) + (VMEM,) * 5,
        [BUFFER, LEFT, LEFTS]
        + [pltpu.SMEM((COUNT,), jnp.int32)] * 4
        + [SEMS, pltpu.SemaphoreType.DMA((4,))],
    )(*far(owner, block_row, block_col, right, blocks))
    inc = exchange(msg)
    keep, send = call(
        first_owner_kernel,
        [VMEM] * 3,
        (swapped, swapped),
        None,
        PARTS + [LINE, pltpu.SMEM((SLOTS,), jnp.int32), ONE],
    )(inc, right, line_row)
    msg, raw, norm_left, left, tab2, cols0, cols1 = call(
        first_send_kernel,
        [VMEM] * 2,
        (msg_shape, vec, col8, left_shape, table, table, table),
        (VMEM,) * 4 + (SMEM,) * 3,
        [LINE] * 3 + [pltpu.SemaphoreType.DMA((3,))],
    )(keep, swap(send))
    start = norm_left
    state = None
    for repeat in range(ITERS):
        inc = exchange(msg)
        if repeat == ITERS - 1:
            break
        if repeat == 0:
            msg, left, norm_right, high2, low2, high2_t, low2_t = call(
                first_user_kernel,
                [SMEM] * 2 + [VMEM] * 8,
                (msg_shape, left_shape, col8, terms, terms, terms, terms),
                (VMEM,) * 7,
                [LEFT, LEFTS2],
            )(*small(tab, tab2), inc, left, norm_left, *near(high, low, high_t, low_t, blocks2))
        else:
            msg, left, norm_right = call(
                user_kernel,
                [SMEM] * 2 + [VMEM] * 11,
                (msg_shape, left_shape, col8),
                None,
                [LEFT, LEFTS2],
            )(
                *small(tab, tab2), inc, left, norm_left,
                *near(high, low, high2, low2, high_t, low_t, high2_t, low2_t),
            )
        inc = exchange(msg)
        first = repeat == 0
        tail = (start,) if first else state
        outs = call(
            lambda *refs, first=first: send_kernel(first, *refs),
            [SMEM] * 2 + [VMEM] * (3 + len(tail)),
            (msg_shape, vec, col8, vec, vec, shape(4 * RHS, BS)),
            None,
            [pltpu.VMEM((VEC, BS), f32)] * 4,
        )(*small(cols0, cols1), inc, raw, norm_right, *tail)
        msg, raw, norm_left = outs[:3]
        state = outs[3:]
    ends = shape(ENDS, BS)
    rows, keep, send = call(
        last_user_kernel,
        [SMEM] * 2 + [VMEM] * 12,
        (shape(2 * OWNERS, BS), ends, ends),
        None,
        [LEFT] * 2,
    )(
        *small(tab, tab2), inc, left, norm_left, *near(high_t, low_t, high2_t, low2_t),
        raw, start, *state,
    )
    theirs = swap(send)
    rows = lax.all_to_all(rows, GRP_SHARD, 0, 0, tiled=True)
    full = shape(COLS_OWN * RHS, BS)
    sol, left, rel = call(final_kernel, [VMEM] * 3, (full, full, shape(RHS)))(rows, keep, theirs)

    def tall(x):
        return x.reshape(COLS_OWN, RHS, BS).transpose(0, 2, 1).reshape(COLS_OWN * BS, RHS)

    return tall(sol), tall(left), rel


def solution(mesh):
    torus = Mesh(
        mesh.devices.reshape(mesh.shape["grp"], 4, 4, 4), ("grp", "shard_0", "shard_1", "shard_2")
    )
    return jax.shard_map(
        on_device,
        mesh=torus,
        in_specs=(
            P(GRP_SHARD, None, None),
            P(GRP_SHARD),
            P(GRP_SHARD, None),
            P(GRP_SHARD),
            P(GRP_SHARD, None),
        ),
        out_specs=(P(SHARD, None), P(GRP_SHARD, None), P()),
        check_vma=False,
    )
```

```python
import jax
import jax.numpy as jnp
from jax import lax
from jax.experimental import pallas as pl
from jax.experimental.pallas import tpu as pltpu
from jax.sharding import Mesh
from jax.sharding import PartitionSpec as P

ITERS = 4
COLS_OWN = 16
SHARD = ("shard_0", "shard_1", "shard_2")
GRP_SHARD = ("grp", "shard_0", "shard_1", "shard_2")

OWNERS = 64
CAP = 2
BS = 128
RHS = 8
COUNT = 64
ROWS = 16
SLOTS = OWNERS * CAP
MSG = RHS * CAP + 1
TALL = OWNERS * MSG
CHUNK = 16
CHUNKS = COUNT // CHUNK
PART = RHS // 2
LINES = 2 * ROWS
VEC = COLS_OWN * PART
ENDS = 2 * VEC + 3 * RHS + ROWS * PART

f32 = jnp.float32
bf16 = jnp.bfloat16


def diag_mask():
    sub = lax.broadcasted_iota(jnp.int32, (RHS, BS), 0)
    lane = lax.broadcasted_iota(jnp.int32, (RHS, BS), 1)
    return sub == lane


def row_of(column):
    return jnp.sum(jnp.where(diag_mask(), column, 0.0), axis=0, keepdims=True)


def column_of(row):
    spread = jnp.broadcast_to(row, (RHS, BS))
    total = jnp.sum(jnp.where(diag_mask(), spread, 0.0), axis=1, keepdims=True)
    return jnp.broadcast_to(total, (RHS, BS))


def squares(values):
    cube = values.reshape(values.shape[0] // RHS, RHS, BS)
    total = jnp.sum(jnp.sum(cube * cube, axis=0), axis=1, keepdims=True)
    return jnp.broadcast_to(total, (RHS, BS))


def part_squares(values):
    cube = values.reshape(values.shape[0] // RHS, RHS, BS)
    total = jnp.sum(cube * cube, axis=0)
    total = total[:PART] + total[PART:]
    total = jnp.sum(jnp.concatenate([total, total], axis=0), axis=1, keepdims=True)
    return jnp.broadcast_to(total, (RHS, BS))


def part_mask(shift):
    sub = lax.broadcasted_iota(jnp.int32, (RHS, BS), 0)
    lane = lax.broadcasted_iota(jnp.int32, (RHS, BS), 1)
    return sub, lane, lane == jnp.where(sub < PART, sub, sub - PART) + shift


def part_row(column, shift=0):
    sub, _, mask = part_mask(shift)
    return jnp.sum(jnp.where(mask & (sub < PART), column, 0.0), axis=0, keepdims=True)


def part_column(row, shift=0):
    _, _, mask = part_mask(shift)
    spread = jnp.broadcast_to(row, (RHS, BS))
    total = jnp.sum(jnp.where(mask, spread, 0.0), axis=1, keepdims=True)
    return jnp.broadcast_to(total, (RHS, BS))


def tiled(column, count):
    return jnp.concatenate([column] * count, axis=0)


def sum_rows(ref, column_of):
    rows = [ref[pl.ds(MSG * o + MSG - 1, 1), :] for o in range(OWNERS)]
    while len(rows) > 1:
        rows = [rows[i] + rows[i + 1] for i in range(0, len(rows), 2)]
    return column_of(rows[0])


def put_rows(ref, row):
    for o in range(OWNERS):
        ref[pl.ds(MSG * o + MSG - 1, 1), :] = row


def split(x):
    high = x.astype(bf16)
    low = (x - high.astype(f32)).astype(bf16)
    return high, low


def stacked(x):
    high = x.astype(bf16).astype(f32)
    both = jnp.concatenate([high, x - high], axis=0).astype(bf16)
    return jnp.concatenate([both, both], axis=1)


def fold(out):
    half = out.shape[0] // 2
    return out[:half] + out[half:]


def chunk_copy(blocks, bbuf, sem, c):
    span = pl.ds(c * CHUNK, CHUNK)
    return pltpu.make_async_copy(blocks.at[span], bbuf.at[span], sem.at[c])


def split_left(us, left, height):
    for r in range(left.shape[0] // height):
        us[r] = stacked(left[r * height : (r + 1) * height])


def adjoint_block(pos, row, us, high, low, msg):
    rhs = jnp.concatenate([high, low], axis=0)
    out = lax.dot_general(us[row], rhs, (((1,), (0,)), ((), ())), preferred_element_type=f32)
    sent = fold(out)
    msg[pl.ds(pos, sent.shape[0]), :] = sent


def forward_block(piece, high, low):
    rhs = jnp.concatenate([high, low], axis=0)
    out = lax.dot_general(
        stacked(piece), rhs, (((1,), (0,)), ((), ())), preferred_element_type=f32
    )
    return fold(out)


def first_kernel(
    owner_in, row_in, col_in, right_in, blocks,
    msg, tab, line_row, high, low, high_t, low_t,
    bbuf, right, us, owner, row, col, taken, sem, little,
):
    loads = [
        pltpu.make_async_copy(owner_in, owner, little.at[0]),
        pltpu.make_async_copy(row_in, row, little.at[1]),
        pltpu.make_async_copy(col_in, col, little.at[2]),
        pltpu.make_async_copy(right_in, right, little.at[3]),
    ]
    for load in loads:
        load.start()

    def begin(c, carry):
        chunk_copy(blocks, bbuf, sem, c).start()
        return carry

    lax.fori_loop(0, CHUNKS, begin, 0)
    msg[...] = jnp.zeros((TALL, BS), f32)

    def clear(g, carry):
        for j in range(8):
            taken[g * 8 + j] = 0
        return carry

    lax.fori_loop(0, OWNERS // 8, clear, 0)
    for load in loads:
        load.wait()
    right_all = right[...]
    put_rows(msg, row_of(squares(right_all)))
    split_left(us, right_all, RHS)
    grp = lax.axis_index("grp")
    listed = jnp.zeros((1, BS), f32)
    lane = lax.broadcasted_iota(jnp.int32, (1, BS), 1)

    for c in range(CHUNKS):
        chunk_copy(blocks, bbuf, sem, c).wait()
        for k in range(c * CHUNK, (c + 1) * CHUNK):
            o = owner[k]
            rank = taken[o]
            taken[o] = rank + 1
            pos = o * MSG + rank * RHS
            line = row[k] & (ROWS - 1)
            place = o * MSG + grp * (CAP * PART) + rank * PART
            here = line + grp * ROWS
            tab[k] = place
            tab[COUNT + k] = here
            listed = jnp.where(lane == k, place.astype(f32), listed)
            listed = jnp.where(lane == COUNT + k, here.astype(f32), listed)
            span = pl.ds(o * MSG + MSG - 1, 1)
            msg[span, :] = jnp.where(lane == RHS + rank, col[k].astype(f32), msg[span, :])
            h, l = split(bbuf[k])
            high[k] = h
            low[k] = l
            adjoint_block(pos, line, us, h, l, msg)
            high_t[k] = h.T
            low_t[k] = l.T
    line_row[...] = jnp.broadcast_to(listed, (RHS, BS))


def first_owner_kernel(inc, right, line_row, keep, send, p0, p1, p2, p3, vcols, cols, sem):
    grp = lax.axis_index("grp")
    parts = (p0, p1, p2, p3)
    lane = lax.broadcasted_iota(jnp.int32, (1, BS), 1)
    pairs = [
        jnp.where(
            lane == o * CAP,
            inc[pl.ds(MSG * o + MSG - 1, 1), RHS : RHS + 1],
            jnp.where(lane == o * CAP + 1, inc[pl.ds(MSG * o + MSG - 1, 1), RHS + 1 : RHS + 2], 0.0),
        )
        for o in range(OWNERS)
    ]
    while len(pairs) > 1:
        pairs = [pairs[i] + pairs[i + 1] for i in range(0, len(pairs), 2)]
    vcols[...] = pairs[0][0].astype(jnp.int32)
    copy = pltpu.make_async_copy(vcols, cols, sem)
    copy.start()
    norm = sum_rows(inc, column_of)
    for ref in (keep, send):
        ref[pl.ds(VEC, RHS), :] = norm
        ref[pl.ds(VEC + RHS, 1), :] = pairs[0]
        ref[pl.ds(VEC + RHS + 1, 1), :] = line_row[pl.ds(0, 1), :]
        ref[pl.ds(VEC + RHS + 2, RHS - 2), :] = jnp.zeros((RHS - 2, BS), f32)
    for part in parts:
        part[...] = jnp.zeros((COLS_OWN * RHS, BS), f32)

    def halves(at, tile):
        first, second = tile[:PART], tile[PART:]
        keep[pl.ds(at, PART), :] = jnp.where(grp == 0, first, second)
        send[pl.ds(at, PART), :] = jnp.where(grp == 0, second, first)

    for r in range(ROWS):
        halves(VEC + 2 * RHS + r * PART, right[pl.ds(r * RHS, RHS), :])
    copy.wait()

    for o in range(OWNERS):
        for s in range(CAP):
            span = pl.ds(pl.multiple_of(cols[o * CAP + s] * RHS, RHS), RHS)
            part = parts[(2 * o + s) % len(parts)]
            part[span, :] = part[span, :] + inc[pl.ds(o * MSG + s * RHS, RHS), :]
    for c in range(COLS_OWN):
        span = pl.ds(c * RHS, RHS)
        halves(c * PART, (p0[span, :] + p1[span, :]) + (p2[span, :] + p3[span, :]))


def send_slots(cols, raw, msg):
    put_rows(msg, part_row(part_squares(raw[...])))
    for o in range(OWNERS):
        for s in range(2 * CAP):
            at = cols[s // CAP][o * CAP + s % CAP]
            msg[pl.ds(o * MSG + s * PART, PART), :] = raw[pl.ds(at, PART), :]


def first_send_kernel(
    keep, theirs,
    msg, raw, nleft, left, tab, cols0, cols1,
    vtab, vcols0, vcols1, sem,
):
    grp = lax.axis_index("grp")
    mine_cols = keep[pl.ds(VEC + RHS, 1), :]
    other_cols = theirs[pl.ds(VEC + RHS, 1), :]
    vtab[...] = theirs[pl.ds(VEC + RHS + 1, 1), :][0].astype(jnp.int32)
    vcols0[...] = jnp.where(grp == 0, mine_cols, other_cols)[0].astype(jnp.int32) * PART
    vcols1[...] = jnp.where(grp == 0, other_cols, mine_cols)[0].astype(jnp.int32) * PART
    copies = [
        pltpu.make_async_copy(vtab, tab, sem.at[0]),
        pltpu.make_async_copy(vcols0, cols0, sem.at[1]),
        pltpu.make_async_copy(vcols1, cols1, sem.at[2]),
    ]
    for copy in copies:
        copy.start()
    norm = jnp.sqrt(keep[pl.ds(VEC, RHS), :] + theirs[pl.ds(VEC, RHS), :])
    own = jnp.where(grp == 0, norm[:PART], norm[PART:])
    norm = jnp.concatenate([own, own], axis=0)
    nleft[...] = norm
    body = pl.ds(0, VEC)
    raw[...] = (keep[body, :] + theirs[body, :]) / tiled(norm, VEC // RHS)
    size = ROWS * PART
    tail = pl.ds(VEC + 2 * RHS, size)
    left[pl.ds(pl.multiple_of(grp * size, RHS), size), :] = keep[tail, :]
    left[pl.ds(pl.multiple_of((1 - grp) * size, RHS), size), :] = theirs[tail, :]
    for copy in copies:
        copy.wait()
    send_slots((cols0, cols1), raw, msg)


def send_kernel(first, cols0, cols1, inc, qprev, nright, *refs):
    parts = refs[-4:]
    if first:
        start, msg, raw, nleft, sol, search, scal = refs[:-4]
    else:
        sol_in, search_in, scal_in, msg, raw, nleft, sol, search, scal = refs[:-4]
    cols = (cols0, cols1)
    for part in parts:
        part[...] = jnp.zeros((VEC, BS), f32)

    for o in range(OWNERS):
        for s in range(2 * CAP):
            span = pl.ds(cols[s // CAP][o * CAP + s % CAP], PART)
            part = parts[s]
            part[span, :] = part[span, :] + inc[pl.ds(o * MSG + s * PART, PART), :]
    total = (parts[0][...] + parts[1][...]) + (parts[2][...] + parts[3][...])
    n = VEC // RHS
    norm_left = jnp.sqrt(sum_rows(inc, part_column))
    norm_right = nright[...]
    nleft[...] = norm_left
    vec = qprev[...] / tiled(norm_right, n)
    raw[...] = total / tiled(norm_left, n) - tiled(norm_left, n) * vec
    send_slots(cols, raw, msg)
    if first:
        old_search = vec
        diag_bar = norm_right
        residual = start[...]
        old_sol = jnp.zeros((VEC, BS), f32)
    else:
        radius = scal_in[pl.ds(0, RHS), :]
        cosine = scal_in[pl.ds(RHS, RHS), :]
        sine_term = scal_in[pl.ds(2 * RHS, RHS), :]
        residual = scal_in[pl.ds(3 * RHS, RHS), :]
        coupling = sine_term * norm_right
        old_search = vec - tiled(coupling / radius, n) * search_in[...]
        diag_bar = -cosine * norm_right
        old_sol = sol_in[...]
    radius = jnp.sqrt(diag_bar * diag_bar + norm_left * norm_left)
    cosine = diag_bar / radius
    sine_term = norm_left / radius
    sol[...] = old_sol + tiled(cosine * residual / radius, n) * old_search
    search[...] = old_search
    scal[pl.ds(0, RHS), :] = radius
    scal[pl.ds(RHS, RHS), :] = cosine
    scal[pl.ds(2 * RHS, RHS), :] = sine_term
    scal[pl.ds(3 * RHS, RHS), :] = sine_term * residual


def forward_all(tab, inc, high, low, into):
    for k in range(COUNT):
        part = forward_block(inc[pl.ds(tab[k], PART), :], high[k], low[k])
        span = pl.ds(tab[COUNT + k] * PART, PART)
        ref = into[k % 2]
        ref[span, :] = ref[span, :] + part


def adjoint_all(tab, us, high, low, msg):
    for k in range(COUNT):
        adjoint_block(tab[k], tab[COUNT + k], us, high[k], low[k], msg)


def left_of(lraw, other, uraw, nleft, norm_right):
    n = LINES * PART // RHS
    left = (lraw[...] + other[...]) / tiled(norm_right, n) - tiled(norm_right, n) * (
        uraw[...] / tiled(nleft[...], n)
    )
    lraw[...] = left
    return left


def first_user_kernel(
    tab, tab2, inc, uraw, nleft, high, low, high_t, low_t, blocks,
    msg, lraw, nright, high2, low2, high2_t, low2_t,
    other, us,
):
    norm_right = jnp.sqrt(sum_rows(inc, part_column))
    nright[...] = norm_right
    lraw[...] = jnp.zeros(lraw.shape, f32)
    other[...] = jnp.zeros(lraw.shape, f32)
    forward_all(tab, inc, high_t, low_t, (lraw, other))
    for k in range(COUNT):
        h, l = split(blocks[k])
        high2[k] = h
        low2[k] = l
        h, l = h.T, l.T
        high2_t[k] = h
        low2_t[k] = l
        part = forward_block(inc[pl.ds(tab2[k], PART), :], h, l)
        span = pl.ds(tab2[COUNT + k] * PART, PART)
        ref = other if k % 2 else lraw
        ref[span, :] = ref[span, :] + part
    left = left_of(lraw, other, uraw, nleft, norm_right)
    msg[...] = jnp.zeros((TALL, BS), f32)
    put_rows(msg, part_row(part_squares(left)))
    split_left(us, left, PART)
    adjoint_all(tab, us, high, low, msg)
    adjoint_all(tab2, us, high2, low2, msg)


def user_kernel(
    tab, tab2, inc, uraw, nleft, high, low, high2, low2, high_t, low_t, high2_t, low2_t,
    msg, lraw, nright, other, us,
):
    norm_right = jnp.sqrt(sum_rows(inc, part_column))
    nright[...] = norm_right
    lraw[...] = jnp.zeros(lraw.shape, f32)
    other[...] = jnp.zeros(lraw.shape, f32)
    forward_all(tab, inc, high_t, low_t, (lraw, other))
    forward_all(tab2, inc, high2_t, low2_t, (lraw, other))
    left = left_of(lraw, other, uraw, nleft, norm_right)
    msg[...] = jnp.zeros((TALL, BS), f32)
    put_rows(msg, part_row(part_squares(left)))
    split_left(us, left, PART)
    adjoint_all(tab, us, high, low, msg)
    adjoint_all(tab2, us, high2, low2, msg)


def last_user_kernel(
    tab, tab2, inc, uraw, nleft, high, low, high2, low2, qprev, start, sol_in, search_in, scal_in,
    msg, keep, send, lraw, other,
):
    grp = lax.axis_index("grp")
    norm_right = jnp.sqrt(sum_rows(inc, part_column))
    lraw[...] = jnp.zeros(lraw.shape, f32)
    other[...] = jnp.zeros(lraw.shape, f32)
    n = VEC // RHS
    radius = scal_in[pl.ds(0, RHS), :]
    cosine = scal_in[pl.ds(RHS, RHS), :]
    sine_term = scal_in[pl.ds(2 * RHS, RHS), :]
    vec = qprev[...] / tiled(norm_right, n)
    search = vec - tiled(sine_term * norm_right / radius, n) * search_in[...]
    for ref in (keep, send):
        ref[pl.ds(0, VEC), :] = sol_in[...]
        ref[pl.ds(VEC, VEC), :] = search
        ref[pl.ds(2 * VEC, RHS), :] = -cosine * norm_right
        ref[pl.ds(2 * VEC + RHS, RHS), :] = scal_in[pl.ds(3 * RHS, RHS), :]
        ref[pl.ds(2 * VEC + 2 * RHS, RHS), :] = start[...]
    forward_all(tab, inc, high, low, (lraw, other))
    forward_all(tab2, inc, high2, low2, (lraw, other))
    left = left_of(lraw, other, uraw, nleft, norm_right)
    row = part_row(part_squares(left), grp * PART)
    msg[...] = jnp.broadcast_to(row, msg.shape)
    size = ROWS * PART
    for ref, at in ((keep, grp), (send, 1 - grp)):
        ref[pl.ds(ENDS - size, size), :] = lraw[pl.ds(pl.multiple_of(at * size, RHS), size), :]


def finished(total, ref, grp):
    norm_left = jnp.sqrt(part_column(total, grp * PART))
    size = ROWS * PART
    left = ref[pl.ds(ENDS - size, size), :] / tiled(norm_left, size // RHS)
    diag_bar = ref[pl.ds(2 * VEC, RHS), :]
    residual = ref[pl.ds(2 * VEC + RHS, RHS), :]
    radius = jnp.sqrt(diag_bar * diag_bar + norm_left * norm_left)
    cosine = diag_bar / radius
    sine_term = norm_left / radius
    step = tiled(cosine * residual / radius, VEC // RHS)
    sol = ref[pl.ds(0, VEC), :] + step * ref[pl.ds(VEC, VEC), :]
    rel = sine_term * residual / ref[pl.ds(2 * VEC + 2 * RHS, RHS), :]
    return sol, left, rel


def final_kernel(rows, keep, theirs, sol, left, rel):
    grp = lax.axis_index("grp")
    total = jnp.sum(rows[...], axis=0, keepdims=True)
    mine = finished(total, keep, grp)
    other = finished(total, theirs, 1 - grp)

    def join(ref, mine, other):
        first = jnp.where(grp == 0, mine, other)
        second = jnp.where(grp == 0, other, mine)
        for c in range(mine.shape[0] // PART):
            ref[pl.ds(c * RHS, PART), :] = first[c * PART : (c + 1) * PART]
            ref[pl.ds(c * RHS + PART, PART), :] = second[c * PART : (c + 1) * PART]

    join(sol, mine[0], other[0])
    join(left, mine[1], other[1])
    first = jnp.where(grp == 0, mine[2], other[2])
    second = jnp.where(grp == 0, other[2], mine[2])
    both = jnp.concatenate([first[:PART], second[:PART]], axis=0)
    rel[...] = row_of(both)[0, :RHS]


def shape(*dims, dtype=f32):
    return jax.ShapeDtypeStruct(dims, dtype)


VMEM = pl.BlockSpec(memory_space=pltpu.VMEM)
SMEM = pl.BlockSpec(memory_space=pltpu.SMEM)
HBM = pl.BlockSpec(memory_space=pltpu.HBM)
PARTS = [pltpu.VMEM((COLS_OWN * RHS, BS), f32)] * 4
LEFTS = pltpu.VMEM((ROWS, 2 * RHS, 2 * BS), bf16)
LEFTS2 = pltpu.VMEM((LINES, RHS, 2 * BS), bf16)
LEFT = pltpu.VMEM((ROWS * RHS, BS), f32)
BUFFER = pltpu.VMEM((COUNT, BS, BS), f32)
SEMS = pltpu.SemaphoreType.DMA((CHUNKS,))
ONE = pltpu.SemaphoreType.DMA(())
LINE = pltpu.VMEM((SLOTS,), jnp.int32)


def call(body, ins, outs, specs_out=None, scratch=()):
    return pl.pallas_call(
        body,
        out_shape=outs,
        in_specs=ins,
        out_specs=specs_out or jax.tree.map(lambda _: VMEM, outs),
        scratch_shapes=scratch,
        compiler_params=pltpu.CompilerParams(vmem_limit_bytes=24 * 1024 * 1024),
    )


def exchange(msg):
    sent = msg.reshape(OWNERS, MSG * BS)
    return lax.all_to_all(sent, SHARD, 0, 0, tiled=True).reshape(TALL, BS)


def swap(half):
    return lax.ppermute(half, "grp", [(0, 1), (1, 0)])


def small(*xs):
    return [pltpu.with_memory_space_constraint(x, pltpu.SMEM) for x in xs]


def near(*xs):
    return [pltpu.with_memory_space_constraint(x, pltpu.VMEM) for x in xs]


def far(*xs):
    return [pltpu.with_memory_space_constraint(x, pltpu.HBM) for x in xs]


def on_device(blocks, block_row, block_owner, block_col, right_side):
    owner = block_owner[:, 0]
    right = right_side.reshape(ROWS, BS, RHS).transpose(0, 2, 1).reshape(ROWS * RHS, BS)
    left_shape = shape(LINES * PART, BS)
    vec = shape(VEC, BS)
    col8 = shape(RHS, BS)
    msg_shape = shape(TALL, BS)
    table = pltpu.MemorySpace.SMEM((SLOTS,), jnp.int32)
    terms = pltpu.MemorySpace.VMEM((COUNT, BS, BS), bf16)
    swapped = shape(VEC + 2 * RHS + ROWS * PART, BS)

    blocks2 = swap(blocks)
    msg, tab, line_row, high, low, high_t, low_t = call(
        first_kernel,
        [HBM] * 5,
        (msg_shape, table, col8, terms, terms, terms, terms),
        (VMEM, SMEM) + (VMEM,) * 5,
        [BUFFER, LEFT, LEFTS]
        + [pltpu.SMEM((COUNT,), jnp.int32)] * 4
        + [SEMS, pltpu.SemaphoreType.DMA((4,))],
    )(*far(owner, block_row, block_col, right, blocks))
    inc = exchange(msg)
    keep, send = call(
        first_owner_kernel,
        [VMEM] * 3,
        (swapped, swapped),
        None,
        PARTS + [LINE, pltpu.SMEM((SLOTS,), jnp.int32), ONE],
    )(inc, right, line_row)
    msg, raw, norm_left, left, tab2, cols0, cols1 = call(
        first_send_kernel,
        [VMEM] * 2,
        (msg_shape, vec, col8, left_shape, table, table, table),
        (VMEM,) * 4 + (SMEM,) * 3,
        [LINE] * 3 + [pltpu.SemaphoreType.DMA((3,))],
    )(keep, swap(send))
    start = norm_left
    state = None
    for repeat in range(ITERS):
        inc = exchange(msg)
        if repeat == ITERS - 1:
            break
        if repeat == 0:
            msg, left, norm_right, high2, low2, high2_t, low2_t = call(
                first_user_kernel,
                [SMEM] * 2 + [VMEM] * 8,
                (msg_shape, left_shape, col8, terms, terms, terms, terms),
                (VMEM,) * 7,
                [LEFT, LEFTS2],
            )(*small(tab, tab2), inc, left, norm_left, *near(high, low, high_t, low_t, blocks2))
        else:
            msg, left, norm_right = call(
                user_kernel,
                [SMEM] * 2 + [VMEM] * 11,
                (msg_shape, left_shape, col8),
                None,
                [LEFT, LEFTS2],
            )(
                *small(tab, tab2), inc, left, norm_left,
                *near(high, low, high2, low2, high_t, low_t, high2_t, low2_t),
            )
        inc = exchange(msg)
        first = repeat == 0
        tail = (start,) if first else state
        outs = call(
            lambda *refs, first=first: send_kernel(first, *refs),
            [SMEM] * 2 + [VMEM] * (3 + len(tail)),
            (msg_shape, vec, col8, vec, vec, shape(4 * RHS, BS)),
            None,
            [pltpu.VMEM((VEC, BS), f32)] * 4,
        )(*small(cols0, cols1), inc, raw, norm_right, *tail)
        msg, raw, norm_left = outs[:3]
        state = outs[3:]
    ends = shape(ENDS, BS)
    rows, keep, send = call(
        last_user_kernel,
        [SMEM] * 2 + [VMEM] * 12,
        (shape(2 * OWNERS, BS), ends, ends),
        None,
        [LEFT] * 2,
    )(
        *small(tab, tab2), inc, left, norm_left, *near(high_t, low_t, high2_t, low2_t),
        raw, start, *state,
    )
    theirs = swap(send)
    rows = lax.all_to_all(rows, GRP_SHARD, 0, 0, tiled=True)
    full = shape(COLS_OWN * RHS, BS)
    sol, left, rel = call(final_kernel, [VMEM] * 3, (full, full, shape(RHS)))(rows, keep, theirs)

    def tall(x):
        return x.reshape(COLS_OWN, RHS, BS).transpose(0, 2, 1).reshape(COLS_OWN * BS, RHS)

    return tall(sol), tall(left), rel


def solution(mesh):
    torus = Mesh(
        mesh.devices.reshape(mesh.shape["grp"], 4, 4, 4), ("grp", "shard_0", "shard_1", "shard_2")
    )
    return jax.shard_map(
        on_device,
        mesh=torus,
        in_specs=(
            P(GRP_SHARD, None, None),
            P(GRP_SHARD),
            P(GRP_SHARD, None),
            P(GRP_SHARD),
            P(GRP_SHARD, None),
        ),
        out_specs=(P(SHARD, None), P(GRP_SHARD, None), P()),
        check_vma=False,
    )
```

```python
import jax
import jax.numpy as jnp
from jax import lax
from jax.experimental import pallas as pl
from jax.experimental.pallas import tpu as pltpu
from jax.sharding import Mesh
from jax.sharding import PartitionSpec as P

ITERS = 4
COLS_OWN = 16
SHARD = ("shard_0", "shard_1", "shard_2")
GRP_SHARD = ("grp", "shard_0", "shard_1", "shard_2")

OWNERS = 64
CAP = 2
BS = 128
RHS = 8
COUNT = 64
ROWS = 16
SLOTS = OWNERS * CAP
MSG = RHS * CAP + 1
TALL = OWNERS * MSG
CHUNK = 8
CHUNKS = COUNT // CHUNK
PART = RHS // 2
LINES = 2 * ROWS
VEC = COLS_OWN * PART
ENDS = 2 * VEC + 3 * RHS + ROWS * PART

f32 = jnp.float32
bf16 = jnp.bfloat16


def diag_mask():
    sub = lax.broadcasted_iota(jnp.int32, (RHS, BS), 0)
    lane = lax.broadcasted_iota(jnp.int32, (RHS, BS), 1)
    return sub == lane


def row_of(column):
    return jnp.sum(jnp.where(diag_mask(), column, 0.0), axis=0, keepdims=True)


def column_of(row):
    spread = jnp.broadcast_to(row, (RHS, BS))
    total = jnp.sum(jnp.where(diag_mask(), spread, 0.0), axis=1, keepdims=True)
    return jnp.broadcast_to(total, (RHS, BS))


def squares(values):
    cube = values.reshape(values.shape[0] // RHS, RHS, BS)
    total = jnp.sum(jnp.sum(cube * cube, axis=0), axis=1, keepdims=True)
    return jnp.broadcast_to(total, (RHS, BS))


def part_squares(values):
    cube = values.reshape(values.shape[0] // RHS, RHS, BS)
    total = jnp.sum(cube * cube, axis=0)
    total = total[:PART] + total[PART:]
    total = jnp.sum(jnp.concatenate([total, total], axis=0), axis=1, keepdims=True)
    return jnp.broadcast_to(total, (RHS, BS))


def part_mask(shift):
    sub = lax.broadcasted_iota(jnp.int32, (RHS, BS), 0)
    lane = lax.broadcasted_iota(jnp.int32, (RHS, BS), 1)
    return sub, lane, lane == jnp.where(sub < PART, sub, sub - PART) + shift


def part_row(column, shift=0):
    sub, _, mask = part_mask(shift)
    return jnp.sum(jnp.where(mask & (sub < PART), column, 0.0), axis=0, keepdims=True)


def part_column(row, shift=0):
    _, _, mask = part_mask(shift)
    spread = jnp.broadcast_to(row, (RHS, BS))
    total = jnp.sum(jnp.where(mask, spread, 0.0), axis=1, keepdims=True)
    return jnp.broadcast_to(total, (RHS, BS))


def tiled(column, count):
    return jnp.concatenate([column] * count, axis=0)


def sum_rows(ref, column_of):
    rows = [ref[pl.ds(MSG * o + MSG - 1, 1), :] for o in range(OWNERS)]
    while len(rows) > 1:
        rows = [rows[i] + rows[i + 1] for i in range(0, len(rows), 2)]
    return column_of(rows[0])


def put_rows(ref, row):
    for o in range(OWNERS):
        ref[pl.ds(MSG * o + MSG - 1, 1), :] = row


def split(x):
    high = x.astype(bf16)
    low = (x - high.astype(f32)).astype(bf16)
    return high, low


def stacked(x):
    high = x.astype(bf16).astype(f32)
    both = jnp.concatenate([high, x - high], axis=0).astype(bf16)
    return jnp.concatenate([both, both], axis=1)


def fold(out):
    half = out.shape[0] // 2
    return out[:half] + out[half:]


def chunk_copy(blocks, bbuf, sem, c):
    span = pl.ds(c * CHUNK, CHUNK)
    return pltpu.make_async_copy(blocks.at[span], bbuf.at[span], sem.at[c])


def split_left(us, left, height):
    for r in range(left.shape[0] // height):
        us[r] = stacked(left[r * height : (r + 1) * height])


def adjoint_block(pos, row, us, high, low, msg):
    rhs = jnp.concatenate([high, low], axis=0)
    out = lax.dot_general(us[row], rhs, (((1,), (0,)), ((), ())), preferred_element_type=f32)
    sent = fold(out)
    msg[pl.ds(pos, sent.shape[0]), :] = sent


def forward_block(piece, high, low):
    rhs = jnp.concatenate([high, low], axis=0)
    out = lax.dot_general(
        stacked(piece), rhs, (((1,), (0,)), ((), ())), preferred_element_type=f32
    )
    return fold(out)


def first_kernel(
    owner_in, row_in, col_in, right_in, blocks,
    msg, tab, line_row, high, low, high_t, low_t,
    bbuf, right, us, owner, row, col, taken, sem, little,
):
    loads = [
        pltpu.make_async_copy(owner_in, owner, little.at[0]),
        pltpu.make_async_copy(row_in, row, little.at[1]),
        pltpu.make_async_copy(col_in, col, little.at[2]),
        pltpu.make_async_copy(right_in, right, little.at[3]),
    ]
    for load in loads:
        load.start()

    def begin(c, carry):
        chunk_copy(blocks, bbuf, sem, c).start()
        return carry

    lax.fori_loop(0, CHUNKS, begin, 0)
    msg[...] = jnp.zeros((TALL, BS), f32)

    def clear(g, carry):
        for j in range(8):
            taken[g * 8 + j] = 0
        return carry

    lax.fori_loop(0, OWNERS // 8, clear, 0)
    for load in loads:
        load.wait()
    right_all = right[...]
    put_rows(msg, row_of(squares(right_all)))
    split_left(us, right_all, RHS)
    grp = lax.axis_index("grp")
    listed = jnp.zeros((1, BS), f32)
    lane = lax.broadcasted_iota(jnp.int32, (1, BS), 1)

    for c in range(CHUNKS):
        chunk_copy(blocks, bbuf, sem, c).wait()
        for k in range(c * CHUNK, (c + 1) * CHUNK):
            o = owner[k]
            rank = taken[o]
            taken[o] = rank + 1
            pos = o * MSG + rank * RHS
            line = row[k] & (ROWS - 1)
            place = o * MSG + grp * (CAP * PART) + rank * PART
            here = line + grp * ROWS
            tab[k] = place
            tab[COUNT + k] = here
            listed = jnp.where(lane == k, place.astype(f32), listed)
            listed = jnp.where(lane == COUNT + k, here.astype(f32), listed)
            span = pl.ds(o * MSG + MSG - 1, 1)
            msg[span, :] = jnp.where(lane == RHS + rank, col[k].astype(f32), msg[span, :])
            h, l = split(bbuf[k])
            high[k] = h
            low[k] = l
            adjoint_block(pos, line, us, h, l, msg)
            high_t[k] = h.T
            low_t[k] = l.T
    line_row[...] = jnp.broadcast_to(listed, (RHS, BS))


def first_owner_kernel(inc, right, line_row, keep, send, p0, p1, p2, p3, vcols, cols, sem):
    grp = lax.axis_index("grp")
    parts = (p0, p1, p2, p3)
    lane = lax.broadcasted_iota(jnp.int32, (1, BS), 1)
    pairs = [
        jnp.where(
            lane == o * CAP,
            inc[pl.ds(MSG * o + MSG - 1, 1), RHS : RHS + 1],
            jnp.where(lane == o * CAP + 1, inc[pl.ds(MSG * o + MSG - 1, 1), RHS + 1 : RHS + 2], 0.0),
        )
        for o in range(OWNERS)
    ]
    while len(pairs) > 1:
        pairs = [pairs[i] + pairs[i + 1] for i in range(0, len(pairs), 2)]
    vcols[...] = pairs[0][0].astype(jnp.int32)
    copy = pltpu.make_async_copy(vcols, cols, sem)
    copy.start()
    norm = sum_rows(inc, column_of)
    for ref in (keep, send):
        ref[pl.ds(VEC, RHS), :] = norm
        ref[pl.ds(VEC + RHS, 1), :] = pairs[0]
        ref[pl.ds(VEC + RHS + 1, 1), :] = line_row[pl.ds(0, 1), :]
        ref[pl.ds(VEC + RHS + 2, RHS - 2), :] = jnp.zeros((RHS - 2, BS), f32)
    for part in parts:
        part[...] = jnp.zeros((COLS_OWN * RHS, BS), f32)

    def halves(at, tile):
        first, second = tile[:PART], tile[PART:]
        keep[pl.ds(at, PART), :] = jnp.where(grp == 0, first, second)
        send[pl.ds(at, PART), :] = jnp.where(grp == 0, second, first)

    for r in range(ROWS):
        halves(VEC + 2 * RHS + r * PART, right[pl.ds(r * RHS, RHS), :])
    copy.wait()

    for o in range(OWNERS):
        for s in range(CAP):
            span = pl.ds(pl.multiple_of(cols[o * CAP + s] * RHS, RHS), RHS)
            part = parts[(2 * o + s) % len(parts)]
            part[span, :] = part[span, :] + inc[pl.ds(o * MSG + s * RHS, RHS), :]
    for c in range(COLS_OWN):
        span = pl.ds(c * RHS, RHS)
        halves(c * PART, (p0[span, :] + p1[span, :]) + (p2[span, :] + p3[span, :]))


def send_slots(cols, raw, msg):
    put_rows(msg, part_row(part_squares(raw[...])))
    for o in range(OWNERS):
        for s in range(2 * CAP):
            at = cols[s // CAP][o * CAP + s % CAP]
            msg[pl.ds(o * MSG + s * PART, PART), :] = raw[pl.ds(at, PART), :]


def first_send_kernel(
    keep, theirs,
    msg, raw, nleft, left, tab, cols0, cols1,
    vtab, vcols0, vcols1, sem,
):
    grp = lax.axis_index("grp")
    mine_cols = keep[pl.ds(VEC + RHS, 1), :]
    other_cols = theirs[pl.ds(VEC + RHS, 1), :]
    vtab[...] = theirs[pl.ds(VEC + RHS + 1, 1), :][0].astype(jnp.int32)
    vcols0[...] = jnp.where(grp == 0, mine_cols, other_cols)[0].astype(jnp.int32) * PART
    vcols1[...] = jnp.where(grp == 0, other_cols, mine_cols)[0].astype(jnp.int32) * PART
    copies = [
        pltpu.make_async_copy(vtab, tab, sem.at[0]),
        pltpu.make_async_copy(vcols0, cols0, sem.at[1]),
        pltpu.make_async_copy(vcols1, cols1, sem.at[2]),
    ]
    for copy in copies:
        copy.start()
    norm = jnp.sqrt(keep[pl.ds(VEC, RHS), :] + theirs[pl.ds(VEC, RHS), :])
    own = jnp.where(grp == 0, norm[:PART], norm[PART:])
    norm = jnp.concatenate([own, own], axis=0)
    nleft[...] = norm
    body = pl.ds(0, VEC)
    raw[...] = (keep[body, :] + theirs[body, :]) / tiled(norm, VEC // RHS)
    size = ROWS * PART
    tail = pl.ds(VEC + 2 * RHS, size)
    left[pl.ds(pl.multiple_of(grp * size, RHS), size), :] = keep[tail, :]
    left[pl.ds(pl.multiple_of((1 - grp) * size, RHS), size), :] = theirs[tail, :]
    for copy in copies:
        copy.wait()
    send_slots((cols0, cols1), raw, msg)


def send_kernel(first, cols0, cols1, inc, qprev, nright, *refs):
    parts = refs[-4:]
    if first:
        start, msg, raw, nleft, sol, search, scal = refs[:-4]
    else:
        sol_in, search_in, scal_in, msg, raw, nleft, sol, search, scal = refs[:-4]
    cols = (cols0, cols1)
    for part in parts:
        part[...] = jnp.zeros((VEC, BS), f32)

    for o in range(OWNERS):
        for s in range(2 * CAP):
            span = pl.ds(cols[s // CAP][o * CAP + s % CAP], PART)
            part = parts[s]
            part[span, :] = part[span, :] + inc[pl.ds(o * MSG + s * PART, PART), :]
    total = (parts[0][...] + parts[1][...]) + (parts[2][...] + parts[3][...])
    n = VEC // RHS
    norm_left = jnp.sqrt(sum_rows(inc, part_column))
    norm_right = nright[...]
    nleft[...] = norm_left
    vec = qprev[...] / tiled(norm_right, n)
    raw[...] = total / tiled(norm_left, n) - tiled(norm_left, n) * vec
    send_slots(cols, raw, msg)
    if first:
        old_search = vec
        diag_bar = norm_right
        residual = start[...]
        old_sol = jnp.zeros((VEC, BS), f32)
    else:
        radius = scal_in[pl.ds(0, RHS), :]
        cosine = scal_in[pl.ds(RHS, RHS), :]
        sine_term = scal_in[pl.ds(2 * RHS, RHS), :]
        residual = scal_in[pl.ds(3 * RHS, RHS), :]
        coupling = sine_term * norm_right
        old_search = vec - tiled(coupling / radius, n) * search_in[...]
        diag_bar = -cosine * norm_right
        old_sol = sol_in[...]
    radius = jnp.sqrt(diag_bar * diag_bar + norm_left * norm_left)
    cosine = diag_bar / radius
    sine_term = norm_left / radius
    sol[...] = old_sol + tiled(cosine * residual / radius, n) * old_search
    search[...] = old_search
    scal[pl.ds(0, RHS), :] = radius
    scal[pl.ds(RHS, RHS), :] = cosine
    scal[pl.ds(2 * RHS, RHS), :] = sine_term
    scal[pl.ds(3 * RHS, RHS), :] = sine_term * residual


def forward_all(tab, inc, high, low, into):
    for k in range(COUNT):
        part = forward_block(inc[pl.ds(tab[k], PART), :], high[k], low[k])
        span = pl.ds(tab[COUNT + k] * PART, PART)
        ref = into[k % 2]
        ref[span, :] = ref[span, :] + part


def adjoint_all(tab, us, high, low, msg):
    for k in range(COUNT):
        adjoint_block(tab[k], tab[COUNT + k], us, high[k], low[k], msg)


def left_of(lraw, other, uraw, nleft, norm_right):
    n = LINES * PART // RHS
    left = (lraw[...] + other[...]) / tiled(norm_right, n) - tiled(norm_right, n) * (
        uraw[...] / tiled(nleft[...], n)
    )
    lraw[...] = left
    return left


def first_user_kernel(
    tab, tab2, inc, uraw, nleft, high, low, high_t, low_t, blocks,
    msg, lraw, nright, high2, low2, high2_t, low2_t,
    other, us,
):
    norm_right = jnp.sqrt(sum_rows(inc, part_column))
    nright[...] = norm_right
    msg[...] = jnp.zeros((TALL, BS), f32)
    lraw[...] = jnp.zeros(lraw.shape, f32)
    other[...] = jnp.zeros(lraw.shape, f32)
    forward_all(tab, inc, high_t, low_t, (lraw, other))
    for k in range(COUNT):
        h, l = split(blocks[k])
        high2[k] = h
        low2[k] = l
        h, l = h.T, l.T
        high2_t[k] = h
        low2_t[k] = l
        part = forward_block(inc[pl.ds(tab2[k], PART), :], h, l)
        span = pl.ds(tab2[COUNT + k] * PART, PART)
        ref = other if k % 2 else lraw
        ref[span, :] = ref[span, :] + part
    left = left_of(lraw, other, uraw, nleft, norm_right)
    put_rows(msg, part_row(part_squares(left)))
    split_left(us, left, PART)
    adjoint_all(tab, us, high, low, msg)
    adjoint_all(tab2, us, high2, low2, msg)


def user_kernel(
    tab, tab2, inc, uraw, nleft, high, low, high2, low2, high_t, low_t, high2_t, low2_t,
    msg, lraw, nright, other, us,
):
    norm_right = jnp.sqrt(sum_rows(inc, part_column))
    nright[...] = norm_right
    msg[...] = jnp.zeros((TALL, BS), f32)
    lraw[...] = jnp.zeros(lraw.shape, f32)
    other[...] = jnp.zeros(lraw.shape, f32)
    forward_all(tab, inc, high_t, low_t, (lraw, other))
    forward_all(tab2, inc, high2_t, low2_t, (lraw, other))
    left = left_of(lraw, other, uraw, nleft, norm_right)
    put_rows(msg, part_row(part_squares(left)))
    split_left(us, left, PART)
    adjoint_all(tab, us, high, low, msg)
    adjoint_all(tab2, us, high2, low2, msg)


def last_user_kernel(
    tab, tab2, inc, uraw, nleft, high, low, high2, low2, qprev, start, sol_in, search_in, scal_in,
    msg, keep, send, lraw, other,
):
    grp = lax.axis_index("grp")
    norm_right = jnp.sqrt(sum_rows(inc, part_column))
    lraw[...] = jnp.zeros(lraw.shape, f32)
    other[...] = jnp.zeros(lraw.shape, f32)
    n = VEC // RHS
    radius = scal_in[pl.ds(0, RHS), :]
    cosine = scal_in[pl.ds(RHS, RHS), :]
    sine_term = scal_in[pl.ds(2 * RHS, RHS), :]
    vec = qprev[...] / tiled(norm_right, n)
    search = vec - tiled(sine_term * norm_right / radius, n) * search_in[...]
    for ref in (keep, send):
        ref[pl.ds(0, VEC), :] = sol_in[...]
        ref[pl.ds(VEC, VEC), :] = search
        ref[pl.ds(2 * VEC, RHS), :] = -cosine * norm_right
        ref[pl.ds(2 * VEC + RHS, RHS), :] = scal_in[pl.ds(3 * RHS, RHS), :]
        ref[pl.ds(2 * VEC + 2 * RHS, RHS), :] = start[...]
    forward_all(tab, inc, high, low, (lraw, other))
    forward_all(tab2, inc, high2, low2, (lraw, other))
    left = left_of(lraw, other, uraw, nleft, norm_right)
    row = part_row(part_squares(left), grp * PART)
    msg[...] = jnp.broadcast_to(row, msg.shape)
    size = ROWS * PART
    for ref, at in ((keep, grp), (send, 1 - grp)):
        ref[pl.ds(ENDS - size, size), :] = lraw[pl.ds(pl.multiple_of(at * size, RHS), size), :]


def finished(total, ref, grp):
    norm_left = jnp.sqrt(part_column(total, grp * PART))
    size = ROWS * PART
    left = ref[pl.ds(ENDS - size, size), :] / tiled(norm_left, size // RHS)
    diag_bar = ref[pl.ds(2 * VEC, RHS), :]
    residual = ref[pl.ds(2 * VEC + RHS, RHS), :]
    radius = jnp.sqrt(diag_bar * diag_bar + norm_left * norm_left)
    cosine = diag_bar / radius
    sine_term = norm_left / radius
    step = tiled(cosine * residual / radius, VEC // RHS)
    sol = ref[pl.ds(0, VEC), :] + step * ref[pl.ds(VEC, VEC), :]
    rel = sine_term * residual / ref[pl.ds(2 * VEC + 2 * RHS, RHS), :]
    return sol, left, rel


def final_kernel(rows, keep, theirs, sol, left, rel):
    grp = lax.axis_index("grp")
    total = jnp.sum(rows[...], axis=0, keepdims=True)
    mine = finished(total, keep, grp)
    other = finished(total, theirs, 1 - grp)

    def join(ref, mine, other):
        first = jnp.where(grp == 0, mine, other)
        second = jnp.where(grp == 0, other, mine)
        for c in range(mine.shape[0] // PART):
            ref[pl.ds(c * RHS, PART), :] = first[c * PART : (c + 1) * PART]
            ref[pl.ds(c * RHS + PART, PART), :] = second[c * PART : (c + 1) * PART]

    join(sol, mine[0], other[0])
    join(left, mine[1], other[1])
    first = jnp.where(grp == 0, mine[2], other[2])
    second = jnp.where(grp == 0, other[2], mine[2])
    both = jnp.concatenate([first[:PART], second[:PART]], axis=0)
    rel[...] = row_of(both)[0, :RHS]


def shape(*dims, dtype=f32):
    return jax.ShapeDtypeStruct(dims, dtype)


VMEM = pl.BlockSpec(memory_space=pltpu.VMEM)
SMEM = pl.BlockSpec(memory_space=pltpu.SMEM)
HBM = pl.BlockSpec(memory_space=pltpu.HBM)
PARTS = [pltpu.VMEM((COLS_OWN * RHS, BS), f32)] * 4
LEFTS = pltpu.VMEM((ROWS, 2 * RHS, 2 * BS), bf16)
LEFTS2 = pltpu.VMEM((LINES, RHS, 2 * BS), bf16)
LEFT = pltpu.VMEM((ROWS * RHS, BS), f32)
BUFFER = pltpu.VMEM((COUNT, BS, BS), f32)
SEMS = pltpu.SemaphoreType.DMA((CHUNKS,))
ONE = pltpu.SemaphoreType.DMA(())
LINE = pltpu.VMEM((SLOTS,), jnp.int32)


def call(body, ins, outs, specs_out=None, scratch=()):
    return pl.pallas_call(
        body,
        out_shape=outs,
        in_specs=ins,
        out_specs=specs_out or jax.tree.map(lambda _: VMEM, outs),
        scratch_shapes=scratch,
        compiler_params=pltpu.CompilerParams(vmem_limit_bytes=24 * 1024 * 1024),
    )


def exchange(msg):
    sent = msg.reshape(OWNERS, MSG * BS)
    return lax.all_to_all(sent, SHARD, 0, 0, tiled=True).reshape(TALL, BS)


def swap(half):
    return lax.ppermute(half, "grp", [(0, 1), (1, 0)])


def small(*xs):
    return [pltpu.with_memory_space_constraint(x, pltpu.SMEM) for x in xs]


def near(*xs):
    return [pltpu.with_memory_space_constraint(x, pltpu.VMEM) for x in xs]


def far(*xs):
    return [pltpu.with_memory_space_constraint(x, pltpu.HBM) for x in xs]


def on_device(blocks, block_row, block_owner, block_col, right_side):
    owner = block_owner[:, 0]
    right = right_side.reshape(ROWS, BS, RHS).transpose(0, 2, 1).reshape(ROWS * RHS, BS)
    left_shape = shape(LINES * PART, BS)
    vec = shape(VEC, BS)
    col8 = shape(RHS, BS)
    msg_shape = shape(TALL, BS)
    table = pltpu.MemorySpace.SMEM((SLOTS,), jnp.int32)
    terms = pltpu.MemorySpace.VMEM((COUNT, BS, BS), bf16)
    swapped = shape(VEC + 2 * RHS + ROWS * PART, BS)

    blocks2 = swap(blocks)
    msg, tab, line_row, high, low, high_t, low_t = call(
        first_kernel,
        [HBM] * 5,
        (msg_shape, table, col8, terms, terms, terms, terms),
        (VMEM, SMEM) + (VMEM,) * 5,
        [BUFFER, LEFT, LEFTS]
        + [pltpu.SMEM((COUNT,), jnp.int32)] * 4
        + [SEMS, pltpu.SemaphoreType.DMA((4,))],
    )(*far(owner, block_row, block_col, right, blocks))
    inc = exchange(msg)
    keep, send = call(
        first_owner_kernel,
        [VMEM] * 3,
        (swapped, swapped),
        None,
        PARTS + [LINE, pltpu.SMEM((SLOTS,), jnp.int32), ONE],
    )(inc, right, line_row)
    msg, raw, norm_left, left, tab2, cols0, cols1 = call(
        first_send_kernel,
        [VMEM] * 2,
        (msg_shape, vec, col8, left_shape, table, table, table),
        (VMEM,) * 4 + (SMEM,) * 3,
        [LINE] * 3 + [pltpu.SemaphoreType.DMA((3,))],
    )(keep, swap(send))
    start = norm_left
    state = None
    for repeat in range(ITERS):
        inc = exchange(msg)
        if repeat == ITERS - 1:
            break
        if repeat == 0:
            msg, left, norm_right, high2, low2, high2_t, low2_t = call(
                first_user_kernel,
                [SMEM] * 2 + [VMEM] * 8,
                (msg_shape, left_shape, col8, terms, terms, terms, terms),
                (VMEM,) * 7,
                [LEFT, LEFTS2],
            )(*small(tab, tab2), inc, left, norm_left, *near(high, low, high_t, low_t, blocks2))
        else:
            msg, left, norm_right = call(
                user_kernel,
                [SMEM] * 2 + [VMEM] * 11,
                (msg_shape, left_shape, col8),
                None,
                [LEFT, LEFTS2],
            )(
                *small(tab, tab2), inc, left, norm_left,
                *near(high, low, high2, low2, high_t, low_t, high2_t, low2_t),
            )
        inc = exchange(msg)
        first = repeat == 0
        tail = (start,) if first else state
        outs = call(
            lambda *refs, first=first: send_kernel(first, *refs),
            [SMEM] * 2 + [VMEM] * (3 + len(tail)),
            (msg_shape, vec, col8, vec, vec, shape(4 * RHS, BS)),
            None,
            [pltpu.VMEM((VEC, BS), f32)] * 4,
        )(*small(cols0, cols1), inc, raw, norm_right, *tail)
        msg, raw, norm_left = outs[:3]
        state = outs[3:]
    ends = shape(ENDS, BS)
    rows, keep, send = call(
        last_user_kernel,
        [SMEM] * 2 + [VMEM] * 12,
        (shape(2 * OWNERS, BS), ends, ends),
        None,
        [LEFT] * 2,
    )(
        *small(tab, tab2), inc, left, norm_left, *near(high_t, low_t, high2_t, low2_t),
        raw, start, *state,
    )
    theirs = swap(send)
    rows = lax.all_to_all(rows, GRP_SHARD, 0, 0, tiled=True)
    full = shape(COLS_OWN * RHS, BS)
    sol, left, rel = call(final_kernel, [VMEM] * 3, (full, full, shape(RHS)))(rows, keep, theirs)

    def tall(x):
        return x.reshape(COLS_OWN, RHS, BS).transpose(0, 2, 1).reshape(COLS_OWN * BS, RHS)

    return tall(sol), tall(left), rel


def solution(mesh):
    torus = Mesh(
        mesh.devices.reshape(mesh.shape["grp"], 4, 4, 4), ("grp", "shard_0", "shard_1", "shard_2")
    )
    return jax.shard_map(
        on_device,
        mesh=torus,
        in_specs=(
            P(GRP_SHARD, None, None),
            P(GRP_SHARD),
            P(GRP_SHARD, None),
            P(GRP_SHARD),
            P(GRP_SHARD, None),
        ),
        out_specs=(P(SHARD, None), P(GRP_SHARD, None), P()),
        check_vma=False,
    )
```
